128 devices in a mesh: lat: 8 (over z, core), lon: 16 (over y, x).
Axes of the slice: x: 4, y: 4, z: 4, core: 2. Of those that a mesh axis runs over, the one named last changes fastest.
Arguments:
- tracers: float32 [16, 8, 128, 2048], P(None, None, 'lat', 'lon'), may hold values from -6 to 6
- winds: float32 [3, 8, 128, 2048], P(None, None, 'lat', 'lon'), may hold values from -4 to 4
- depart_first: int32 [3, 8, 128, 2048], P(None, None, 'lat', 'lon'), may hold values from -3 to 2, as said below
- depart_second: int32 [3, 8, 128, 2048], P(None, None, 'lat', 'lon'), may hold values from -2 to 1, as said below
- fluxes: bfloat16 [6144, 128, 256], P(('lat', 'lon')), may hold values from 0.049804688 to 5
- remap_weights: bfloat16 [6144, 4, 256, 128], P(('lat', 'lon')), may hold values from 0.00019931793 to 0.019897461
- target_device: int32 [6144, 4], P(('lat', 'lon')), may hold values from 0 to 127, all different within a row; in each aligned block of 48 rows (0 to 47, 48 to 95, ...) at most 2 rows name the same one
- target_block: int32 [6144, 4], P(('lat', 'lon')), may hold values from 0 to 15
Outputs:
- advected: float32 [16, 8, 128, 2048], P(None, None, 'lat', 'lon')
The draws below stay inside these ranges and needn't reach their ends.
Inputs may be any that keep to these rules, and one draw needn't show every extreme that they name: `depart_first`: component 0 (levels) is -1 or 0; components 1 and 2 are row and column offsets. `depart_second`: component 0 (levels) is -1 or 0; components 1 and 2 are row and column offsets. `target_device`: device g is the one at lat index g // 16 and lon index g % 16. Each row names 4 different devices; among the rows of one device no device is named more than 2 times.
All inputs are finite; a program needn't handle non-finite values.
Results may differ from the reference program's by a relative error of at most 0.00088.
Values may be sent and summed in bfloat16 or wider, within the bound.
No kernel may reach another device: no remote copies, remote signals or barrier semaphores. Data moves between devices by JAX's collectives and lax.ppermute only.
A program may use at most 192 MiB of HBM per device.

```python
import math
import jax
import jax.numpy as jnp
import numpy as np
from jax import lax

NTR = 16
LEV = 8
CLAT = 16
CLON = 128
K = 4
CAP = 2
NTILE = 48
TILE_CELLS = 256
BLK_DEV = 16
HMAX = 3
ROWS = 128
BCOLS = 128
NLAT = 128
NLON = 2048
TILES = 6144
N_LAT = 8
N_LON = 16
DEVICES = 128


def offsets_first(key):
    vertical = jax.random.randint(jax.random.fold_in(key, 1), (1, LEV, NLAT, NLON), -1, 1)
    across = jax.random.randint(jax.random.fold_in(key, 2), (2, LEV, NLAT, NLON), -HMAX, HMAX)
    return jnp.concatenate([vertical, across], axis=0).astype(jnp.int32)


def draw_depart_first(key, part):
    return offsets_first(jax.random.fold_in(key, 11))


def draw_depart_second(key, part):
    first = offsets_first(jax.random.fold_in(key, 11))
    extra = jax.random.randint(jax.random.fold_in(key, 12), first.shape, 0, 2)
    return jnp.floor_divide(first + extra, 2).astype(jnp.int32)


def draw_winds(key, part):
    first = offsets_first(jax.random.fold_in(key, 11)).astype(jnp.float32)
    phase = jax.random.uniform(jax.random.fold_in(key, 13), first.shape, jnp.float32, -0.25, 1.25)
    return -(first + phase)


def touch_ends(entries, stream_key, low, top_value):
    longest = entries.shape.index(max(entries.shape))
    spots = []
    for shift in (0, 1):
        where = [jax.random.randint(jax.random.fold_in(stream_key, axis), (), 0, length) for axis, length in enumerate(entries.shape)]
        where[longest] = (where[longest] + shift) % entries.shape[longest]
        spots.append(tuple(where))
    return entries.at[spots[0]].set(low).at[spots[1]].set(top_value)


def level_of(rng, extent, pieces, smallest, largest):
    gain, own = 1.0, jax.random.fold_in(rng, 6)
    for dim, blocks in pieces:
        steps = jnp.exp(jax.random.uniform(jax.random.fold_in(own, dim), (blocks,), jnp.float32, smallest / len(pieces), largest / len(pieces)))
        gain = gain * jnp.repeat(steps, extent[dim] // blocks).reshape([-1 if axis == dim else 1 for axis in range(len(extent))])
    return gain


def deal_out(key, own, number, rows, count, top, reach, lean):
    order = jax.random.permutation(key, count)
    crowded, usual = load_shares(count, rows * top, reach, lean, True), load_shares(count, rows * top, reach, lean, False)
    places = jnp.arange(count)

    def named(tallies, offset_by):
        used = int((tallies > 0).sum())
        fixed = max(1, used // 4)
        passed = fixed + (places - fixed + offset_by * (used - fixed)) % max(1, count - fixed)
        return jnp.zeros((count,), jnp.int32).at[order[jnp.where(places < fixed, places, passed)]].set(jnp.asarray(tallies, jnp.int32))

    tallies = jnp.where(number % 4 == 0, named(crowded, number // 4), named(usual, number - number // 4 - 1))
    mixed = jax.random.permutation(jax.random.fold_in(own, 3), count)
    source_of, sink = mixed[0:count // 2 * 2:2], mixed[1:count // 2 * 2:2]
    slack = jnp.minimum(tallies[source_of] - 1, reach - tallies[sink]) // 2
    slack = jnp.where((source_of == order[0]) | (sink == order[0]) | (tallies[sink] == 0), 0, jnp.maximum(slack, 0))
    passed = jax.random.randint(jax.random.fold_in(own, 4), (count // 2,), 0, 1 << 20) % (slack + 1)
    tallies = tallies.at[source_of].add(-passed).at[sink].add(passed)
    labels = jnp.searchsorted(jnp.cumsum(tallies), jnp.arange(rows * top), side="right").astype(jnp.int32)
    table = labels.reshape(top, rows).T
    table = table[jax.random.permutation(jax.random.fold_in(own, 1), rows)]
    offset_by = jax.random.randint(jax.random.fold_in(own, 2), (rows, 1), 0, top)
    return jnp.take_along_axis(table, (jnp.arange(top)[None, :] + offset_by) % top, axis=1)


def load_shares(amount, total, most, slope, full):
    loads = [(1 << 20) // math.isqrt(grade ** slope) + 1 for grade in range(1, amount + 1)]
    largest = most if full else min(most, max(-(-total // amount), total * loads[0] // sum(loads)))
    least = 1 if total - largest >= amount - 1 else 0
    counts, surplus = [largest] + [least] * (amount - 1), total - largest - least * (amount - 1)
    while surplus > 0:
        movable = [i for i in range(1, amount) if counts[i] < largest] or [i for i in range(1, amount) if counts[i] < most]
        pool, left = sum([loads[i] for i in movable]), surplus
        for i in movable:
            addition = min(most - counts[i], max(1, left * loads[i] // pool), surplus)
            counts[i] = counts[i] + addition
            surplus = surplus - addition
    return np.array(counts)


def bell_draw(key, dims, deviation, bound, cuts=(), held_as=jnp.bfloat16):
    result = deviation * jax.random.normal(key, dims, jnp.float32)
    if cuts:
        result = result * level_of(key, dims, cuts, -0.22, 0.18)
    return jnp.clip(result, -bound, bound).astype(held_as)


def setup_inputs(seed: int = 0) -> dict:
    key_of = jax.random.split(jax.random.key(seed), 9)
    tracers = bell_draw(key_of[0], (NTR, LEV, NLAT, NLON), 1.0, 6.0, ((2, 8), (3, 16)), jnp.float32)
    winds = draw_winds(jax.random.fold_in(key_of[8], 71), 0)
    depart_first = draw_depart_first(jax.random.fold_in(key_of[8], 71), 0)
    depart_second = draw_depart_second(jax.random.fold_in(key_of[8], 71), 0)
    fluxes = jnp.clip(jnp.exp(math.log(5.0) - 4.609084 * jax.random.uniform(key_of[4], (TILES, ROWS, TILE_CELLS), jnp.float32) ** level_of(key_of[4], (TILES, ROWS, TILE_CELLS), ((0, 128),), -0.2, 0.2)), 0.049804688, 5.0).astype(jnp.bfloat16)
    remap_weights = jnp.clip(jnp.exp(math.log(0.019897461) - 4.603446 * jax.random.uniform(key_of[5], (TILES, K, TILE_CELLS, BCOLS), jnp.float32) ** level_of(key_of[5], (TILES, K, TILE_CELLS, BCOLS), ((0, 128),), -0.2, 0.2)), 0.00019931793, 0.019897461).astype(jnp.bfloat16)
    target_device_keys = jax.random.split(jax.random.fold_in(key_of[6], 1), TILES // NTILE)
    target_device_turns = jax.random.permutation(jax.random.fold_in(key_of[6], 3), TILES // NTILE)
    target_device = jax.vmap(lambda own, number: deal_out(jax.random.fold_in(key_of[6], 2), own, number, NTILE, DEVICES, K, CAP, 2))(target_device_keys, target_device_turns).reshape((TILES, K))
    target_block = touch_ends(jax.random.randint(key_of[7], (TILES, K), 0, BLK_DEV), jax.random.fold_in(key_of[7], 1), 0, BLK_DEV - 1).astype(jnp.int32)
    return {"tracers": tracers, "winds": winds, "depart_first": depart_first, "depart_second": depart_second, "fluxes": fluxes, "remap_weights": remap_weights, "target_device": target_device, "target_block": target_block}


def cubic_weights(frac):
    first = -frac * (frac - 1.0) * (frac - 2.0) / 6.0
    second = (frac + 1.0) * (frac - 1.0) * (frac - 2.0) / 2.0
    third = -(frac + 1.0) * frac * (frac - 2.0) / 2.0
    fourth = (frac + 1.0) * frac * (frac - 1.0) / 6.0
    return (first, second, third, fourth)


def tricubic(padded, base, frac):
    chans, levels, rows, cols = padded.shape
    flat = padded.reshape(chans, levels * rows * cols)
    level_w = cubic_weights(frac[0])
    row_w = cubic_weights(frac[1])
    col_w = jnp.stack(cubic_weights(frac[2]))
    col_index = jnp.stack([base[2] + step for step in (-1, 0, 1, 2)]).astype(jnp.int32)
    total = jnp.zeros((chans,) + base.shape[1:], jnp.float32)
    for above in range(4):
        level_index = jnp.clip(base[0] + above - 1, 0, levels - 1).astype(jnp.int32)
        for across in range(4):
            row_index = (base[1] + across - 1).astype(jnp.int32)
            index = ((level_index * rows + row_index) * cols)[None] + col_index
            picked = jnp.take(flat, index.reshape(-1), axis=1).reshape((chans,) + index.shape)
            summed = jnp.sum(picked * col_w[None], axis=1)
            total = total + (level_w[above] * row_w[across])[None] * summed
    return total


def per_channel(padded, base, frac):
    return lax.map(lambda single: tricubic(single[None], base, frac)[0], padded)


def extend(field, width):
    padded = jnp.pad(field, ((0, 0), (0, 0), (width, width), (0, 0)))
    return jnp.concatenate([padded[..., -width:], padded, padded[..., :width]], axis=3)


def reference(tracers, winds, depart_first, depart_second, fluxes, remap_weights, target_device, target_block):
    width = HMAX + 1
    shape = (LEV, NLAT, NLON)
    position = jnp.stack([
        lax.broadcasted_iota(jnp.int32, shape, 0),
        lax.broadcasted_iota(jnp.int32, shape, 1) + width,
        lax.broadcasted_iota(jnp.int32, shape, 2) + width,
    ])
    frac_first = jnp.clip(-winds - depart_first.astype(winds.dtype), 0.0, 1.0)
    midwind = per_channel(extend(winds, width), position + depart_first, frac_first)
    frac_second = jnp.clip(-(winds + midwind) * 0.5 - depart_second.astype(winds.dtype), 0.0, 1.0)
    moved = per_channel(extend(tracers, width), position + depart_second, frac_second)

    groups = TILES // NTILE
    block_ids = (target_device * BLK_DEV + target_block).astype(jnp.int32)

    def accumulate(total, piece):
        flux_group, weight_group, id_group = piece
        product = jnp.einsum("trc,tkcb->tkrb", flux_group.astype(jnp.float32), weight_group.astype(jnp.float32))
        product = lax.optimization_barrier(product.astype(jnp.bfloat16)).astype(jnp.float32)
        total = total.at[id_group.reshape(-1)].add(product.reshape(-1, ROWS, BCOLS))
        return total, None

    start = jnp.zeros((groups * BLK_DEV, ROWS, BCOLS), jnp.float32)
    blocks, unused = lax.scan(accumulate, start, (
        fluxes.reshape(groups, NTILE, ROWS, TILE_CELLS),
        remap_weights.reshape(groups, NTILE, K, TILE_CELLS, BCOLS),
        block_ids.reshape(groups, NTILE, K)))
    grid = blocks.reshape(N_LAT, N_LON, BLK_DEV, NTR, LEV, BCOLS).transpose(3, 4, 0, 1, 2, 5)
    grid = grid.reshape(NTR, LEV, N_LAT, N_LON, CLAT, CLON).transpose(0, 1, 2, 4, 3, 5)
    emission = grid.reshape(NTR, LEV, NLAT, NLON)
    return moved + emission
```

```python
import jax
import jax.numpy as jnp
from jax import lax
from jax.experimental import pallas as pl
from jax.experimental.pallas import tpu as pltpu
from jax.sharding import PartitionSpec as P

NTR = 16
LEV = 8
CAP = 2
BLK_DEV = 16
ROWS = 16
COLS = 128
WIDE = 4
NEAR = 3
WROWS = ROWS + 2 * WIDE
TROWS = ROWS + 2 * NEAR
TILE_STEP = 4
SLOT_STEP = 16
VMEM_LIMIT = 60 * 1024 * 1024


def params(*semantics):
    return pltpu.CompilerParams(
        dimension_semantics=semantics or None, vmem_limit_bytes=VMEM_LIMIT
    )


def remap_kernel(device_ref, block_ref, flux_ref, weight_ref, out_hbm, mark_ref, held, sems, counts):
    step = pl.program_id(0)
    steps = pl.num_programs(0)
    links = weight_ref.shape[1]
    bank = lax.rem(step, 2)

    @pl.when(step == 0)
    def _():
        def clear(i, carry):
            counts[i] = 0
            return carry

        lax.fori_loop(0, counts.shape[0], clear, 0)
        mark_ref[...] = jnp.full(mark_ref.shape, BLK_DEV, jnp.int32)

    def copy(which, slot, bank_at):
        return pltpu.make_async_copy(
            held.at[bank_at, which], out_hbm.at[slot], sems.at[bank_at, which]
        )

    @pl.when(step >= 2)
    def _():
        for which in range(TILE_STEP * links):
            copy(which, 0, bank).wait()

    lanes = lax.broadcasted_iota(jnp.int32, (1, COLS), 1)
    for part in range(TILE_STEP):
        flux = flux_ref[part]
        for pair in range(links // 2):
            both = jnp.concatenate(
                [weight_ref[part, 2 * pair], weight_ref[part, 2 * pair + 1]], axis=1
            )
            made = jnp.dot(flux, both, preferred_element_type=jnp.float32)
            made = made.astype(jnp.bfloat16)
            for side in range(2):
                link = 2 * pair + side
                which = part * links + link
                held[bank, which] = made[:, side * COLS : (side + 1) * COLS]
                tile = step * TILE_STEP + part
                owner = device_ref[tile, link]
                rank = counts[owner]
                counts[owner] = rank + 1
                mark_ref[owner] = jnp.where(
                    lanes == rank, block_ref[tile, link], mark_ref[owner]
                )
                copy(which, owner * CAP + rank, bank).start()

    @pl.when(step == steps - 1)
    def _():
        for which in range(TILE_STEP * links):
            copy(which, 0, 1 - bank).wait()
        for which in range(TILE_STEP * links):
            copy(which, 0, bank).wait()


def remap(fluxes, remap_weights, target_device, target_block, devices):
    tiles, rows, cells = fluxes.shape
    links, cols = remap_weights.shape[1], remap_weights.shape[3]
    return pl.pallas_call(
        remap_kernel,
        grid_spec=pltpu.PrefetchScalarGridSpec(
            num_scalar_prefetch=2,
            grid=(tiles // TILE_STEP,),
            in_specs=[
                pl.BlockSpec((TILE_STEP, rows, cells), lambda i, *_: (i, 0, 0)),
                pl.BlockSpec((TILE_STEP, links, cells, cols), lambda i, *_: (i, 0, 0, 0)),
            ],
            out_specs=[
                pl.BlockSpec(memory_space=pl.ANY),
                pl.BlockSpec((devices, 1, COLS), lambda i, *_: (0, 0, 0)),
            ],
            scratch_shapes=[
                pltpu.VMEM((2, TILE_STEP * links, rows, cols), jnp.bfloat16),
                pltpu.SemaphoreType.DMA((2, TILE_STEP * links)),
                pltpu.SMEM((devices,), jnp.int32),
            ],
        ),
        out_shape=[
            jax.ShapeDtypeStruct((devices * CAP, rows, cols), jnp.bfloat16),
            jax.ShapeDtypeStruct((devices, 1, COLS), jnp.int32),
        ],
        compiler_params=params("arbitrary"),
    )(target_device, target_block, fluxes, remap_weights)


def wind_piece(winds_ref, row, comp):
    return winds_ref[pl.ds(comp * LEV * ROWS + row, LEV, stride=ROWS), :]


def tracer_piece(tracers_ref, row, level, half):
    start = half * 8 * LEV * ROWS + level * ROWS + row
    return tracers_ref[pl.ds(start, 8, stride=LEV * ROWS), :]


WIND_MSG = WIDE * 3 * LEV
TRACER_MSG = NEAR * LEV * NTR


def edge_rows_kernel(tracers_ref, winds_ref, top_ref, bottom_ref):
    for target, wind_from, tracer_from in (
        (top_ref, 0, 0),
        (bottom_ref, ROWS - WIDE, ROWS - NEAR),
    ):
        for row in range(WIDE):
            for comp in range(3):
                at = (row * 3 + comp) * LEV
                target[at : at + LEV, :] = wind_piece(winds_ref, wind_from + row, comp)
        for row in range(NEAR):
            for level in range(LEV):
                for half in range(2):
                    at = WIND_MSG + (row * LEV + level) * NTR + half * 8
                    target[at : at + 8, :] = tracer_piece(
                        tracers_ref, tracer_from + row, level, half
                    )


def edge_rows(tracers, winds):
    shape = jax.ShapeDtypeStruct((WIND_MSG + TRACER_MSG, COLS), jnp.float32)
    return pl.pallas_call(
        edge_rows_kernel, out_shape=[shape, shape], compiler_params=params()
    )(tracers, winds)


EDGE = 2 * WIDE
PER_GROUP = COLS // EDGE
WIND_GROUPS = -(-WROWS // PER_GROUP)
GROUPS = TROWS + 3 * WIND_GROUPS


def edge_cols_kernel(tracers_ref, winds_ref, low_ref, high_ref, twide_ref, wwide_ref, edge_ref):
    per_row = LEV * NTR
    twide_ref[0:TRACER_MSG, :] = low_ref[WIND_MSG : WIND_MSG + TRACER_MSG, :]
    last = (NEAR + ROWS) * per_row
    twide_ref[last : last + TRACER_MSG, :] = high_ref[WIND_MSG : WIND_MSG + TRACER_MSG, :]
    wwide_ref[0:WIND_MSG, :] = low_ref[0:WIND_MSG, :]
    last = (WIDE + ROWS) * 3 * LEV
    wwide_ref[last : last + WIND_MSG, :] = high_ref[0:WIND_MSG, :]

    def rearrange(row, carry):
        for comp in range(3):
            at = pl.multiple_of((row + WIDE) * 3 * LEV + comp * LEV, 8)
            wwide_ref[pl.ds(at, LEV), :] = wind_piece(winds_ref, row, comp)
        for level in range(LEV):
            for half in range(2):
                at = pl.multiple_of((row + NEAR) * per_row + level * NTR + half * 8, 8)
                twide_ref[pl.ds(at, 8), :] = tracer_piece(tracers_ref, row, level, half)
        return carry

    lax.fori_loop(0, ROWS, rearrange, 0)
    group_of = lax.broadcasted_iota(jnp.int32, (8, COLS), 1) // EDGE

    def gather_tracers(row, carry):
        packed = jnp.zeros((8, COLS), jnp.float32)
        for spot in range(PER_GROUP):
            at = pl.multiple_of(row * per_row + spot * 8, 8)
            turned = pltpu.roll(twide_ref[pl.ds(at, 8), :], (WIDE + EDGE * spot) % COLS, 1)
            packed = jnp.where(group_of == spot, turned, packed)
        edge_ref[pl.ds(pl.multiple_of(row * 8, 8), 8), :] = packed
        return carry

    lax.fori_loop(0, TROWS, gather_tracers, 0)
    for comp in range(3):
        for part in range(WIND_GROUPS):
            packed = jnp.zeros((8, COLS), jnp.float32)
            for spot in range(min(PER_GROUP, WROWS - part * PER_GROUP)):
                at = ((part * PER_GROUP + spot) * 3 + comp) * LEV
                turned = pltpu.roll(wwide_ref[at : at + 8, :], (WIDE + EDGE * spot) % COLS, 1)
                packed = jnp.where(group_of == spot, turned, packed)
            at = (TROWS + comp * WIND_GROUPS + part) * 8
            edge_ref[at : at + 8, :] = packed


def edge_cols(tracers, winds, low, high):
    return pl.pallas_call(
        edge_cols_kernel,
        out_shape=[
            jax.ShapeDtypeStruct((TROWS * LEV * NTR, COLS), jnp.float32),
            jax.ShapeDtypeStruct((WROWS * 3 * LEV, COLS), jnp.float32),
            jax.ShapeDtypeStruct((GROUPS * 8, COLS), jnp.float32),
        ],
        compiler_params=params(),
    )(tracers, winds, low, high)


def cubic_weights(frac):
    first = -frac * (frac - 1.0) * (frac - 2.0) / 6.0
    second = (frac + 1.0) * (frac - 1.0) * (frac - 2.0) / 2.0
    third = -(frac + 1.0) * frac * (frac - 2.0) / 2.0
    fourth = (frac + 1.0) * frac * (frac - 1.0) / 6.0
    return (first, second, third, fourth)


def spread_weights(offset, frac, lowest, highest):
    stencil = cubic_weights(frac)
    hits = {value: offset == value for value in range(lowest, highest + 1)}
    spread = []
    for target in range(lowest - 1, highest + 3):
        weight = jnp.zeros(frac.shape, jnp.float32)
        for step in range(4):
            value = target - step + 1
            if value in hits:
                weight = weight + jnp.where(hits[value], stencil[step], 0.0)
        spread.append(weight)
    return spread


def column_shifts(main, edge, reach):
    lane = lax.broadcasted_iota(jnp.int32, main.shape, 1)
    shifted = []
    for step in range(-reach, reach + 1):
        if step == 0:
            shifted.append(main)
            continue
        inside = lane < COLS - step if step > 0 else lane >= -step
        turn = (COLS - step) % COLS
        shifted.append(jnp.where(inside, pltpu.roll(main, turn, 1), pltpu.roll(edge, turn, 1)))
    return shifted


def level_shift(value, step):
    if step == 0:
        return value
    level = lax.broadcasted_iota(jnp.int32, value.shape, 0)
    turned = pltpu.roll(value, (LEV - step) % LEV, 0)
    if step > 0:
        end = jnp.broadcast_to(value[LEV - 1 : LEV, :], value.shape)
        return jnp.where(level >= LEV - step, end, turned)
    end = jnp.broadcast_to(value[0:1, :], value.shape)
    return jnp.where(level < -step, end, turned)


W_TAPS = 9
T_TAPS = 7
L_TAPS = 5
SPREADS = L_TAPS + 2 * T_TAPS


def advect_kernel(
    twide_ref, wwide_ref, left_ref, right_ref, first_ref, second_ref, winds_ref, out_ref,
    wind_taps, tracer_taps, spread_ref,
):
    lane = lax.broadcasted_iota(jnp.int32, (8, COLS), 1)
    from_left = lax.rem(lane, EDGE) < WIDE

    def edge_at(group, spot):
        at = group * 8 if isinstance(group, int) else pl.multiple_of(group * 8, 8)
        both = jnp.where(from_left, left_ref[pl.ds(at, 8), :], right_ref[pl.ds(at, 8), :])
        return pltpu.roll(both, (COLS - WIDE - EDGE * spot) % COLS, 1)

    for comp in range(3):
        for row in range(WROWS):
            edge = edge_at(TROWS + comp * WIND_GROUPS + row // PER_GROUP, row % PER_GROUP)
            at = (row * 3 + comp) * LEV
            shifted = column_shifts(wwide_ref[at : at + LEV, :], edge, WIDE)
            for side in range(W_TAPS):
                for above in range(L_TAPS):
                    wind_taps[row, comp, above, side] = level_shift(shifted[side], above - 2)

    def wind_row(row, carry):
        def component(ref, comp):
            return ref[pl.ds(comp * LEV * ROWS + row, LEV, stride=ROWS), :]

        wind = [component(winds_ref, comp) for comp in range(3)]
        first = [component(first_ref, comp) for comp in range(3)]
        frac = [
            jnp.clip(-wind[comp] - first[comp].astype(jnp.float32), 0.0, 1.0)
            for comp in range(3)
        ]
        level_w = spread_weights(first[0], frac[0], -1, 0)
        row_w = spread_weights(first[1], frac[1], -3, 2)
        col_w = spread_weights(first[2], frac[2], -3, 2)
        total = [jnp.zeros((LEV, COLS), jnp.float32) for _ in range(3)]
        for above in range(L_TAPS):
            part = [jnp.zeros((LEV, COLS), jnp.float32) for _ in range(3)]
            for across in range(W_TAPS):
                for comp in range(3):
                    inner = col_w[0] * wind_taps[row + across, comp, above, 0]
                    for side in range(1, W_TAPS):
                        inner = inner + col_w[side] * wind_taps[row + across, comp, above, side]
                    part[comp] = part[comp] + row_w[across] * inner
            for comp in range(3):
                total[comp] = total[comp] + level_w[above] * part[comp]
        second = [component(second_ref, comp) for comp in range(3)]
        frac = [
            jnp.clip(
                -(wind[comp] + total[comp]) * 0.5 - second[comp].astype(jnp.float32), 0.0, 1.0
            )
            for comp in range(3)
        ]
        weights = spread_weights(second[0], frac[0], -1, 0)
        weights += spread_weights(second[1], frac[1], -2, 1)
        weights += spread_weights(second[2], frac[2], -2, 1)
        for which in range(SPREADS):
            spread_ref[row, which] = weights[which]
        return carry

    lax.fori_loop(0, ROWS, wind_row, 0)

    def tracer_shifts(row, carry):
        for spot in range(PER_GROUP):
            edge = edge_at(row, spot)
            at = pl.multiple_of(row * LEV * NTR + spot * 8, 8)
            shifted = column_shifts(twide_ref[pl.ds(at, 8), :], edge, NEAR)
            for side in range(T_TAPS):
                tracer_taps[row, spot, side] = shifted[side]
        return carry

    lax.fori_loop(0, TROWS, tracer_shifts, 0)

    def tracer_cell(cell, carry):
        row, level = cell // LEV, lax.rem(cell, LEV)

        def weight(which):
            return jnp.broadcast_to(spread_ref[row, which, pl.ds(level, 1), :], (8, COLS))

        row_w = [weight(L_TAPS + which) for which in range(T_TAPS)]
        col_w = [weight(L_TAPS + T_TAPS + which) for which in range(T_TAPS)]
        total = [jnp.zeros((8, COLS), jnp.float32) for _ in range(2)]
        for above in range(L_TAPS):
            source = jnp.clip(level + above - 2, 0, LEV - 1)
            level_w = weight(above)
            part = [jnp.zeros((8, COLS), jnp.float32) for _ in range(2)]
            for across in range(T_TAPS):
                for half in range(2):
                    taps = tracer_taps.at[row + across, source * 2 + half]
                    inner = col_w[0] * taps[0]
                    for side in range(1, T_TAPS):
                        inner = inner + col_w[side] * taps[side]
                    part[half] = part[half] + row_w[across] * inner
            for half in range(2):
                total[half] = total[half] + level_w * part[half]
        for half in range(2):
            start = half * 8 * LEV * ROWS + level * ROWS + row
            out_ref[pl.ds(start, 8, stride=LEV * ROWS), :] = total[half]
        return carry

    lax.fori_loop(0, ROWS * LEV, tracer_cell, 0)


def advect(twide, wwide, left, right, first, second, winds):
    return pl.pallas_call(
        advect_kernel,
        out_shape=jax.ShapeDtypeStruct((NTR * LEV * ROWS, COLS), jnp.float32),
        scratch_shapes=[
            pltpu.VMEM((WROWS, 3, L_TAPS, W_TAPS, LEV, COLS), jnp.float32),
            pltpu.VMEM((TROWS, LEV * 2, T_TAPS, 8, COLS), jnp.float32),
            pltpu.VMEM((ROWS, SPREADS, LEV, COLS), jnp.float32),
        ],
        compiler_params=params(),
    )(twide, wwide, left, right, first, second, winds)


def combine_kernel(mark_ref, arrived_ref, moved_ref, out_ref, total):
    step = pl.program_id(0)
    rows = arrived_ref.shape[1]

    @pl.when(step == 0)
    def _():
        total[...] = jnp.zeros(total.shape, jnp.float32)

    for which in range(SLOT_STEP):
        slot = step * SLOT_STEP + which
        block = mark_ref[slot // CAP, 0, lax.rem(slot, CAP)]
        at = pl.ds(pl.multiple_of(block * rows, rows), rows)
        total[at, :] = total[at, :] + arrived_ref[which].astype(jnp.float32)

    @pl.when(step == pl.num_programs(0) - 1)
    def _():
        for row in range(rows):
            picked = total[pl.ds(row, BLK_DEV, stride=rows), :]
            at = row * ROWS
            out_ref[at : at + ROWS, :] = moved_ref[at : at + ROWS, :] + picked


def combine(marks, arrived, moved):
    slots, rows, cols = arrived.shape
    return pl.pallas_call(
        combine_kernel,
        grid_spec=pltpu.PrefetchScalarGridSpec(
            num_scalar_prefetch=1,
            grid=(slots // SLOT_STEP,),
            in_specs=[
                pl.BlockSpec((SLOT_STEP, rows, cols), lambda i, *_: (i, 0, 0)),
                pl.BlockSpec(moved.shape, lambda i, *_: (0, 0)),
            ],
            out_specs=pl.BlockSpec(moved.shape, lambda i, *_: (0, 0)),
            scratch_shapes=[pltpu.VMEM(((BLK_DEV + 1) * rows, cols), jnp.float32)],
        ),
        out_shape=jax.ShapeDtypeStruct(moved.shape, jnp.float32),
        compiler_params=params("arbitrary"),
    )(marks, arrived, moved)


def body(
    tracers, winds, depart_first, depart_second, fluxes, remap_weights, target_device, target_block
):
    lat_count, lon_count = lax.axis_size("lat"), lax.axis_size("lon")
    both = ("lat", "lon")
    slots, marks = remap(
        fluxes, remap_weights, target_device, target_block, lat_count * lon_count
    )
    shape = tracers.shape
    tracers, winds, slots, marks = lax.optimization_barrier((tracers, winds, slots, marks))
    arrived = lax.all_to_all(slots, both, split_axis=0, concat_axis=0, tiled=True)
    flat = lambda field: field.reshape(-1, COLS)
    tracers, winds = flat(tracers), flat(winds)
    top, bottom = edge_rows(tracers, winds)
    up = [(i, i + 1) for i in range(lat_count - 1)]
    low = lax.ppermute(bottom, "lat", up)
    high = lax.ppermute(top, "lat", [(b, a) for a, b in up])
    twide, wwide, edge = edge_cols(tracers, winds, low, high)
    around = [(i, (i + 1) % lon_count) for i in range(lon_count)]
    left = lax.ppermute(edge, "lon", around)
    right = lax.ppermute(edge, "lon", [(b, a) for a, b in around])
    edge, marks = lax.optimization_barrier((edge, marks))
    arrived_marks = lax.all_to_all(marks, both, split_axis=0, concat_axis=0, tiled=True)
    moved = advect(
        twide, wwide, left, right, flat(depart_first), flat(depart_second), winds
    )
    return combine(arrived_marks, arrived, moved).reshape(shape)


def solution(mesh):
    in_specs = (
        P(None, None, "lat", "lon"),
        P(None, None, "lat", "lon"),
        P(None, None, "lat", "lon"),
        P(None, None, "lat", "lon"),
        P(("lat", "lon"), None, None),
        P(("lat", "lon"), None, None, None),
        P(("lat", "lon"), None),
        P(("lat", "lon"), None),
    )
    out_specs = P(None, None, "lat", "lon")
    return jax.shard_map(body, mesh=mesh, in_specs=in_specs, out_specs=out_specs, check_vma=False)
```

```python
import jax
import jax.numpy as jnp
from jax import lax
from jax.experimental import pallas as pl
from jax.experimental.pallas import tpu as pltpu
from jax.sharding import PartitionSpec as P

NTR = 16
LEV = 8
CAP = 2
BLK_DEV = 16
ROWS = 16
COLS = 128
WIDE = 4
NEAR = 3
WROWS = ROWS + 2 * WIDE
TROWS = ROWS + 2 * NEAR
EDGE = 2 * WIDE
PER_GROUP = COLS // EDGE
TILE_STEP = 4
SOURCE_STEP = 8
SUMS = 4
MARK_ROWS = 8
VMEM_LIMIT = 60 * 1024 * 1024


def params(*semantics):
    return pltpu.CompilerParams(
        dimension_semantics=semantics or None, vmem_limit_bytes=VMEM_LIMIT
    )


def remap_kernel(
    device_ref, block_ref, flux_ref, weight_ref, out_hbm, held, marks, sent, sems, mark_sem, counts
):
    step = pl.program_id(0)
    steps = pl.num_programs(0)
    links, rows = weight_ref.shape[1], flux_ref.shape[1]
    bank = lax.rem(step, 2)

    @pl.when(step == 0)
    def _():
        def clear(i, carry):
            counts[i] = 0
            return carry

        lax.fori_loop(0, counts.shape[0], clear, 0)
        marks[...] = jnp.full(marks.shape, BLK_DEV, jnp.float32)

    def copy(which, owner, rank, bank_at):
        into = pl.ds(pl.multiple_of(rank * rows, rows), rows)
        return pltpu.make_async_copy(
            held.at[bank_at, which], out_hbm.at[owner, into], sems.at[bank_at, which]
        )

    @pl.when(step >= 2)
    def _():
        for which in range(TILE_STEP * links):
            copy(which, 0, 0, bank).wait()

    for part in range(TILE_STEP):
        flux = flux_ref[part]
        for pair in range(links // 2):
            both = jnp.concatenate(
                [weight_ref[part, 2 * pair], weight_ref[part, 2 * pair + 1]], axis=1
            )
            made = jnp.dot(flux, both, preferred_element_type=jnp.float32)
            made = made.astype(jnp.bfloat16)
            for side in range(2):
                which = part * links + 2 * pair + side
                held[bank, which] = made[:, side * COLS : (side + 1) * COLS]
    for part in range(TILE_STEP):
        for link in range(links):
            tile = step * TILE_STEP + part
            owner = device_ref[link, tile]
            rank = counts[owner]
            counts[owner] = rank + 1
            copy(part * links + link, owner, rank, bank).start()
            value = block_ref[link, tile].astype(jnp.float32)
            marks[owner, pl.ds(rank, 1), :] = jnp.full((1, COLS), value, jnp.float32)

    @pl.when(step == steps - 1)
    def _():
        sent[...] = marks[...].astype(jnp.bfloat16)
        last = pltpu.make_async_copy(
            sent, out_hbm.at[:, pl.ds(CAP * rows, MARK_ROWS)], mark_sem
        )
        last.start()
        for which in range(TILE_STEP * links):
            copy(which, 0, 0, 1 - bank).wait()
        for which in range(TILE_STEP * links):
            copy(which, 0, 0, bank).wait()
        last.wait()


def remap(fluxes, remap_weights, target_device, target_block, devices):
    tiles, rows, cells = fluxes.shape
    links, cols = remap_weights.shape[1], remap_weights.shape[3]
    return pl.pallas_call(
        remap_kernel,
        grid_spec=pltpu.PrefetchScalarGridSpec(
            num_scalar_prefetch=2,
            grid=(tiles // TILE_STEP,),
            in_specs=[
                pl.BlockSpec((TILE_STEP, rows, cells), lambda i, *_: (i, 0, 0)),
                pl.BlockSpec((TILE_STEP, links, cells, cols), lambda i, *_: (i, 0, 0, 0)),
            ],
            out_specs=pl.BlockSpec(memory_space=pl.ANY),
            scratch_shapes=[
                pltpu.VMEM((2, TILE_STEP * links, rows, cols), jnp.bfloat16),
                pltpu.VMEM((devices, MARK_ROWS, cols), jnp.float32),
                pltpu.VMEM((devices, MARK_ROWS, cols), jnp.bfloat16),
                pltpu.SemaphoreType.DMA((2, TILE_STEP * links)),
                pltpu.SemaphoreType.DMA,
                pltpu.SMEM((devices,), jnp.int32),
            ],
        ),
        out_shape=jax.ShapeDtypeStruct((devices, CAP * rows + MARK_ROWS, cols), jnp.bfloat16),
        compiler_params=params("arbitrary"),
    )(target_device.T, target_block.T, fluxes, remap_weights)


def wind_piece(winds_ref, row, comp):
    return winds_ref[pl.ds(comp * LEV * ROWS + row, LEV, stride=ROWS), :]


def tracer_piece(tracers_ref, row, level, half):
    start = half * 8 * LEV * ROWS + level * ROWS + row
    return tracers_ref[pl.ds(start, 8, stride=LEV * ROWS), :]


WIND_MSG = WIDE * 3 * LEV
TRACER_MSG = NEAR * LEV * NTR
TRACER_EDGE = WIND_MSG + TRACER_MSG
WIND_EDGE = TRACER_EDGE + NEAR * 8
MSG = WIND_EDGE + 3 * 8
EDGE_ROWS = (ROWS + 3) * 8


def edge_cols_kernel(tracers_ref, winds_ref, edge_ref):
    group_of = lax.broadcasted_iota(jnp.int32, (8, COLS), 1) // EDGE

    def packed(pieces):
        held = jnp.zeros((8, COLS), jnp.float32)
        for spot, piece in enumerate(pieces):
            turned = pltpu.roll(piece, (WIDE + EDGE * spot) % COLS, 1)
            held = jnp.where(group_of == spot, turned, held)
        return held

    def tracer_row(row, carry):
        pieces = [tracer_piece(tracers_ref, row, spot // 2, spot % 2) for spot in range(PER_GROUP)]
        edge_ref[pl.ds(pl.multiple_of(row * 8, 8), 8), :] = packed(pieces)
        return carry

    lax.fori_loop(0, ROWS, tracer_row, 0)
    for comp in range(3):
        at = (ROWS + comp) * 8
        edge_ref[at : at + 8, :] = packed([wind_piece(winds_ref, row, comp) for row in range(ROWS)])


def edge_cols(tracers, winds):
    return pl.pallas_call(
        edge_cols_kernel,
        out_shape=jax.ShapeDtypeStruct((EDGE_ROWS, COLS), jnp.float32),
        compiler_params=params(),
    )(tracers, winds)


def edge_rows_kernel(tracers_ref, winds_ref, left_ref, right_ref, top_ref, bottom_ref, both_ref):
    lane = lax.broadcasted_iota(jnp.int32, (EDGE_ROWS, COLS), 1)
    both_ref[...] = jnp.where(lax.rem(lane, EDGE) < WIDE, left_ref[...], right_ref[...])
    for target, wind_from, tracer_from in (
        (top_ref, 0, 0),
        (bottom_ref, ROWS - WIDE, ROWS - NEAR),
    ):
        for row in range(WIDE):
            for comp in range(3):
                at = (row * 3 + comp) * LEV
                target[at : at + LEV, :] = wind_piece(winds_ref, wind_from + row, comp)
        for row in range(NEAR):
            for level in range(LEV):
                for half in range(2):
                    at = WIND_MSG + (row * LEV + level) * NTR + half * 8
                    target[at : at + 8, :] = tracer_piece(
                        tracers_ref, tracer_from + row, level, half
                    )
        target[TRACER_EDGE:WIND_EDGE, :] = both_ref[tracer_from * 8 : (tracer_from + NEAR) * 8, :]
        target[WIND_EDGE:MSG, :] = both_ref[ROWS * 8 : EDGE_ROWS, :]


def edge_rows(tracers, winds, left, right):
    shape = jax.ShapeDtypeStruct((MSG, COLS), jnp.float32)
    return pl.pallas_call(
        edge_rows_kernel,
        out_shape=[shape, shape, jax.ShapeDtypeStruct((EDGE_ROWS, COLS), jnp.float32)],
        compiler_params=params(),
    )(tracers, winds, left, right)


def cubic_weights(frac):
    first = -frac * (frac - 1.0) * (frac - 2.0) / 6.0
    second = (frac + 1.0) * (frac - 1.0) * (frac - 2.0) / 2.0
    third = -(frac + 1.0) * frac * (frac - 2.0) / 2.0
    fourth = (frac + 1.0) * frac * (frac - 1.0) / 6.0
    return (first, second, third, fourth)


def spread_weights(offset, frac, lowest, highest):
    stencil = cubic_weights(frac)
    hits = {value: offset == value for value in range(lowest, highest + 1)}
    spread = []
    for target in range(lowest - 1, highest + 3):
        weight = jnp.zeros(frac.shape, jnp.float32)
        for step in range(4):
            value = target - step + 1
            if value in hits:
                weight = weight + jnp.where(hits[value], stencil[step], 0.0)
        spread.append(weight)
    return spread


def column_shifts(main, edge, reach):
    lane = lax.broadcasted_iota(jnp.int32, main.shape, 1)
    shifted = []
    for step in range(-reach, reach + 1):
        if step == 0:
            shifted.append(main)
            continue
        inside = lane < COLS - step if step > 0 else lane >= -step
        turn = (COLS - step) % COLS
        shifted.append(jnp.where(inside, pltpu.roll(main, turn, 1), pltpu.roll(edge, turn, 1)))
    return shifted


def level_shift(value, step):
    if step == 0:
        return value
    level = lax.broadcasted_iota(jnp.int32, value.shape, 0)
    turned = pltpu.roll(value, (LEV - step) % LEV, 0)
    if step > 0:
        end = jnp.broadcast_to(value[LEV - 1 : LEV, :], value.shape)
        return jnp.where(level >= LEV - step, end, turned)
    end = jnp.broadcast_to(value[0:1, :], value.shape)
    return jnp.where(level < -step, end, turned)


W_TAPS = 9
T_TAPS = 7
L_TAPS = 5
SPREADS = L_TAPS + 2 * T_TAPS


def advect_kernel(
    tracers_ref, low_ref, high_ref, both_ref, first_ref, second_ref, winds_ref, out_ref,
    wind_taps, tracer_taps, spread_ref,
):
    def edge_piece(ref, at, spot):
        return pltpu.roll(ref[pl.ds(at, 8), :], (COLS - WIDE - EDGE * spot) % COLS, 1)

    for comp in range(3):
        for row in range(WROWS):
            if row < WIDE:
                at = (row * 3 + comp) * LEV
                main = low_ref[at : at + LEV, :]
                edge = edge_piece(low_ref, WIND_EDGE + comp * 8, ROWS - WIDE + row)
            elif row < WIDE + ROWS:
                main = wind_piece(winds_ref, row - WIDE, comp)
                edge = edge_piece(both_ref, (ROWS + comp) * 8, row - WIDE)
            else:
                at = ((row - WIDE - ROWS) * 3 + comp) * LEV
                main = high_ref[at : at + LEV, :]
                edge = edge_piece(high_ref, WIND_EDGE + comp * 8, row - WIDE - ROWS)
            shifted = column_shifts(main, edge, WIDE)
            for side in range(W_TAPS):
                for above in range(L_TAPS):
                    wind_taps[row, comp, above, side] = level_shift(shifted[side], above - 2)

    def wind_row(row, carry):
        def component(ref, comp):
            return ref[pl.ds(comp * LEV * ROWS + row, LEV, stride=ROWS), :]

        wind = [component(winds_ref, comp) for comp in range(3)]
        first = [component(first_ref, comp) for comp in range(3)]
        frac = [
            jnp.clip(-wind[comp] - first[comp].astype(jnp.float32), 0.0, 1.0)
            for comp in range(3)
        ]
        level_w = spread_weights(first[0], frac[0], -1, 0)
        row_w = spread_weights(first[1], frac[1], -3, 2)
        col_w = spread_weights(first[2], frac[2], -3, 2)
        total = [jnp.zeros((LEV, COLS), jnp.float32) for _ in range(3)]
        for above in range(L_TAPS):
            part = [jnp.zeros((LEV, COLS), jnp.float32) for _ in range(3)]
            for across in range(W_TAPS):
                for comp in range(3):
                    inner = col_w[0] * wind_taps[row + across, comp, above, 0]
                    for side in range(1, W_TAPS):
                        inner = inner + col_w[side] * wind_taps[row + across, comp, above, side]
                    part[comp] = part[comp] + row_w[across] * inner
            for comp in range(3):
                total[comp] = total[comp] + level_w[above] * part[comp]
        second = [component(second_ref, comp) for comp in range(3)]
        frac = [
            jnp.clip(
                -(wind[comp] + total[comp]) * 0.5 - second[comp].astype(jnp.float32), 0.0, 1.0
            )
            for comp in range(3)
        ]
        weights = spread_weights(second[0], frac[0], -1, 0)
        weights += spread_weights(second[1], frac[1], -2, 1)
        weights += spread_weights(second[2], frac[2], -2, 1)
        for which in range(SPREADS):
            spread_ref[row, which] = weights[which]
        return carry

    lax.fori_loop(0, ROWS, wind_row, 0)

    def own_shifts(row, carry):
        for spot in range(PER_GROUP):
            main = tracer_piece(tracers_ref, row, spot // 2, spot % 2)
            edge = edge_piece(both_ref, pl.multiple_of(row * 8, 8), spot)
            shifted = column_shifts(main, edge, NEAR)
            for side in range(T_TAPS):
                tracer_taps[row + NEAR, spot, side] = shifted[side]
        return carry

    lax.fori_loop(0, ROWS, own_shifts, 0)
    for ref, onto in ((low_ref, 0), (high_ref, NEAR + ROWS)):

        def halo_shifts(row, carry, ref=ref, onto=onto):
            for spot in range(PER_GROUP):
                at = pl.multiple_of(WIND_MSG + row * LEV * NTR + spot * 8, 8)
                edge = edge_piece(ref, pl.multiple_of(TRACER_EDGE + row * 8, 8), spot)
                shifted = column_shifts(ref[pl.ds(at, 8), :], edge, NEAR)
                for side in range(T_TAPS):
                    tracer_taps[row + onto, spot, side] = shifted[side]
            return carry

        lax.fori_loop(0, NEAR, halo_shifts, 0)

    def tracer_cell(cell, carry):
        row, level = cell // LEV, lax.rem(cell, LEV)

        def weight(which):
            return jnp.broadcast_to(spread_ref[row, which, pl.ds(level, 1), :], (8, COLS))

        row_w = [weight(L_TAPS + which) for which in range(T_TAPS)]
        col_w = [weight(L_TAPS + T_TAPS + which) for which in range(T_TAPS)]
        total = [jnp.zeros((8, COLS), jnp.float32) for _ in range(2)]
        for above in range(L_TAPS):
            source = jnp.clip(level + above - 2, 0, LEV - 1)
            level_w = weight(above)
            part = [jnp.zeros((8, COLS), jnp.float32) for _ in range(2)]
            for across in range(T_TAPS):
                for half in range(2):
                    taps = tracer_taps.at[row + across, source * 2 + half]
                    inner = col_w[0] * taps[0]
                    for side in range(1, T_TAPS):
                        inner = inner + col_w[side] * taps[side]
                    part[half] = part[half] + row_w[across] * inner
            for half in range(2):
                total[half] = total[half] + level_w * part[half]
        for half in range(2):
            start = half * 8 * LEV * ROWS + level * ROWS + row
            out_ref[pl.ds(start, 8, stride=LEV * ROWS), :] = total[half]
        return carry

    lax.fori_loop(0, ROWS * LEV, tracer_cell, 0)


def advect(tracers, low, high, both, first, second, winds):
    return pl.pallas_call(
        advect_kernel,
        out_shape=jax.ShapeDtypeStruct((NTR * LEV * ROWS, COLS), jnp.float32),
        scratch_shapes=[
            pltpu.VMEM((WROWS, 3, L_TAPS, W_TAPS, LEV, COLS), jnp.float32),
            pltpu.VMEM((TROWS, LEV * 2, T_TAPS, 8, COLS), jnp.float32),
            pltpu.VMEM((ROWS, SPREADS, LEV, COLS), jnp.float32),
        ],
        compiler_params=params(),
    )(tracers, low, high, both, first, second, winds)


def combine_kernel(arrived_ref, moved_ref, out_ref, *totals):
    step = pl.program_id(0)
    rows = (arrived_ref.shape[1] - MARK_ROWS) // CAP

    @pl.when(step == 0)
    def _():
        for total in totals:
            total[...] = jnp.zeros(total.shape, jnp.float32)

    blocks = []
    for which in range(SOURCE_STEP):
        marks = arrived_ref[which, CAP * rows : CAP * rows + MARK_ROWS, :]
        marks = marks.astype(jnp.float32).astype(jnp.int32)
        blocks += [marks[rank, 0] for rank in range(CAP)]
    for which in range(SOURCE_STEP):
        for rank in range(CAP):
            total = totals[(which * CAP + rank) % SUMS]
            at = pl.ds(pl.multiple_of(blocks[which * CAP + rank] * rows, rows), rows)
            piece = arrived_ref[which, rank * rows : (rank + 1) * rows, :]
            total[at, :] = total[at, :] + piece.astype(jnp.float32)

    @pl.when(step == pl.num_programs(0) - 1)
    def _():
        for row in range(rows):
            at = row * ROWS
            picked = moved_ref[at : at + ROWS, :]
            for total in totals:
                picked = picked + total[pl.ds(row, BLK_DEV, stride=rows), :]
            out_ref[at : at + ROWS, :] = picked


def combine(arrived, moved):
    sources, deep, cols = arrived.shape
    rows = (deep - MARK_ROWS) // CAP
    return pl.pallas_call(
        combine_kernel,
        grid=(sources // SOURCE_STEP,),
        in_specs=[
            pl.BlockSpec((SOURCE_STEP, deep, cols), lambda i: (i, 0, 0)),
            pl.BlockSpec(moved.shape, lambda i: (0, 0)),
        ],
        out_specs=pl.BlockSpec(moved.shape, lambda i: (0, 0)),
        scratch_shapes=[pltpu.VMEM(((BLK_DEV + 1) * rows, cols), jnp.float32)] * SUMS,
        out_shape=jax.ShapeDtypeStruct(moved.shape, jnp.float32),
        compiler_params=params("arbitrary"),
    )(arrived, moved)


def halo_advect(tracers, winds, left, right, depart_first, depart_second):
    lat_count = lax.axis_size("lat")
    top, bottom, both = edge_rows(tracers, winds, left, right)
    up = [(i, i + 1) for i in range(lat_count - 1)]
    low = lax.ppermute(bottom, "lat", up)
    high = lax.ppermute(top, "lat", [(b, a) for a, b in up])
    return advect(tracers, low, high, both, depart_first, depart_second, winds)


def side_columns(tracers, winds):
    lon_count = lax.axis_size("lon")
    edge = edge_cols(tracers, winds)
    around = [(i, (i + 1) % lon_count) for i in range(lon_count)]
    left = lax.ppermute(edge, "lon", around)
    right = lax.ppermute(edge, "lon", [(b, a) for a, b in around])
    return left, right


def body(
    tracers, winds, depart_first, depart_second, fluxes, remap_weights, target_device, target_block
):
    shape = tracers.shape
    devices = lax.axis_size("lat") * lax.axis_size("lon")
    tracers, winds, depart_first, depart_second = (
        field.reshape(-1, COLS) for field in (tracers, winds, depart_first, depart_second)
    )
    left, right = side_columns(tracers, winds)
    chunks = remap(fluxes, remap_weights, target_device, target_block, devices)
    chunks, left, right = lax.optimization_barrier((chunks, left, right))
    arrived = lax.all_to_all(chunks, ("lat", "lon"), split_axis=0, concat_axis=0, tiled=True)
    moved = halo_advect(tracers, winds, left, right, depart_first, depart_second)
    return combine(arrived, moved).reshape(shape)


def solution(mesh):
    in_specs = (
        P(None, None, "lat", "lon"),
        P(None, None, "lat", "lon"),
        P(None, None, "lat", "lon"),
        P(None, None, "lat", "lon"),
        P(("lat", "lon"), None, None),
        P(("lat", "lon"), None, None, None),
        P(("lat", "lon"), None),
        P(("lat", "lon"), None),
    )
    out_specs = P(None, None, "lat", "lon")
    return jax.shard_map(body, mesh=mesh, in_specs=in_specs, out_specs=out_specs, check_vma=False)
```

```python
import functools

import jax
import jax.numpy as jnp
from jax import lax
from jax.experimental import pallas as pl
from jax.experimental.pallas import tpu as pltpu
from jax.sharding import PartitionSpec as P

NTR = 16
LEV = 8
CAP = 2
BLK_DEV = 16
ROWS = 16
COLS = 128
WIDE = 4
NEAR = 3
WROWS = ROWS + 2 * WIDE
TROWS = ROWS + 2 * NEAR
EDGE = 2 * WIDE
PER_GROUP = COLS // EDGE
TILE_STEP = 2
SOURCE_STEP = 8
SUMS = 2
MARK_ROWS = 8
OUT_PARTS = 4
VMEM_LIMIT = 60 * 1024 * 1024


def params(*semantics):
    return pltpu.CompilerParams(
        dimension_semantics=semantics or None, vmem_limit_bytes=VMEM_LIMIT
    )


def remap_kernel(
    first, tiles, final, device_ref, block_ref, flux_hbm, weight_hbm, *refs
):
    out_hbm, flux_buf, weight_buf, held, marks, sent, flux_sems, weight_sems, out_sem, mark_sem, counts = refs[-11:]
    links, rows = weight_hbm.shape[1], flux_hbm.shape[1]
    groups = tiles // TILE_STEP

    def loads(group):
        at = pl.ds(group * TILE_STEP, TILE_STEP)
        source = pl.ds(first + group * TILE_STEP, TILE_STEP)
        return (
            pltpu.make_async_copy(flux_hbm.at[source], flux_buf.at[at], flux_sems.at[group]),
            pltpu.make_async_copy(weight_hbm.at[source], weight_buf.at[at], weight_sems.at[group]),
        )

    for group in range(groups):
        for load in loads(group):
            load.start()

    def clear(i, carry):
        counts[i] = 0
        return carry

    lax.fori_loop(0, counts.shape[0], clear, 0, unroll=8)
    if final:
        marks[...] = jnp.full(marks.shape, BLK_DEV, jnp.float32)

    def place(tile, link):
        owner = device_ref[link, tile]
        rank = counts[owner]
        counts[owner] = rank + 1
        if final:
            value = block_ref[link, tile].astype(jnp.float32)
            marks[owner, pl.ds(rank, 1), :] = jnp.full((1, COLS), value, jnp.float32)
        return owner, pl.ds(pl.multiple_of(rank * rows, rows), rows)

    def earlier(tile, carry):
        for link in range(links):
            place(tile, link)
        return carry

    lax.fori_loop(0, first, earlier, 0)

    def work(group, carry):
        for load in loads(group):
            load.wait()
        for part in range(TILE_STEP):
            at = group * TILE_STEP + part
            flux = flux_buf[at]
            for pair in range(links // 2):
                both = jnp.concatenate(
                    [weight_buf[at, 2 * pair], weight_buf[at, 2 * pair + 1]], axis=1
                )
                made = jnp.dot(flux, both, preferred_element_type=jnp.float32)
                made = made.astype(jnp.bfloat16)
                for side in range(2):
                    into = pl.ds(side * rows, rows)
                    held[at * (links // 2) + pair, into] = made[:, side * COLS : (side + 1) * COLS]
        for part in range(TILE_STEP):
            at = group * TILE_STEP + part
            for link in range(links):
                owner, into = place(first + at, link)
                source = held.at[at * (links // 2) + link // 2, pl.ds(link % 2 * rows, rows)]
                pltpu.make_async_copy(source, out_hbm.at[owner, into], out_sem).start()
        return carry

    lax.fori_loop(0, groups, work, 0)
    if final:
        sent[...] = marks[...].astype(jnp.bfloat16)
        last = pltpu.make_async_copy(
            sent, out_hbm.at[:, pl.ds(CAP * rows, MARK_ROWS)], mark_sem
        )
        last.start()
        last.wait()
    everything = out_hbm.at[pl.ds(0, tiles * links // 2), pl.ds(0, 2 * rows)]
    pltpu.make_async_copy(held, everything, out_sem).wait()


def remap(fluxes, remap_weights, target_device, target_block, devices, first, tiles, chunks=None):
    rows, cells = fluxes.shape[1:]
    links, cols = remap_weights.shape[1], remap_weights.shape[3]
    final = chunks is not None
    anywhere = pl.BlockSpec(memory_space=pl.ANY)
    inputs = (target_device.T, target_block.T, fluxes, remap_weights) + ((chunks,) if final else ())
    groups = tiles // TILE_STEP
    return pl.pallas_call(
        functools.partial(remap_kernel, first, tiles, final),
        in_specs=[pl.BlockSpec(memory_space=pltpu.SMEM)] * 2 + [anywhere] * (3 if final else 2),
        out_specs=anywhere,
        scratch_shapes=[
            pltpu.VMEM((tiles, rows, cells), jnp.bfloat16),
            pltpu.VMEM((tiles, links, cells, cols), jnp.bfloat16),
            pltpu.VMEM((tiles * links // 2, 2 * rows, cols), jnp.bfloat16),
            pltpu.VMEM((devices, MARK_ROWS, cols), jnp.float32),
            pltpu.VMEM((devices, MARK_ROWS, cols), jnp.bfloat16),
            pltpu.SemaphoreType.DMA((groups,)),
            pltpu.SemaphoreType.DMA((groups,)),
            pltpu.SemaphoreType.DMA,
            pltpu.SemaphoreType.DMA,
            pltpu.SMEM((devices,), jnp.int32),
        ],
        out_shape=jax.ShapeDtypeStruct((devices, CAP * rows + MARK_ROWS, cols), jnp.bfloat16),
        input_output_aliases={4: 0} if final else {},
        compiler_params=params(),
    )(*inputs)


def wind_piece(winds_ref, row, comp):
    return winds_ref[pl.ds(comp * LEV * ROWS + row, LEV, stride=ROWS), :]


def tracer_piece(tracers_ref, row, level, half):
    start = half * 8 * LEV * ROWS + level * ROWS + row
    return tracers_ref[pl.ds(start, 8, stride=LEV * ROWS), :]


WIND_MSG = WIDE * 3 * LEV
TRACER_MSG = NEAR * LEV * NTR
TRACER_EDGE = WIND_MSG + TRACER_MSG
WIND_EDGE = TRACER_EDGE + NEAR * 8
MSG = WIND_EDGE + 3 * 8
EDGE_ROWS = (ROWS + 3) * 8


def edge_cols_kernel(tracers_ref, winds_ref, edge_ref):
    group_of = lax.broadcasted_iota(jnp.int32, (8, COLS), 1) // EDGE

    def packed(pieces):
        held = jnp.zeros((8, COLS), jnp.float32)
        for spot, piece in enumerate(pieces):
            turned = pltpu.roll(piece, (WIDE + EDGE * spot) % COLS, 1)
            held = jnp.where(group_of == spot, turned, held)
        return held

    def tracer_row(row, carry):
        pieces = [tracer_piece(tracers_ref, row, spot // 2, spot % 2) for spot in range(PER_GROUP)]
        edge_ref[pl.ds(pl.multiple_of(row * 8, 8), 8), :] = packed(pieces)
        return carry

    lax.fori_loop(0, ROWS, tracer_row, 0)
    for comp in range(3):
        at = (ROWS + comp) * 8
        edge_ref[at : at + 8, :] = packed([wind_piece(winds_ref, row, comp) for row in range(ROWS)])


def edge_cols(tracers, winds):
    return pl.pallas_call(
        edge_cols_kernel,
        out_shape=jax.ShapeDtypeStruct((EDGE_ROWS, COLS), jnp.float32),
        compiler_params=params(),
    )(tracers, winds)


def edge_rows_kernel(tracers_ref, winds_ref, left_ref, right_ref, top_ref, bottom_ref, both_ref):
    lane = lax.broadcasted_iota(jnp.int32, (EDGE_ROWS, COLS), 1)
    both_ref[...] = jnp.where(lax.rem(lane, EDGE) < WIDE, left_ref[...], right_ref[...])
    for target, wind_from, tracer_from in (
        (top_ref, 0, 0),
        (bottom_ref, ROWS - WIDE, ROWS - NEAR),
    ):
        for row in range(WIDE):
            for comp in range(3):
                at = (row * 3 + comp) * LEV
                target[at : at + LEV, :] = wind_piece(winds_ref, wind_from + row, comp)
        for row in range(NEAR):
            for level in range(LEV):
                for half in range(2):
                    at = WIND_MSG + (row * LEV + level) * NTR + half * 8
                    target[at : at + 8, :] = tracer_piece(
                        tracers_ref, tracer_from + row, level, half
                    )
        target[TRACER_EDGE:WIND_EDGE, :] = both_ref[tracer_from * 8 : (tracer_from + NEAR) * 8, :]
        target[WIND_EDGE:MSG, :] = both_ref[ROWS * 8 : EDGE_ROWS, :]


def edge_rows(tracers, winds, left, right):
    shape = jax.ShapeDtypeStruct((MSG, COLS), jnp.float32)
    return pl.pallas_call(
        edge_rows_kernel,
        out_shape=[shape, shape, jax.ShapeDtypeStruct((EDGE_ROWS, COLS), jnp.float32)],
        compiler_params=params(),
    )(tracers, winds, left, right)


def cubic_weights(frac):
    first = -frac * (frac - 1.0) * (frac - 2.0) / 6.0
    second = (frac + 1.0) * (frac - 1.0) * (frac - 2.0) / 2.0
    third = -(frac + 1.0) * frac * (frac - 2.0) / 2.0
    fourth = (frac + 1.0) * frac * (frac - 1.0) / 6.0
    return (first, second, third, fourth)


def spread_weights(offset, frac, lowest, highest):
    stencil = cubic_weights(frac)
    hits = {value: offset == value for value in range(lowest, highest + 1)}
    spread = []
    for target in range(lowest - 1, highest + 3):
        weight = jnp.zeros(frac.shape, jnp.float32)
        for step in range(4):
            value = target - step + 1
            if value in hits:
                weight = weight + jnp.where(hits[value], stencil[step], 0.0)
        spread.append(weight)
    return spread


def column_shifts(main, edge, reach):
    lane = lax.broadcasted_iota(jnp.int32, main.shape, 1)
    shifted = []
    for step in range(-reach, reach + 1):
        if step == 0:
            shifted.append(main)
            continue
        inside = lane < COLS - step if step > 0 else lane >= -step
        turn = (COLS - step) % COLS
        shifted.append(jnp.where(inside, pltpu.roll(main, turn, 1), pltpu.roll(edge, turn, 1)))
    return shifted


def level_shift(value, step):
    if step == 0:
        return value
    level = lax.broadcasted_iota(jnp.int32, value.shape, 0)
    turned = pltpu.roll(value, (LEV - step) % LEV, 0)
    if step > 0:
        end = jnp.broadcast_to(value[LEV - 1 : LEV, :], value.shape)
        return jnp.where(level >= LEV - step, end, turned)
    end = jnp.broadcast_to(value[0:1, :], value.shape)
    return jnp.where(level < -step, end, turned)


W_TAPS = 9
T_TAPS = 7
L_TAPS = 5
SPREADS = L_TAPS + 2 * T_TAPS


def advect_kernel(
    tracers_ref, low_ref, high_ref, both_ref, first_ref, second_ref, winds_ref, out_ref,
    wind_taps, tracer_taps, spread_ref,
):
    def edge_piece(ref, at, spot):
        return pltpu.roll(ref[pl.ds(at, 8), :], (COLS - WIDE - EDGE * spot) % COLS, 1)

    for comp in range(3):
        for row in range(WROWS):
            if row < WIDE:
                at = (row * 3 + comp) * LEV
                main = low_ref[at : at + LEV, :]
                edge = edge_piece(low_ref, WIND_EDGE + comp * 8, ROWS - WIDE + row)
            elif row < WIDE + ROWS:
                main = wind_piece(winds_ref, row - WIDE, comp)
                edge = edge_piece(both_ref, (ROWS + comp) * 8, row - WIDE)
            else:
                at = ((row - WIDE - ROWS) * 3 + comp) * LEV
                main = high_ref[at : at + LEV, :]
                edge = edge_piece(high_ref, WIND_EDGE + comp * 8, row - WIDE - ROWS)
            shifted = column_shifts(main, edge, WIDE)
            for side in range(W_TAPS):
                for above in range(L_TAPS):
                    wind_taps[row, comp, above, side] = level_shift(shifted[side], above - 2)

    def wind_row(row, carry):
        def component(ref, comp):
            return ref[pl.ds(comp * LEV * ROWS + row, LEV, stride=ROWS), :]

        wind = [component(winds_ref, comp) for comp in range(3)]
        first = [component(first_ref, comp) for comp in range(3)]
        frac = [
            jnp.clip(-wind[comp] - first[comp].astype(jnp.float32), 0.0, 1.0)
            for comp in range(3)
        ]
        level_w = spread_weights(first[0], frac[0], -1, 0)
        row_w = spread_weights(first[1], frac[1], -3, 2)
        col_w = spread_weights(first[2], frac[2], -3, 2)
        total = [jnp.zeros((LEV, COLS), jnp.float32) for _ in range(3)]
        for above in range(L_TAPS):
            part = [jnp.zeros((LEV, COLS), jnp.float32) for _ in range(3)]
            for across in range(W_TAPS):
                for comp in range(3):
                    inner = col_w[0] * wind_taps[row + across, comp, above, 0]
                    for side in range(1, W_TAPS):
                        inner = inner + col_w[side] * wind_taps[row + across, comp, above, side]
                    part[comp] = part[comp] + row_w[across] * inner
            for comp in range(3):
                total[comp] = total[comp] + level_w[above] * part[comp]
        second = [component(second_ref, comp) for comp in range(3)]
        frac = [
            jnp.clip(
                -(wind[comp] + total[comp]) * 0.5 - second[comp].astype(jnp.float32), 0.0, 1.0
            )
            for comp in range(3)
        ]
        weights = spread_weights(second[0], frac[0], -1, 0)
        weights += spread_weights(second[1], frac[1], -2, 1)
        weights += spread_weights(second[2], frac[2], -2, 1)
        for which in range(SPREADS):
            spread_ref[row, which] = weights[which]
        return carry

    lax.fori_loop(0, ROWS, wind_row, 0)

    def own_shifts(row, carry):
        for spot in range(PER_GROUP):
            main = tracer_piece(tracers_ref, row, spot // 2, spot % 2)
            edge = edge_piece(both_ref, pl.multiple_of(row * 8, 8), spot)
            shifted = column_shifts(main, edge, NEAR)
            for side in range(T_TAPS):
                tracer_taps[row + NEAR, spot, side] = shifted[side]
        return carry

    lax.fori_loop(0, ROWS, own_shifts, 0)
    for ref, onto in ((low_ref, 0), (high_ref, NEAR + ROWS)):

        def halo_shifts(row, carry, ref=ref, onto=onto):
            for spot in range(PER_GROUP):
                at = pl.multiple_of(WIND_MSG + row * LEV * NTR + spot * 8, 8)
                edge = edge_piece(ref, pl.multiple_of(TRACER_EDGE + row * 8, 8), spot)
                shifted = column_shifts(ref[pl.ds(at, 8), :], edge, NEAR)
                for side in range(T_TAPS):
                    tracer_taps[row + onto, spot, side] = shifted[side]
            return carry

        lax.fori_loop(0, NEAR, halo_shifts, 0)

    def tracer_cell(cell, carry):
        row, level = cell // LEV, lax.rem(cell, LEV)

        def weight(which):
            return jnp.broadcast_to(spread_ref[row, which, pl.ds(level, 1), :], (8, COLS))

        row_w = [weight(L_TAPS + which) for which in range(T_TAPS)]
        col_w = [weight(L_TAPS + T_TAPS + which) for which in range(T_TAPS)]
        total = [jnp.zeros((8, COLS), jnp.float32) for _ in range(2)]
        for above in range(L_TAPS):
            source = jnp.clip(level + above - 2, 0, LEV - 1)
            level_w = weight(above)
            part = [jnp.zeros((8, COLS), jnp.float32) for _ in range(2)]
            for across in range(T_TAPS):
                for half in range(2):
                    taps = tracer_taps.at[row + across, source * 2 + half]
                    inner = col_w[0] * taps[0]
                    for side in range(1, T_TAPS):
                        inner = inner + col_w[side] * taps[side]
                    part[half] = part[half] + row_w[across] * inner
            for half in range(2):
                total[half] = total[half] + level_w * part[half]
        for half in range(2):
            start = half * 8 * LEV * ROWS + level * ROWS + row
            out_ref[pl.ds(start, 8, stride=LEV * ROWS), :] = total[half]
        return carry

    lax.fori_loop(0, ROWS * LEV, tracer_cell, 0)


def advect(tracers, low, high, both, first, second, winds):
    return pl.pallas_call(
        advect_kernel,
        out_shape=jax.ShapeDtypeStruct((NTR * LEV * ROWS, COLS), jnp.float32),
        scratch_shapes=[
            pltpu.VMEM((WROWS, 3, L_TAPS, W_TAPS, LEV, COLS), jnp.float32),
            pltpu.VMEM((TROWS, LEV * 2, T_TAPS, 8, COLS), jnp.float32),
            pltpu.VMEM((ROWS, SPREADS, LEV, COLS), jnp.float32),
        ],
        compiler_params=params(),
    )(tracers, low, high, both, first, second, winds)


def combine_kernel(
    arrived_hbm, moved_hbm, out_hbm, arrived_buf, moved_buf, out_buf, arrived_sems, moved_sem, out_sems, *totals
):
    sources, deep, cols = arrived_hbm.shape
    rows = (deep - MARK_ROWS) // CAP
    groups = sources // SOURCE_STEP

    def load(group):
        at = pl.ds(group * SOURCE_STEP, SOURCE_STEP)
        return pltpu.make_async_copy(arrived_hbm.at[at], arrived_buf.at[at], arrived_sems.at[group])

    for group in range(groups):
        load(group).start()
    moved_load = pltpu.make_async_copy(moved_hbm, moved_buf, moved_sem)
    moved_load.start()
    for total in totals:
        total[...] = jnp.zeros(total.shape, jnp.float32)

    def add(group, carry):
        load(group).wait()
        blocks = []
        for which in range(SOURCE_STEP):
            marks = arrived_buf[group * SOURCE_STEP + which, CAP * rows : deep, :]
            marks = marks.astype(jnp.float32).astype(jnp.int32)
            blocks += [marks[rank, 0] for rank in range(CAP)]
        for which in range(SOURCE_STEP):
            for rank in range(CAP):
                item = which * CAP + rank
                total = totals[item % SUMS]
                at = pl.ds(pl.multiple_of(blocks[item] * rows, rows), rows)
                piece = arrived_buf[group * SOURCE_STEP + which, rank * rows : (rank + 1) * rows, :]
                total[at, :] = total[at, :] + piece.astype(jnp.float32)
        return carry

    lax.fori_loop(0, groups, add, 0)
    moved_load.wait()
    share = rows // OUT_PARTS
    stores = []
    for part in range(OUT_PARTS):
        for row in range(part * share, (part + 1) * share):
            at = row * ROWS
            picked = moved_buf[at : at + ROWS, :]
            for total in totals:
                picked = picked + total[pl.ds(row, BLK_DEV, stride=rows), :]
            out_buf[at : at + ROWS, :] = picked
        at = pl.ds(part * share * ROWS, share * ROWS)
        stores.append(pltpu.make_async_copy(out_buf.at[at], out_hbm.at[at], out_sems.at[part]))
        stores[-1].start()
    for store in stores:
        store.wait()


def combine(arrived, moved):
    sources, deep, cols = arrived.shape
    rows = (deep - MARK_ROWS) // CAP
    anywhere = pl.BlockSpec(memory_space=pl.ANY)
    return pl.pallas_call(
        combine_kernel,
        in_specs=[anywhere] * 2,
        out_specs=anywhere,
        scratch_shapes=[
            pltpu.VMEM(arrived.shape, arrived.dtype),
            pltpu.VMEM(moved.shape, moved.dtype),
            pltpu.VMEM(moved.shape, moved.dtype),
            pltpu.SemaphoreType.DMA((sources // SOURCE_STEP,)),
            pltpu.SemaphoreType.DMA,
            pltpu.SemaphoreType.DMA((OUT_PARTS,)),
        ]
        + [pltpu.VMEM(((BLK_DEV + 1) * rows, cols), jnp.float32)] * SUMS,
        out_shape=jax.ShapeDtypeStruct(moved.shape, jnp.float32),
        compiler_params=params(),
    )(arrived, moved)


def side_columns(tracers, winds):
    lon_count = lax.axis_size("lon")
    edge = edge_cols(tracers, winds)
    around = [(i, (i + 1) % lon_count) for i in range(lon_count)]
    left = lax.ppermute(edge, "lon", around)
    right = lax.ppermute(edge, "lon", [(b, a) for a, b in around])
    return left, right


def outer_rows(top, bottom):
    lat_count = lax.axis_size("lat")
    up = [(i, i + 1) for i in range(lat_count - 1)]
    low = lax.ppermute(bottom, "lat", up)
    high = lax.ppermute(top, "lat", [(b, a) for a, b in up])
    return low, high


def body(
    tracers, winds, depart_first, depart_second, fluxes, remap_weights, target_device, target_block
):
    shape = tracers.shape
    devices = lax.axis_size("lat") * lax.axis_size("lon")
    tracers, winds, depart_first, depart_second = (
        field.reshape(-1, COLS) for field in (tracers, winds, depart_first, depart_second)
    )
    tiles = fluxes.shape[0]
    half = tiles // 2
    emission = (fluxes, remap_weights, target_device, target_block, devices)
    left, right = side_columns(tracers, winds)
    chunks = remap(*emission, 0, half)
    chunks, left, right = lax.optimization_barrier((chunks, left, right))
    top, bottom, both = edge_rows(tracers, winds, left, right)
    chunks, top, bottom = lax.optimization_barrier((chunks, top, bottom))
    low, high = outer_rows(top, bottom)
    chunks = remap(*emission, half, tiles - half, chunks)
    chunks, low, high = lax.optimization_barrier((chunks, low, high))
    arrived = lax.all_to_all(chunks, ("lat", "lon"), split_axis=0, concat_axis=0, tiled=True)
    moved = advect(tracers, low, high, both, depart_first, depart_second, winds)
    return combine(arrived, moved).reshape(shape)


def solution(mesh):
    in_specs = (
        P(None, None, "lat", "lon"),
        P(None, None, "lat", "lon"),
        P(None, None, "lat", "lon"),
        P(None, None, "lat", "lon"),
        P(("lat", "lon"), None, None),
        P(("lat", "lon"), None, None, None),
        P(("lat", "lon"), None),
        P(("lat", "lon"), None),
    )
    out_specs = P(None, None, "lat", "lon")
    return jax.shard_map(body, mesh=mesh, in_specs=in_specs, out_specs=out_specs, check_vma=False)
```

```python
import functools

import jax
import jax.numpy as jnp
from jax import lax
from jax.experimental import pallas as pl
from jax.experimental.pallas import tpu as pltpu
from jax.sharding import PartitionSpec as P

NTR = 16
LEV = 8
CAP = 2
BLK_DEV = 16
ROWS = 16
COLS = 128
WIDE = 4
NEAR = 3
WROWS = ROWS + 2 * WIDE
TROWS = ROWS + 2 * NEAR
EDGE = 2 * WIDE
PER_GROUP = COLS // EDGE
TILE_STEP = 4
SOURCE_STEP = 8
SUMS = 2
MARK_ROWS = 8
OUT_PARTS = 4


def params(mebibytes):
    return pltpu.CompilerParams(vmem_limit_bytes=mebibytes * 1024 * 1024)


def remap_kernel(
    device_ref, block_ref, flux_hbm, weight_hbm, out_hbm, flux_buf, weight_buf, held, marks, sent,
    flux_sems, weight_sems, out_sem, mark_sem, counts,
):
    tiles = flux_hbm.shape[0]
    links, rows = weight_hbm.shape[1], flux_hbm.shape[1]
    groups = tiles // TILE_STEP

    def loads(group):
        at = pl.ds(group * TILE_STEP, TILE_STEP)
        return (
            pltpu.make_async_copy(flux_hbm.at[at], flux_buf.at[at], flux_sems.at[group]),
            pltpu.make_async_copy(weight_hbm.at[at], weight_buf.at[at], weight_sems.at[group]),
        )

    for group in range(groups):
        for load in loads(group):
            load.start()

    def clear(i, carry):
        counts[i] = 0
        return carry

    lax.fori_loop(0, counts.shape[0], clear, 0, unroll=8)
    marks[...] = jnp.full(marks.shape, BLK_DEV, jnp.float32)

    def place(tile, link):
        owner = device_ref[link, tile]
        rank = counts[owner]
        counts[owner] = rank + 1
        value = block_ref[link, tile].astype(jnp.float32)
        marks[owner, pl.ds(rank, 1), :] = jnp.full((1, COLS), value, jnp.float32)
        return owner, pl.ds(pl.multiple_of(rank * rows, rows), rows)

    def work(group, carry):
        for load in loads(group):
            load.wait()
        for part in range(TILE_STEP):
            at = group * TILE_STEP + part
            flux = flux_buf[at]
            for pair in range(links // 2):
                both = jnp.concatenate(
                    [weight_buf[at, 2 * pair], weight_buf[at, 2 * pair + 1]], axis=1
                )
                made = jnp.dot(flux, both, preferred_element_type=jnp.float32)
                made = made.astype(jnp.bfloat16)
                for side in range(2):
                    into = pl.ds(side * rows, rows)
                    held[at * (links // 2) + pair, into] = made[:, side * COLS : (side + 1) * COLS]
        for part in range(TILE_STEP):
            at = group * TILE_STEP + part
            for link in range(links):
                owner, into = place(at, link)
                source = held.at[at * (links // 2) + link // 2, pl.ds(link % 2 * rows, rows)]
                pltpu.make_async_copy(source, out_hbm.at[owner, into], out_sem).start()
        return carry

    lax.fori_loop(0, groups, work, 0)
    sent[...] = marks[...].astype(jnp.bfloat16)
    last = pltpu.make_async_copy(sent, out_hbm.at[:, pl.ds(CAP * rows, MARK_ROWS)], mark_sem)
    last.start()
    last.wait()
    everything = out_hbm.at[pl.ds(0, tiles * links // 2), pl.ds(0, 2 * rows)]
    pltpu.make_async_copy(held, everything, out_sem).wait()


def remap(fluxes, remap_weights, target_device, target_block, devices):
    tiles, rows, cells = fluxes.shape
    links, cols = remap_weights.shape[1], remap_weights.shape[3]
    anywhere = pl.BlockSpec(memory_space=pl.ANY)
    groups = tiles // TILE_STEP
    return pl.pallas_call(
        remap_kernel,
        in_specs=[pl.BlockSpec(memory_space=pltpu.SMEM)] * 2 + [anywhere] * 2,
        out_specs=anywhere,
        scratch_shapes=[
            pltpu.VMEM(fluxes.shape, jnp.bfloat16),
            pltpu.VMEM(remap_weights.shape, jnp.bfloat16),
            pltpu.VMEM((tiles * links // 2, 2 * rows, cols), jnp.bfloat16),
            pltpu.VMEM((devices, MARK_ROWS, cols), jnp.float32),
            pltpu.VMEM((devices, MARK_ROWS, cols), jnp.bfloat16),
            pltpu.SemaphoreType.DMA((groups,)),
            pltpu.SemaphoreType.DMA((groups,)),
            pltpu.SemaphoreType.DMA,
            pltpu.SemaphoreType.DMA,
            pltpu.SMEM((devices,), jnp.int32),
        ],
        out_shape=jax.ShapeDtypeStruct((devices, CAP * rows + MARK_ROWS, cols), jnp.bfloat16),
        compiler_params=params(60),
    )(target_device.T, target_block.T, fluxes, remap_weights)


def wind_piece(winds_ref, row, comp):
    return winds_ref[pl.ds(comp * LEV * ROWS + row, LEV, stride=ROWS), :]


def tracer_piece(tracers_ref, row, level, half):
    start = half * 8 * LEV * ROWS + level * ROWS + row
    return tracers_ref[pl.ds(start, 8, stride=LEV * ROWS), :]


WIND_MSG = WIDE * 3 * LEV
TRACER_MSG = NEAR * LEV * NTR
MSG = WIND_MSG + TRACER_MSG
EDGE_ROWS = (NTR + LEV) * 8
LOADS = 8


def pack_kernel(tracers_hbm, winds_hbm, edge_ref, top_ref, bottom_ref, tracers_ref, winds_ref, sems):
    share = NTR * LEV * ROWS // LOADS
    loads = [pltpu.make_async_copy(winds_hbm, winds_ref, sems.at[LOADS])]
    for part in range(LOADS):
        at = pl.ds(part * share, share)
        loads.append(pltpu.make_async_copy(tracers_hbm.at[at], tracers_ref.at[at], sems.at[part]))
    for load in loads:
        load.start()
    group_of = lax.broadcasted_iota(jnp.int32, (8, COLS), 1) // EDGE

    def packed(pieces):
        held = jnp.zeros((8, COLS), jnp.float32)
        for spot, piece in enumerate(pieces):
            turned = pltpu.roll(piece, (WIDE + EDGE * spot) % COLS, 1)
            held = jnp.where(group_of == spot, turned, held)
        return held

    loads[0].wait()
    for level in range(LEV):
        starts = [
            comp * LEV * ROWS + level * ROWS + half * 8 for comp in range(3) for half in range(2)
        ]
        at = (NTR + level) * 8
        edge_ref[at : at + 8, :] = packed([winds_ref[start : start + 8, :] for start in starts])
    for tracer in range(NTR):
        if tracer % (NTR // LOADS) == 0:
            loads[1 + tracer // (NTR // LOADS)].wait()
        starts = [tracer * LEV * ROWS + spot * 8 for spot in range(PER_GROUP)]
        at = tracer * 8
        edge_ref[at : at + 8, :] = packed([tracers_ref[start : start + 8, :] for start in starts])
    for target, wind_from, tracer_from in (
        (top_ref, 0, 0),
        (bottom_ref, ROWS - WIDE, ROWS - NEAR),
    ):
        for row in range(WIDE):
            for comp in range(3):
                at = (row * 3 + comp) * LEV
                target[at : at + LEV, :] = wind_piece(winds_ref, wind_from + row, comp)
        for row in range(NEAR):
            for level in range(LEV):
                for half in range(2):
                    at = WIND_MSG + (row * LEV + level) * NTR + half * 8
                    target[at : at + 8, :] = tracer_piece(
                        tracers_ref, tracer_from + row, level, half
                    )


def pack(tracers, winds):
    shapes = [jax.ShapeDtypeStruct((rows, COLS), jnp.float32) for rows in (EDGE_ROWS, MSG, MSG)]
    return pl.pallas_call(
        pack_kernel,
        in_specs=[pl.BlockSpec(memory_space=pl.ANY)] * 2,
        out_specs=[pl.BlockSpec(memory_space=pltpu.VMEM)] * 3,
        out_shape=shapes,
        scratch_shapes=[
            pltpu.VMEM(tracers.shape, jnp.float32),
            pltpu.VMEM(winds.shape, jnp.float32),
            pltpu.SemaphoreType.DMA((LOADS + 1,)),
        ],
        compiler_params=params(60),
    )(tracers, winds)


def cubic_weights(frac):
    first = -frac * (frac - 1.0) * (frac - 2.0) / 6.0
    second = (frac + 1.0) * (frac - 1.0) * (frac - 2.0) / 2.0
    third = -(frac + 1.0) * frac * (frac - 2.0) / 2.0
    fourth = (frac + 1.0) * frac * (frac - 1.0) / 6.0
    return (first, second, third, fourth)


def spread_weights(offset, frac, lowest, highest):
    stencil = cubic_weights(frac)
    hits = {value: offset == value for value in range(lowest, highest + 1)}
    spread = []
    for target in range(lowest - 1, highest + 3):
        weight = jnp.zeros(frac.shape, jnp.float32)
        for step in range(4):
            value = target - step + 1
            if value in hits:
                weight = weight + jnp.where(hits[value], stencil[step], 0.0)
        spread.append(weight)
    return spread


def column_shifts(main, edge, reach):
    lane = lax.broadcasted_iota(jnp.int32, main.shape, 1)
    shifted = []
    for step in range(-reach, reach + 1):
        if step == 0:
            shifted.append(main)
            continue
        inside = lane < COLS - step if step > 0 else lane >= -step
        turn = (COLS - step) % COLS
        shifted.append(jnp.where(inside, pltpu.roll(main, turn, 1), pltpu.roll(edge, turn, 1)))
    return shifted


def level_shift(value, step):
    if step == 0:
        return value
    level = lax.broadcasted_iota(jnp.int32, value.shape, 0)
    turned = pltpu.roll(value, (LEV - step) % LEV, 0)
    if step > 0:
        end = jnp.broadcast_to(value[LEV - 1 : LEV, :], value.shape)
        return jnp.where(level >= LEV - step, end, turned)
    end = jnp.broadcast_to(value[0:1, :], value.shape)
    return jnp.where(level < -step, end, turned)


W_TAPS = 9
T_TAPS = 7
L_TAPS = 5
SPREADS = L_TAPS + 2 * T_TAPS


def advect_kernel(
    tracers_ref, low_ref, high_ref, left_ref, right_ref, low_left_ref, low_right_ref,
    high_left_ref, high_right_ref, first_ref, second_ref, winds_ref, out_ref,
    own_edge, low_edge, high_edge, wind_taps, tracer_taps, spread_ref,
):
    lane = lax.broadcasted_iota(jnp.int32, (EDGE_ROWS, COLS), 1)
    from_left = lax.rem(lane, EDGE) < WIDE
    own_edge[...] = jnp.where(from_left, left_ref[...], right_ref[...])
    low_edge[...] = jnp.where(from_left, low_left_ref[...], low_right_ref[...])
    high_edge[...] = jnp.where(from_left, high_left_ref[...], high_right_ref[...])

    def edge_piece(ref, start, spot):
        return pltpu.roll(ref[pl.ds(start, 8, stride=8), :], (COLS - WIDE - EDGE * spot) % COLS, 1)

    def wind_edge(ref, row, comp):
        return edge_piece(ref, NTR * 8 + row % 8, comp * 2 + row // 8)

    for comp in range(3):
        for row in range(WROWS):
            if row < WIDE:
                at = (row * 3 + comp) * LEV
                main = low_ref[at : at + LEV, :]
                edge = wind_edge(low_edge, ROWS - WIDE + row, comp)
            elif row < WIDE + ROWS:
                main = wind_piece(winds_ref, row - WIDE, comp)
                edge = wind_edge(own_edge, row - WIDE, comp)
            else:
                at = ((row - WIDE - ROWS) * 3 + comp) * LEV
                main = high_ref[at : at + LEV, :]
                edge = wind_edge(high_edge, row - WIDE - ROWS, comp)
            shifted = column_shifts(main, edge, WIDE)
            for side in range(W_TAPS):
                for above in range(L_TAPS):
                    wind_taps[row, comp, above, side] = level_shift(shifted[side], above - 2)

    def wind_row(row, carry):
        def component(ref, comp):
            return ref[pl.ds(comp * LEV * ROWS + row, LEV, stride=ROWS), :]

        wind = [component(winds_ref, comp) for comp in range(3)]
        first = [component(first_ref, comp) for comp in range(3)]
        frac = [
            jnp.clip(-wind[comp] - first[comp].astype(jnp.float32), 0.0, 1.0)
            for comp in range(3)
        ]
        level_w = spread_weights(first[0], frac[0], -1, 0)
        row_w = spread_weights(first[1], frac[1], -3, 2)
        col_w = spread_weights(first[2], frac[2], -3, 2)
        total = [jnp.zeros((LEV, COLS), jnp.float32) for _ in range(3)]
        for above in range(L_TAPS):
            part = [jnp.zeros((LEV, COLS), jnp.float32) for _ in range(3)]
            for across in range(W_TAPS):
                for comp in range(3):
                    inner = col_w[0] * wind_taps[row + across, comp, above, 0]
                    for side in range(1, W_TAPS):
                        inner = inner + col_w[side] * wind_taps[row + across, comp, above, side]
                    part[comp] = part[comp] + row_w[across] * inner
            for comp in range(3):
                total[comp] = total[comp] + level_w[above] * part[comp]
        second = [component(second_ref, comp) for comp in range(3)]
        frac = [
            jnp.clip(
                -(wind[comp] + total[comp]) * 0.5 - second[comp].astype(jnp.float32), 0.0, 1.0
            )
            for comp in range(3)
        ]
        weights = spread_weights(second[0], frac[0], -1, 0)
        weights += spread_weights(second[1], frac[1], -2, 1)
        weights += spread_weights(second[2], frac[2], -2, 1)
        for which in range(SPREADS):
            spread_ref[row, which] = weights[which]
        return carry

    lax.fori_loop(0, ROWS, wind_row, 0)

    def keep_shifts(main_of, ref, onto, within, upper):
        for spot in range(PER_GROUP):
            level, half = spot // 2, spot % 2
            edge = edge_piece(ref, half * 64 + within, level * 2 + upper)
            shifted = column_shifts(main_of(level, half), edge, NEAR)
            for side in range(T_TAPS):
                tracer_taps[onto, spot, side] = shifted[side]

    for upper in range(2):

        def own_shifts(within, carry, upper=upper):
            row = upper * 8 + within
            main_of = functools.partial(tracer_piece, tracers_ref, row)
            keep_shifts(main_of, own_edge, row + NEAR, within, upper)
            return carry

        lax.fori_loop(0, 8, own_shifts, 0)
    for ref, edges, onto, upper in ((low_ref, low_edge, 0, 1), (high_ref, high_edge, NEAR + ROWS, 0)):

        def halo_shifts(row, carry, ref=ref, edges=edges, onto=onto, upper=upper):
            def main_of(level, half):
                at = WIND_MSG + row * LEV * NTR + level * NTR + half * 8
                return ref[pl.ds(pl.multiple_of(at, 8), 8), :]

            within = row + (8 - NEAR if upper else 0)
            keep_shifts(main_of, edges, row + onto, within, upper)
            return carry

        lax.fori_loop(0, NEAR, halo_shifts, 0)

    def tracer_cell(cell, carry):
        row, level = cell // LEV, lax.rem(cell, LEV)

        def weight(which):
            return jnp.broadcast_to(spread_ref[row, which, pl.ds(level, 1), :], (8, COLS))

        row_w = [weight(L_TAPS + which) for which in range(T_TAPS)]
        col_w = [weight(L_TAPS + T_TAPS + which) for which in range(T_TAPS)]
        total = [jnp.zeros((8, COLS), jnp.float32) for _ in range(2)]
        for above in range(L_TAPS):
            source = jnp.clip(level + above - 2, 0, LEV - 1)
            level_w = weight(above)
            part = [jnp.zeros((8, COLS), jnp.float32) for _ in range(2)]
            for across in range(T_TAPS):
                for half in range(2):
                    taps = tracer_taps.at[row + across, source * 2 + half]
                    inner = col_w[0] * taps[0]
                    for side in range(1, T_TAPS):
                        inner = inner + col_w[side] * taps[side]
                    part[half] = part[half] + row_w[across] * inner
            for half in range(2):
                total[half] = total[half] + level_w * part[half]
        for half in range(2):
            start = half * 8 * LEV * ROWS + level * ROWS + row
            out_ref[pl.ds(start, 8, stride=LEV * ROWS), :] = total[half]
        return carry

    lax.fori_loop(0, ROWS * LEV, tracer_cell, 0)


def advect(tracers, low, high, edges, first, second, winds):
    return pl.pallas_call(
        advect_kernel,
        in_specs=[pl.BlockSpec(memory_space=pltpu.VMEM)] * (6 + len(edges)),
        out_specs=pl.BlockSpec(memory_space=pltpu.VMEM),
        out_shape=jax.ShapeDtypeStruct((NTR * LEV * ROWS, COLS), jnp.float32),
        scratch_shapes=[pltpu.VMEM((EDGE_ROWS, COLS), jnp.float32)] * 3
        + [
            pltpu.VMEM((WROWS, 3, L_TAPS, W_TAPS, LEV, COLS), jnp.float32),
            pltpu.VMEM((TROWS, LEV * 2, T_TAPS, 8, COLS), jnp.float32),
            pltpu.VMEM((ROWS, SPREADS, LEV, COLS), jnp.float32),
        ],
        compiler_params=params(60),
    )(tracers, low, high, *edges, first, second, winds)


def combine_kernel(
    arrived_hbm, moved_hbm, out_hbm, arrived_buf, moved_buf, out_buf, arrived_sems, moved_sem, out_sems, *totals
):
    sources, deep, cols = arrived_hbm.shape
    rows = (deep - MARK_ROWS) // CAP
    groups = sources // SOURCE_STEP

    def load(group):
        at = pl.ds(group * SOURCE_STEP, SOURCE_STEP)
        return pltpu.make_async_copy(arrived_hbm.at[at], arrived_buf.at[at], arrived_sems.at[group])

    for group in range(groups):
        load(group).start()
    moved_load = pltpu.make_async_copy(moved_hbm, moved_buf, moved_sem)
    moved_load.start()
    for total in totals:
        total[...] = jnp.zeros(total.shape, jnp.float32)

    def add(group, carry):
        load(group).wait()
        blocks = []
        for which in range(SOURCE_STEP):
            marks = arrived_buf[group * SOURCE_STEP + which, CAP * rows : deep, :]
            marks = marks.astype(jnp.float32).astype(jnp.int32)
            blocks += [marks[rank, 0] for rank in range(CAP)]
        for which in range(SOURCE_STEP):
            for rank in range(CAP):
                item = which * CAP + rank
                total = totals[item % SUMS]
                at = pl.ds(pl.multiple_of(blocks[item] * rows, rows), rows)
                piece = arrived_buf[group * SOURCE_STEP + which, rank * rows : (rank + 1) * rows, :]
                total[at, :] = total[at, :] + piece.astype(jnp.float32)
        return carry

    lax.fori_loop(0, groups, add, 0)
    moved_load.wait()
    share = rows // OUT_PARTS
    stores = []
    for part in range(OUT_PARTS):
        for row in range(part * share, (part + 1) * share):
            at = row * ROWS
            picked = moved_buf[at : at + ROWS, :]
            for total in totals:
                picked = picked + total[pl.ds(row, BLK_DEV, stride=rows), :]
            out_buf[at : at + ROWS, :] = picked
        at = pl.ds(part * share * ROWS, share * ROWS)
        stores.append(pltpu.make_async_copy(out_buf.at[at], out_hbm.at[at], out_sems.at[part]))
        stores[-1].start()
    for store in stores:
        store.wait()


def combine(arrived, moved):
    sources, deep, cols = arrived.shape
    rows = (deep - MARK_ROWS) // CAP
    anywhere = pl.BlockSpec(memory_space=pl.ANY)
    return pl.pallas_call(
        combine_kernel,
        in_specs=[anywhere] * 2,
        out_specs=anywhere,
        scratch_shapes=[
            pltpu.VMEM(arrived.shape, arrived.dtype),
            pltpu.VMEM(moved.shape, moved.dtype),
            pltpu.VMEM(moved.shape, moved.dtype),
            pltpu.SemaphoreType.DMA((sources // SOURCE_STEP,)),
            pltpu.SemaphoreType.DMA,
            pltpu.SemaphoreType.DMA((OUT_PARTS,)),
        ]
        + [pltpu.VMEM(((BLK_DEV + 1) * rows, cols), jnp.float32)] * SUMS,
        out_shape=jax.ShapeDtypeStruct(moved.shape, jnp.float32),
        compiler_params=params(60),
    )(arrived, moved)


def halos(packed):
    edge, top, bottom = packed
    lats, lons = lax.axis_size("lat"), lax.axis_size("lon")

    def received(value, lat_step, lon_step):
        pairs = []
        for lat in range(lats):
            for lon in range(lons):
                if 0 <= lat + lat_step < lats:
                    source = (lat + lat_step) * lons + (lon + lon_step) % lons
                    pairs.append((source, lat * lons + lon))
        return lax.ppermute(value, ("lat", "lon"), pairs)

    low, high = received(bottom, -1, 0), received(top, 1, 0)
    edges = [received(edge, lat, lon) for lat in (0, -1, 1) for lon in (-1, 1)]
    return low, high, edges


def body(
    tracers, winds, depart_first, depart_second, fluxes, remap_weights, target_device, target_block
):
    shape = tracers.shape
    devices = lax.axis_size("lat") * lax.axis_size("lon")
    tracers, winds, depart_first, depart_second = (
        field.reshape(-1, COLS) for field in (tracers, winds, depart_first, depart_second)
    )
    low, high, edges = halos(pack(tracers, winds))
    chunks = remap(fluxes, remap_weights, target_device, target_block, devices)
    chunks, low, high, edges = lax.optimization_barrier((chunks, low, high, edges))
    arrived = lax.all_to_all(chunks, ("lat", "lon"), split_axis=0, concat_axis=0, tiled=True)
    moved = advect(tracers, low, high, edges, depart_first, depart_second, winds)
    return combine(arrived, moved).reshape(shape)


def solution(mesh):
    in_specs = (
        P(None, None, "lat", "lon"),
        P(None, None, "lat", "lon"),
        P(None, None, "lat", "lon"),
        P(None, None, "lat", "lon"),
        P(("lat", "lon"), None, None),
        P(("lat", "lon"), None, None, None),
        P(("lat", "lon"), None),
        P(("lat", "lon"), None),
    )
    out_specs = P(None, None, "lat", "lon")
    return jax.shard_map(body, mesh=mesh, in_specs=in_specs, out_specs=out_specs, check_vma=False)
```

```python
import functools

import jax
import jax.numpy as jnp
from jax import lax
from jax.experimental import pallas as pl
from jax.experimental.pallas import tpu as pltpu
from jax.sharding import PartitionSpec as P

NTR = 16
LEV = 8
CAP = 2
BLK_DEV = 16
ROWS = 16
COLS = 128
WIDE = 4
NEAR = 3
WROWS = ROWS + 2 * WIDE
TROWS = ROWS + 2 * NEAR
EDGE = 2 * WIDE
PER_GROUP = COLS // EDGE
TILE_STEP = 4
SOURCE_STEP = 8
SUMS = 2
MARK_ROWS = 8
OUT_PARTS = 4


def params(mebibytes):
    return pltpu.CompilerParams(vmem_limit_bytes=mebibytes * 1024 * 1024)


def remap_kernel(
    device_ref, block_ref, flux_hbm, weight_hbm, out_hbm, flux_buf, weight_buf, held, marks, sent,
    flux_sems, weight_sems, out_sem, mark_sem, counts,
):
    tiles = flux_hbm.shape[0]
    links, rows = weight_hbm.shape[1], flux_hbm.shape[1]
    groups = tiles // TILE_STEP

    def loads(group):
        at = pl.ds(group * TILE_STEP, TILE_STEP)
        return (
            pltpu.make_async_copy(flux_hbm.at[at], flux_buf.at[at], flux_sems.at[group]),
            pltpu.make_async_copy(weight_hbm.at[at], weight_buf.at[at], weight_sems.at[group]),
        )

    for group in range(groups):
        for load in loads(group):
            load.start()

    def clear(i, carry):
        counts[i] = 0
        return carry

    lax.fori_loop(0, counts.shape[0], clear, 0, unroll=8)
    marks[...] = jnp.full(marks.shape, BLK_DEV, jnp.float32)

    def place(tile, link):
        owner = device_ref[link, tile]
        rank = counts[owner]
        counts[owner] = rank + 1
        value = block_ref[link, tile].astype(jnp.float32)
        marks[owner, pl.ds(rank, 1), :] = jnp.full((1, COLS), value, jnp.float32)
        return owner, pl.ds(pl.multiple_of(rank * rows, rows), rows)

    def work(group, carry):
        for load in loads(group):
            load.wait()
        for part in range(TILE_STEP):
            at = group * TILE_STEP + part
            flux = flux_buf[at]
            for pair in range(links // 2):
                both = jnp.concatenate(
                    [weight_buf[at, 2 * pair], weight_buf[at, 2 * pair + 1]], axis=1
                )
                made = jnp.dot(flux, both, preferred_element_type=jnp.float32)
                made = made.astype(jnp.bfloat16)
                for side in range(2):
                    into = pl.ds(side * rows, rows)
                    held[at * (links // 2) + pair, into] = made[:, side * COLS : (side + 1) * COLS]
        for part in range(TILE_STEP):
            at = group * TILE_STEP + part
            for link in range(links):
                owner, into = place(at, link)
                source = held.at[at * (links // 2) + link // 2, pl.ds(link % 2 * rows, rows)]
                pltpu.make_async_copy(source, out_hbm.at[owner, into], out_sem).start()
        return carry

    lax.fori_loop(0, groups, work, 0)
    sent[...] = marks[...].astype(jnp.bfloat16)
    last = pltpu.make_async_copy(sent, out_hbm.at[:, pl.ds(CAP * rows, MARK_ROWS)], mark_sem)
    last.start()
    last.wait()
    everything = out_hbm.at[pl.ds(0, tiles * links // 2), pl.ds(0, 2 * rows)]
    pltpu.make_async_copy(held, everything, out_sem).wait()


def remap(fluxes, remap_weights, target_device, target_block, devices):
    tiles, rows, cells = fluxes.shape
    links, cols = remap_weights.shape[1], remap_weights.shape[3]
    anywhere = pl.BlockSpec(memory_space=pl.ANY)
    groups = tiles // TILE_STEP
    return pl.pallas_call(
        remap_kernel,
        in_specs=[pl.BlockSpec(memory_space=pltpu.SMEM)] * 2 + [anywhere] * 2,
        out_specs=anywhere,
        scratch_shapes=[
            pltpu.VMEM(fluxes.shape, jnp.bfloat16),
            pltpu.VMEM(remap_weights.shape, jnp.bfloat16),
            pltpu.VMEM((tiles * links // 2, 2 * rows, cols), jnp.bfloat16),
            pltpu.VMEM((devices, MARK_ROWS, cols), jnp.float32),
            pltpu.VMEM((devices, MARK_ROWS, cols), jnp.bfloat16),
            pltpu.SemaphoreType.DMA((groups,)),
            pltpu.SemaphoreType.DMA((groups,)),
            pltpu.SemaphoreType.DMA,
            pltpu.SemaphoreType.DMA,
            pltpu.SMEM((devices,), jnp.int32),
        ],
        out_shape=jax.ShapeDtypeStruct((devices, CAP * rows + MARK_ROWS, cols), jnp.bfloat16),
        compiler_params=params(60),
    )(target_device.T, target_block.T, fluxes, remap_weights)


def wind_piece(winds_ref, row, comp):
    return winds_ref[pl.ds(comp * LEV * ROWS + row, LEV, stride=ROWS), :]


def tracer_piece(tracers_ref, row, level, half):
    start = half * 8 * LEV * ROWS + level * ROWS + row
    return tracers_ref[pl.ds(start, 8, stride=LEV * ROWS), :]


WIND_MSG = WIDE * 3 * LEV
TRACER_MSG = NEAR * LEV * NTR
MSG = WIND_MSG + TRACER_MSG
EDGE_ROWS = (NTR + LEV) * 8
LOADS = 8


def pack_kernel(tracers_hbm, winds_hbm, edge_ref, tracers_ref, winds_ref, sems):
    share = NTR * LEV * ROWS // LOADS
    loads = [pltpu.make_async_copy(winds_hbm, winds_ref, sems.at[LOADS])]
    for part in range(LOADS):
        at = pl.ds(part * share, share)
        loads.append(pltpu.make_async_copy(tracers_hbm.at[at], tracers_ref.at[at], sems.at[part]))
    for load in loads:
        load.start()
    group_of = lax.broadcasted_iota(jnp.int32, (8, COLS), 1) // EDGE

    def packed(pieces):
        held = jnp.zeros((8, COLS), jnp.float32)
        for spot, piece in enumerate(pieces):
            turned = pltpu.roll(piece, (WIDE + EDGE * spot) % COLS, 1)
            held = jnp.where(group_of == spot, turned, held)
        return held

    loads[0].wait()
    for level in range(LEV):
        starts = [
            comp * LEV * ROWS + level * ROWS + half * 8 for comp in range(3) for half in range(2)
        ]
        at = (NTR + level) * 8
        edge_ref[at : at + 8, :] = packed([winds_ref[start : start + 8, :] for start in starts])
    for tracer in range(NTR):
        if tracer % (NTR // LOADS) == 0:
            loads[1 + tracer // (NTR // LOADS)].wait()
        starts = [tracer * LEV * ROWS + spot * 8 for spot in range(PER_GROUP)]
        at = tracer * 8
        edge_ref[at : at + 8, :] = packed([tracers_ref[start : start + 8, :] for start in starts])


def pack(tracers, winds):
    return pl.pallas_call(
        pack_kernel,
        in_specs=[pl.BlockSpec(memory_space=pl.ANY)] * 2,
        out_specs=pl.BlockSpec(memory_space=pltpu.VMEM),
        out_shape=jax.ShapeDtypeStruct((EDGE_ROWS, COLS), jnp.float32),
        scratch_shapes=[
            pltpu.VMEM(tracers.shape, jnp.float32),
            pltpu.VMEM(winds.shape, jnp.float32),
            pltpu.SemaphoreType.DMA((LOADS + 1,)),
        ],
        compiler_params=params(60),
    )(tracers, winds)


def merged_edges(left, right):
    lane = lax.broadcasted_iota(jnp.int32, left.shape, 1)
    return jnp.where(lax.rem(lane, EDGE) < WIDE, left, right)


def rows_kernel(tracers_ref, winds_ref, left_ref, right_ref, top_ref, bottom_ref):
    both = merged_edges(left_ref[...], right_ref[...])
    for target, wind_from, tracer_from in (
        (top_ref, 0, 0),
        (bottom_ref, ROWS - WIDE, ROWS - NEAR),
    ):
        for row in range(WIDE):
            for comp in range(3):
                at = (row * 3 + comp) * LEV
                target[at : at + LEV, :] = wind_piece(winds_ref, wind_from + row, comp)
        for row in range(NEAR):
            for level in range(LEV):
                for half in range(2):
                    at = WIND_MSG + (row * LEV + level) * NTR + half * 8
                    target[at : at + 8, :] = tracer_piece(
                        tracers_ref, tracer_from + row, level, half
                    )
        target[MSG : MSG + EDGE_ROWS, :] = both


def outer_rows(tracers, winds, left, right):
    return pl.pallas_call(
        rows_kernel,
        out_shape=[jax.ShapeDtypeStruct((MSG + EDGE_ROWS, COLS), jnp.float32)] * 2,
        compiler_params=params(60),
    )(tracers, winds, left, right)


def cubic_weights(frac):
    first = -frac * (frac - 1.0) * (frac - 2.0) / 6.0
    second = (frac + 1.0) * (frac - 1.0) * (frac - 2.0) / 2.0
    third = -(frac + 1.0) * frac * (frac - 2.0) / 2.0
    fourth = (frac + 1.0) * frac * (frac - 1.0) / 6.0
    return (first, second, third, fourth)


def spread_weights(offset, frac, lowest, highest):
    stencil = cubic_weights(frac)
    hits = {value: offset == value for value in range(lowest, highest + 1)}
    spread = []
    for target in range(lowest - 1, highest + 3):
        weight = jnp.zeros(frac.shape, jnp.float32)
        for step in range(4):
            value = target - step + 1
            if value in hits:
                weight = weight + jnp.where(hits[value], stencil[step], 0.0)
        spread.append(weight)
    return spread


def column_shifts(main, edge, reach):
    lane = lax.broadcasted_iota(jnp.int32, main.shape, 1)
    shifted = []
    for step in range(-reach, reach + 1):
        if step == 0:
            shifted.append(main)
            continue
        inside = lane < COLS - step if step > 0 else lane >= -step
        turn = (COLS - step) % COLS
        shifted.append(jnp.where(inside, pltpu.roll(main, turn, 1), pltpu.roll(edge, turn, 1)))
    return shifted


def level_shift(value, step):
    if step == 0:
        return value
    level = lax.broadcasted_iota(jnp.int32, value.shape, 0)
    turned = pltpu.roll(value, (LEV - step) % LEV, 0)
    if step > 0:
        end = jnp.broadcast_to(value[LEV - 1 : LEV, :], value.shape)
        return jnp.where(level >= LEV - step, end, turned)
    end = jnp.broadcast_to(value[0:1, :], value.shape)
    return jnp.where(level < -step, end, turned)


W_TAPS = 9
T_TAPS = 7
L_TAPS = 5
SPREADS = L_TAPS + 2 * T_TAPS
SIDE_ROWS = 2 * WIDE
SIDE_TAPS = WIDE + 2 * NEAR


def edge_piece(ref, start, spot):
    return pltpu.roll(ref[pl.ds(start, 8, stride=8), :], (COLS - WIDE - EDGE * spot) % COLS, 1)


def keep_wind_taps(taps, onto, comp, main, edge):
    shifted = column_shifts(main, edge, WIDE)
    for side in range(W_TAPS):
        for above in range(L_TAPS):
            taps[onto, comp, above, side] = level_shift(shifted[side], above - 2)


def keep_tracer_taps(taps, onto, main_of, edges, base, within, upper):
    for spot in range(PER_GROUP):
        level, half = spot // 2, spot % 2
        edge = edge_piece(edges, base + half * 64 + within, level * 2 + upper)
        shifted = column_shifts(main_of(level, half), edge, NEAR)
        for side in range(T_TAPS):
            taps[onto, spot, side] = shifted[side]


def components(ref, row):
    return [ref[pl.ds(comp * LEV * ROWS + row, LEV, stride=ROWS), :] for comp in range(3)]


def first_weights(winds_ref, first_ref, row):
    wind, first = components(winds_ref, row), components(first_ref, row)
    frac = [jnp.clip(-w - d.astype(jnp.float32), 0.0, 1.0) for w, d in zip(wind, first)]
    level_w = spread_weights(first[0], frac[0], -1, 0)
    row_w = spread_weights(first[1], frac[1], -3, 2)
    col_w = spread_weights(first[2], frac[2], -3, 2)
    return wind, level_w, row_w, col_w


def wind_sum(taps, rows, total, level_w, row_w, col_w):
    total = list(total)
    for above in range(L_TAPS):
        part = [jnp.zeros((LEV, COLS), jnp.float32) for _ in range(3)]
        for across, place in rows:
            for comp in range(3):
                inner = col_w[0] * taps[place, comp, above, 0]
                for side in range(1, W_TAPS):
                    inner = inner + col_w[side] * taps[place, comp, above, side]
                part[comp] = part[comp] + row_w[across] * inner
        for comp in range(3):
            total[comp] = total[comp] + level_w[above] * part[comp]
    return total


def keep_second_weights(spread_ref, place, wind, midwind, second_ref, row):
    second = components(second_ref, row)
    frac = [
        jnp.clip(-(w + m) * 0.5 - d.astype(jnp.float32), 0.0, 1.0)
        for w, m, d in zip(wind, midwind, second)
    ]
    weights = spread_weights(second[0], frac[0], -1, 0)
    weights += spread_weights(second[1], frac[1], -2, 1)
    weights += spread_weights(second[2], frac[2], -2, 1)
    for which in range(SPREADS):
        spread_ref[place, which] = weights[which]


def move_cell(taps, first_tap, spread_ref, place, level, row, out_ref):
    def weight(which):
        return jnp.broadcast_to(spread_ref[place, which, pl.ds(level, 1), :], (8, COLS))

    row_w = [weight(L_TAPS + which) for which in range(T_TAPS)]
    col_w = [weight(L_TAPS + T_TAPS + which) for which in range(T_TAPS)]
    total = [jnp.zeros((8, COLS), jnp.float32) for _ in range(2)]
    for above in range(L_TAPS):
        source = jnp.clip(level + above - 2, 0, LEV - 1)
        level_w = weight(above)
        part = [jnp.zeros((8, COLS), jnp.float32) for _ in range(2)]
        for across in range(T_TAPS):
            for half in range(2):
                piece = taps.at[first_tap + across, source * 2 + half]
                inner = col_w[0] * piece[0]
                for side in range(1, T_TAPS):
                    inner = inner + col_w[side] * piece[side]
                part[half] = part[half] + row_w[across] * inner
        for half in range(2):
            total[half] = total[half] + level_w * part[half]
    for half in range(2):
        start = half * 8 * LEV * ROWS + level * ROWS + row
        out_ref[pl.ds(start, 8, stride=LEV * ROWS), :] = total[half]


def inner_kernel(
    tracers_ref, winds_ref, left_ref, right_ref, first_ref, second_ref, out_ref, partial_ref,
    taps_hbm, edges, wind_taps, tracer_taps, spread_ref, taps_sem,
):
    edges[...] = merged_edges(left_ref[...], right_ref[...])
    for upper in range(2):

        def own_taps(within, carry, upper=upper):
            row = upper * 8 + within
            main_of = functools.partial(tracer_piece, tracers_ref, row)
            keep_tracer_taps(tracer_taps, row, main_of, edges, 0, within, upper)
            return carry

        lax.fori_loop(0, 8, own_taps, 0)
    save = pltpu.make_async_copy(tracer_taps, taps_hbm, taps_sem)
    save.start()
    for comp in range(3):
        for row in range(ROWS):
            edge = edge_piece(edges, NTR * 8 + row % 8, comp * 2 + row // 8)
            keep_wind_taps(wind_taps, row + WIDE, comp, wind_piece(winds_ref, row, comp), edge)
    for place in (0, WIDE + ROWS):
        wind_taps[pl.ds(place, WIDE)] = jnp.zeros((WIDE,) + wind_taps.shape[1:], jnp.float32)

    def midwind_of(row):
        wind, level_w, row_w, col_w = first_weights(winds_ref, first_ref, row)
        zero = [jnp.zeros((LEV, COLS), jnp.float32)] * 3
        rows = [(across, row + across) for across in range(W_TAPS)]
        return wind, wind_sum(wind_taps, rows, zero, level_w, row_w, col_w)

    def middle_row(place, carry):
        row = place + WIDE
        wind, midwind = midwind_of(row)
        keep_second_weights(spread_ref, place, wind, midwind, second_ref, row)
        return carry

    lax.fori_loop(0, ROWS - SIDE_ROWS, middle_row, 0)

    def side_row(place, carry):
        row = jnp.where(place < WIDE, place, place + ROWS - SIDE_ROWS)
        midwind = midwind_of(row)[1]
        for comp in range(3):
            partial_ref[place, comp] = midwind[comp]
        return carry

    lax.fori_loop(0, SIDE_ROWS, side_row, 0)

    def cell(index, carry):
        place, level = index // LEV, lax.rem(index, LEV)
        row = place + WIDE
        move_cell(tracer_taps, row - NEAR, spread_ref, place, level, row, out_ref)
        return carry

    lax.fori_loop(0, (ROWS - SIDE_ROWS) * LEV, cell, 0)
    save.wait()


def inner_advect(tracers, winds, left, right, first, second):
    vmem = pl.BlockSpec(memory_space=pltpu.VMEM)
    taps = (ROWS, PER_GROUP, T_TAPS, 8, COLS)
    return pl.pallas_call(
        inner_kernel,
        in_specs=[vmem] * 6,
        out_specs=[vmem, vmem, pl.BlockSpec(memory_space=pl.ANY)],
        out_shape=[
            jax.ShapeDtypeStruct((NTR * LEV * ROWS, COLS), jnp.float32),
            jax.ShapeDtypeStruct((SIDE_ROWS, 3, LEV, COLS), jnp.float32),
            jax.ShapeDtypeStruct(taps, jnp.float32),
        ],
        scratch_shapes=[
            pltpu.VMEM((EDGE_ROWS, COLS), jnp.float32),
            pltpu.VMEM((WROWS, 3, L_TAPS, W_TAPS, LEV, COLS), jnp.float32),
            pltpu.VMEM(taps, jnp.float32),
            pltpu.VMEM((ROWS - SIDE_ROWS, SPREADS, LEV, COLS), jnp.float32),
            pltpu.SemaphoreType.DMA,
        ],
        compiler_params=params(60),
    )(tracers, winds, left, right, first, second)


def outer_kernel(
    low_ref, high_ref, partial_ref, winds_ref, first_ref, second_ref, taps_hbm, inner_hbm, out_ref,
    wind_taps, tracer_taps, spread_ref, sems,
):
    own = SIDE_TAPS - NEAR
    loads = (
        pltpu.make_async_copy(taps_hbm.at[pl.ds(0, own)], tracer_taps.at[pl.ds(NEAR, own)], sems.at[0]),
        pltpu.make_async_copy(
            taps_hbm.at[pl.ds(ROWS - own, own)], tracer_taps.at[pl.ds(SIDE_TAPS, own)], sems.at[1]
        ),
        pltpu.make_async_copy(inner_hbm, out_ref, sems.at[2]),
    )
    for load in loads:
        load.start()
    for comp in range(3):
        for ref, onto, upper in ((low_ref, 0, 1), (high_ref, WIDE, 0)):
            for row in range(WIDE):
                at = (row * 3 + comp) * LEV
                within = row + (8 - WIDE if upper else 0)
                edge = edge_piece(ref, MSG + NTR * 8 + within, comp * 2 + upper)
                keep_wind_taps(wind_taps, onto + row, comp, ref[at : at + LEV, :], edge)
    for place in range(SIDE_ROWS):
        row = place if place < WIDE else place + ROWS - SIDE_ROWS
        wind, level_w, row_w, col_w = first_weights(winds_ref, first_ref, row)
        if place < WIDE:
            rows = [(across, place + across) for across in range(WIDE - place)]
        else:
            rows = [
                (across, row + across - ROWS) for across in range(WIDE + ROWS - row, W_TAPS)
            ]
        total = [partial_ref[place, comp] for comp in range(3)]
        midwind = wind_sum(wind_taps, rows, total, level_w, row_w, col_w)
        keep_second_weights(spread_ref, place, wind, midwind, second_ref, row)
    for ref, onto, upper in ((low_ref, 0, 1), (high_ref, SIDE_TAPS + own, 0)):

        def halo_taps(row, carry, ref=ref, onto=onto, upper=upper):
            def main_of(level, half):
                at = WIND_MSG + row * LEV * NTR + level * NTR + half * 8
                return ref[pl.ds(pl.multiple_of(at, 8), 8), :]

            within = row + (8 - NEAR if upper else 0)
            keep_tracer_taps(tracer_taps, row + onto, main_of, ref, MSG, within, upper)
            return carry

        lax.fori_loop(0, NEAR, halo_taps, 0)
    for load in loads:
        load.wait()

    def cell(index, carry):
        place, level = index // LEV, lax.rem(index, LEV)
        late = place >= WIDE
        row = jnp.where(late, place + ROWS - SIDE_ROWS, place)
        first_tap = jnp.where(late, place - WIDE + SIDE_TAPS, place)
        move_cell(tracer_taps, first_tap, spread_ref, place, level, row, out_ref)
        return carry

    lax.fori_loop(0, SIDE_ROWS * LEV, cell, 0)


def outer_advect(low, high, partial, winds, first, second, taps, inner):
    vmem = pl.BlockSpec(memory_space=pltpu.VMEM)
    return pl.pallas_call(
        outer_kernel,
        in_specs=[vmem] * 6 + [pl.BlockSpec(memory_space=pl.ANY)] * 2,
        out_specs=vmem,
        out_shape=jax.ShapeDtypeStruct((NTR * LEV * ROWS, COLS), jnp.float32),
        scratch_shapes=[
            pltpu.VMEM((SIDE_ROWS, 3, L_TAPS, W_TAPS, LEV, COLS), jnp.float32),
            pltpu.VMEM((2 * SIDE_TAPS, PER_GROUP, T_TAPS, 8, COLS), jnp.float32),
            pltpu.VMEM((SIDE_ROWS, SPREADS, LEV, COLS), jnp.float32),
            pltpu.SemaphoreType.DMA((3,)),
        ],
        compiler_params=params(60),
    )(low, high, partial, winds, first, second, taps, inner)


def combine_kernel(
    arrived_hbm, moved_hbm, out_hbm, arrived_buf, moved_buf, out_buf, arrived_sems, moved_sem, out_sems, *totals
):
    sources, deep, cols = arrived_hbm.shape
    rows = (deep - MARK_ROWS) // CAP
    groups = sources // SOURCE_STEP

    def load(group):
        at = pl.ds(group * SOURCE_STEP, SOURCE_STEP)
        return pltpu.make_async_copy(arrived_hbm.at[at], arrived_buf.at[at], arrived_sems.at[group])

    for group in range(groups):
        load(group).start()
    moved_load = pltpu.make_async_copy(moved_hbm, moved_buf, moved_sem)
    moved_load.start()
    for total in totals:
        total[...] = jnp.zeros(total.shape, jnp.float32)

    def add(group, carry):
        load(group).wait()
        blocks = []
        for which in range(SOURCE_STEP):
            marks = arrived_buf[group * SOURCE_STEP + which, CAP * rows : deep, :]
            marks = marks.astype(jnp.float32).astype(jnp.int32)
            blocks += [marks[rank, 0] for rank in range(CAP)]
        for which in range(SOURCE_STEP):
            for rank in range(CAP):
                item = which * CAP + rank
                total = totals[item % SUMS]
                at = pl.ds(pl.multiple_of(blocks[item] * rows, rows), rows)
                piece = arrived_buf[group * SOURCE_STEP + which, rank * rows : (rank + 1) * rows, :]
                total[at, :] = total[at, :] + piece.astype(jnp.float32)
        return carry

    lax.fori_loop(0, groups, add, 0)
    moved_load.wait()
    share = rows // OUT_PARTS
    stores = []
    for part in range(OUT_PARTS):
        for row in range(part * share, (part + 1) * share):
            at = row * ROWS
            picked = moved_buf[at : at + ROWS, :]
            for total in totals:
                picked = picked + total[pl.ds(row, BLK_DEV, stride=rows), :]
            out_buf[at : at + ROWS, :] = picked
        at = pl.ds(part * share * ROWS, share * ROWS)
        stores.append(pltpu.make_async_copy(out_buf.at[at], out_hbm.at[at], out_sems.at[part]))
        stores[-1].start()
    for store in stores:
        store.wait()


def combine(arrived, moved):
    sources, deep, cols = arrived.shape
    rows = (deep - MARK_ROWS) // CAP
    anywhere = pl.BlockSpec(memory_space=pl.ANY)
    return pl.pallas_call(
        combine_kernel,
        in_specs=[anywhere] * 2,
        out_specs=anywhere,
        scratch_shapes=[
            pltpu.VMEM(arrived.shape, arrived.dtype),
            pltpu.VMEM(moved.shape, moved.dtype),
            pltpu.VMEM(moved.shape, moved.dtype),
            pltpu.SemaphoreType.DMA((sources // SOURCE_STEP,)),
            pltpu.SemaphoreType.DMA,
            pltpu.SemaphoreType.DMA((OUT_PARTS,)),
        ]
        + [pltpu.VMEM(((BLK_DEV + 1) * rows, cols), jnp.float32)] * SUMS,
        out_shape=jax.ShapeDtypeStruct(moved.shape, jnp.float32),
        compiler_params=params(60),
    )(arrived, moved)


def side_columns(tracers, winds):
    lons = lax.axis_size("lon")
    edge = pack(tracers, winds)
    around = [(i, (i + 1) % lons) for i in range(lons)]
    return lax.ppermute(edge, "lon", around), lax.ppermute(edge, "lon", [(b, a) for a, b in around])


def advect(tracers, winds, left, right, first, second):
    lats = lax.axis_size("lat")
    top, bottom = outer_rows(tracers, winds, left, right)
    up = [(i, i + 1) for i in range(lats - 1)]
    low = lax.ppermute(bottom, "lat", up)
    high = lax.ppermute(top, "lat", [(b, a) for a, b in up])
    inner, partial, taps = inner_advect(tracers, winds, left, right, first, second)
    return outer_advect(low, high, partial, winds, first, second, taps, inner)


def body(
    tracers, winds, depart_first, depart_second, fluxes, remap_weights, target_device, target_block
):
    shape = tracers.shape
    devices = lax.axis_size("lat") * lax.axis_size("lon")
    tracers, winds, depart_first, depart_second = (
        field.reshape(-1, COLS) for field in (tracers, winds, depart_first, depart_second)
    )
    left, right = side_columns(tracers, winds)
    chunks = remap(fluxes, remap_weights, target_device, target_block, devices)
    chunks, left, right = lax.optimization_barrier((chunks, left, right))
    arrived = lax.all_to_all(chunks, ("lat", "lon"), split_axis=0, concat_axis=0, tiled=True)
    moved = advect(tracers, winds, left, right, depart_first, depart_second)
    return combine(arrived, moved).reshape(shape)


def solution(mesh):
    in_specs = (
        P(None, None, "lat", "lon"),
        P(None, None, "lat", "lon"),
        P(None, None, "lat", "lon"),
        P(None, None, "lat", "lon"),
        P(("lat", "lon"), None, None),
        P(("lat", "lon"), None, None, None),
        P(("lat", "lon"), None),
        P(("lat", "lon"), None),
    )
    out_specs = P(None, None, "lat", "lon")
    return jax.shard_map(body, mesh=mesh, in_specs=in_specs, out_specs=out_specs, check_vma=False)
```

```python
import functools

import jax
import jax.numpy as jnp
from jax import lax
from jax.experimental import pallas as pl
from jax.experimental.pallas import tpu as pltpu
from jax.sharding import PartitionSpec as P

NTR = 16
LEV = 8
CAP = 2
BLK_DEV = 16
ROWS = 16
COLS = 128
WIDE = 4
NEAR = 3
WROWS = ROWS + 2 * WIDE
TROWS = ROWS + 2 * NEAR
EDGE = 2 * WIDE
PER_GROUP = COLS // EDGE
TILE_STEP = 4
SOURCE_STEP = 8
SUMS = 2
MARK_ROWS = 8
OUT_PARTS = 4


def params(mebibytes):
    return pltpu.CompilerParams(vmem_limit_bytes=mebibytes * 1024 * 1024)


def remap_kernel(
    device_ref, block_ref, flux_hbm, weight_hbm, out_hbm, flux_buf, weight_buf, held, marks, sent,
    flux_sems, weight_sems, out_sem, mark_sem, counts,
):
    tiles = flux_hbm.shape[0]
    links, rows = weight_hbm.shape[1], flux_hbm.shape[1]
    groups = tiles // TILE_STEP

    def loads(group):
        at = pl.ds(group * TILE_STEP, TILE_STEP)
        return (
            pltpu.make_async_copy(flux_hbm.at[at], flux_buf.at[at], flux_sems.at[group]),
            pltpu.make_async_copy(weight_hbm.at[at], weight_buf.at[at], weight_sems.at[group]),
        )

    for group in range(groups):
        for load in loads(group):
            load.start()

    def clear(i, carry):
        counts[i] = 0
        return carry

    lax.fori_loop(0, counts.shape[0], clear, 0, unroll=8)
    marks[...] = jnp.full(marks.shape, BLK_DEV, jnp.float32)

    def place(tile, link):
        owner = device_ref[link, tile]
        rank = counts[owner]
        counts[owner] = rank + 1
        value = block_ref[link, tile].astype(jnp.float32)
        marks[owner, pl.ds(rank, 1), :] = jnp.full((1, COLS), value, jnp.float32)
        return owner, pl.ds(pl.multiple_of(rank * rows, rows), rows)

    def work(group, carry):
        for load in loads(group):
            load.wait()
        for part in range(TILE_STEP):
            at = group * TILE_STEP + part
            flux = flux_buf[at]
            for pair in range(links // 2):
                both = jnp.concatenate(
                    [weight_buf[at, 2 * pair], weight_buf[at, 2 * pair + 1]], axis=1
                )
                made = jnp.dot(flux, both, preferred_element_type=jnp.float32)
                made = made.astype(jnp.bfloat16)
                for side in range(2):
                    into = pl.ds(side * rows, rows)
                    held[at * (links // 2) + pair, into] = made[:, side * COLS : (side + 1) * COLS]
        for part in range(TILE_STEP):
            at = group * TILE_STEP + part
            for link in range(links):
                owner, into = place(at, link)
                source = held.at[at * (links // 2) + link // 2, pl.ds(link % 2 * rows, rows)]
                pltpu.make_async_copy(source, out_hbm.at[owner, into], out_sem).start()
        return carry

    lax.fori_loop(0, groups, work, 0)
    sent[...] = marks[...].astype(jnp.bfloat16)
    last = pltpu.make_async_copy(sent, out_hbm.at[:, pl.ds(CAP * rows, MARK_ROWS)], mark_sem)
    last.start()
    last.wait()
    everything = out_hbm.at[pl.ds(0, tiles * links // 2), pl.ds(0, 2 * rows)]
    pltpu.make_async_copy(held, everything, out_sem).wait()


def remap(fluxes, remap_weights, target_device, target_block, devices):
    tiles, rows, cells = fluxes.shape
    links, cols = remap_weights.shape[1], remap_weights.shape[3]
    anywhere = pl.BlockSpec(memory_space=pl.ANY)
    groups = tiles // TILE_STEP
    return pl.pallas_call(
        remap_kernel,
        in_specs=[pl.BlockSpec(memory_space=pltpu.SMEM)] * 2 + [anywhere] * 2,
        out_specs=anywhere,
        scratch_shapes=[
            pltpu.VMEM(fluxes.shape, jnp.bfloat16),
            pltpu.VMEM(remap_weights.shape, jnp.bfloat16),
            pltpu.VMEM((tiles * links // 2, 2 * rows, cols), jnp.bfloat16),
            pltpu.VMEM((devices, MARK_ROWS, cols), jnp.float32),
            pltpu.VMEM((devices, MARK_ROWS, cols), jnp.bfloat16),
            pltpu.SemaphoreType.DMA((groups,)),
            pltpu.SemaphoreType.DMA((groups,)),
            pltpu.SemaphoreType.DMA,
            pltpu.SemaphoreType.DMA,
            pltpu.SMEM((devices,), jnp.int32),
        ],
        out_shape=jax.ShapeDtypeStruct((devices, CAP * rows + MARK_ROWS, cols), jnp.bfloat16),
        compiler_params=params(60),
    )(target_device.T, target_block.T, fluxes, remap_weights)


def wind_piece(winds_ref, row, comp):
    return winds_ref[pl.ds(comp * LEV * ROWS + row, LEV, stride=ROWS), :]


def tracer_piece(tracers_ref, row, level, half):
    start = half * 8 * LEV * ROWS + level * ROWS + row
    return tracers_ref[pl.ds(start, 8, stride=LEV * ROWS), :]


WIND_MSG = WIDE * 3 * LEV
TRACER_MSG = NEAR * LEV * NTR
MSG = WIND_MSG + TRACER_MSG
EDGE_ROWS = (NTR + LEV) * 8
LOADS = 8


def pack_kernel(tracers_hbm, winds_hbm, edge_ref, tracers_ref, winds_ref, sems):
    share = NTR * LEV * ROWS // LOADS
    loads = [pltpu.make_async_copy(winds_hbm, winds_ref, sems.at[LOADS])]
    for part in range(LOADS):
        at = pl.ds(part * share, share)
        loads.append(pltpu.make_async_copy(tracers_hbm.at[at], tracers_ref.at[at], sems.at[part]))
    for load in loads:
        load.start()
    group_of = lax.broadcasted_iota(jnp.int32, (8, COLS), 1) // EDGE

    def packed(pieces):
        held = jnp.zeros((8, COLS), jnp.float32)
        for spot, piece in enumerate(pieces):
            turned = pltpu.roll(piece, (WIDE + EDGE * spot) % COLS, 1)
            held = jnp.where(group_of == spot, turned, held)
        return held

    loads[0].wait()
    for level in range(LEV):
        starts = [
            comp * LEV * ROWS + level * ROWS + half * 8 for comp in range(3) for half in range(2)
        ]
        at = (NTR + level) * 8
        edge_ref[at : at + 8, :] = packed([winds_ref[start : start + 8, :] for start in starts])
    for tracer in range(NTR):
        if tracer % (NTR // LOADS) == 0:
            loads[1 + tracer // (NTR // LOADS)].wait()
        starts = [tracer * LEV * ROWS + spot * 8 for spot in range(PER_GROUP)]
        at = tracer * 8
        edge_ref[at : at + 8, :] = packed([tracers_ref[start : start + 8, :] for start in starts])


def pack(tracers, winds):
    return pl.pallas_call(
        pack_kernel,
        in_specs=[pl.BlockSpec(memory_space=pl.ANY)] * 2,
        out_specs=pl.BlockSpec(memory_space=pltpu.VMEM),
        out_shape=jax.ShapeDtypeStruct((EDGE_ROWS, COLS), jnp.float32),
        scratch_shapes=[
            pltpu.VMEM(tracers.shape, jnp.float32),
            pltpu.VMEM(winds.shape, jnp.float32),
            pltpu.SemaphoreType.DMA((LOADS + 1,)),
        ],
        compiler_params=params(60),
    )(tracers, winds)


def merged_edges(left, right):
    lane = lax.broadcasted_iota(jnp.int32, left.shape, 1)
    return jnp.where(lax.rem(lane, EDGE) < WIDE, left, right)


def rows_kernel(odd_ref, tracers_ref, winds_ref, left_ref, right_ref, near_ref, far_ref):
    both = merged_edges(left_ref[...], right_ref[...])

    def fill(target, wind_from, tracer_from):
        for row in range(WIDE):
            for comp in range(3):
                at = (row * 3 + comp) * LEV
                target[at : at + LEV, :] = wind_piece(winds_ref, wind_from + row, comp)
        for row in range(NEAR):
            for level in range(LEV):
                for half in range(2):
                    at = WIND_MSG + (row * LEV + level) * NTR + half * 8
                    target[at : at + 8, :] = tracer_piece(
                        tracers_ref, tracer_from + row, level, half
                    )
        target[MSG : MSG + EDGE_ROWS, :] = both

    @pl.when(odd_ref[0] == 0)
    def _():
        fill(near_ref, ROWS - WIDE, ROWS - NEAR)
        fill(far_ref, 0, 0)

    @pl.when(odd_ref[0] == 1)
    def _():
        fill(near_ref, 0, 0)
        fill(far_ref, ROWS - WIDE, ROWS - NEAR)


def outer_rows(odd, tracers, winds, left, right):
    return pl.pallas_call(
        rows_kernel,
        in_specs=[pl.BlockSpec(memory_space=pltpu.SMEM)]
        + [pl.BlockSpec(memory_space=pltpu.VMEM)] * 4,
        out_shape=[jax.ShapeDtypeStruct((MSG + EDGE_ROWS, COLS), jnp.float32)] * 2,
        compiler_params=params(60),
    )(odd, tracers, winds, left, right)


def cubic_weights(frac):
    first = -frac * (frac - 1.0) * (frac - 2.0) / 6.0
    second = (frac + 1.0) * (frac - 1.0) * (frac - 2.0) / 2.0
    third = -(frac + 1.0) * frac * (frac - 2.0) / 2.0
    fourth = (frac + 1.0) * frac * (frac - 1.0) / 6.0
    return (first, second, third, fourth)


def spread_weights(offset, frac, lowest, highest):
    stencil = cubic_weights(frac)
    hits = {value: offset == value for value in range(lowest, highest + 1)}
    spread = []
    for target in range(lowest - 1, highest + 3):
        weight = jnp.zeros(frac.shape, jnp.float32)
        for step in range(4):
            value = target - step + 1
            if value in hits:
                weight = weight + jnp.where(hits[value], stencil[step], 0.0)
        spread.append(weight)
    return spread


def column_shifts(main, edge, reach):
    lane = lax.broadcasted_iota(jnp.int32, main.shape, 1)
    shifted = []
    for step in range(-reach, reach + 1):
        if step == 0:
            shifted.append(main)
            continue
        inside = lane < COLS - step if step > 0 else lane >= -step
        turn = (COLS - step) % COLS
        shifted.append(jnp.where(inside, pltpu.roll(main, turn, 1), pltpu.roll(edge, turn, 1)))
    return shifted


def level_shift(value, step):
    if step == 0:
        return value
    level = lax.broadcasted_iota(jnp.int32, value.shape, 0)
    turned = pltpu.roll(value, (LEV - step) % LEV, 0)
    if step > 0:
        end = jnp.broadcast_to(value[LEV - 1 : LEV, :], value.shape)
        return jnp.where(level >= LEV - step, end, turned)
    end = jnp.broadcast_to(value[0:1, :], value.shape)
    return jnp.where(level < -step, end, turned)


W_TAPS = 9
T_TAPS = 7
L_TAPS = 5
SPREADS = L_TAPS + 2 * T_TAPS
SIDE_ROWS = 2 * WIDE
SIDE_TAPS = WIDE + 2 * NEAR


def edge_piece(ref, start, spot):
    return pltpu.roll(ref[pl.ds(start, 8, stride=8), :], (COLS - WIDE - EDGE * spot) % COLS, 1)


def keep_wind_taps(taps, onto, comp, main, edge):
    shifted = column_shifts(main, edge, WIDE)
    for side in range(W_TAPS):
        for above in range(L_TAPS):
            taps[onto, comp, above, side] = level_shift(shifted[side], above - 2)


def keep_tracer_taps(taps, onto, main_of, edges, base, within, upper):
    for spot in range(PER_GROUP):
        level, half = spot // 2, spot % 2
        edge = edge_piece(edges, base + half * 64 + within, level * 2 + upper)
        shifted = column_shifts(main_of(level, half), edge, NEAR)
        for side in range(T_TAPS):
            taps[onto, spot, side] = shifted[side]


def components(ref, row):
    return [ref[pl.ds(comp * LEV * ROWS + row, LEV, stride=ROWS), :] for comp in range(3)]


def first_weights(winds_ref, first_ref, row):
    wind, first = components(winds_ref, row), components(first_ref, row)
    frac = [jnp.clip(-w - d.astype(jnp.float32), 0.0, 1.0) for w, d in zip(wind, first)]
    level_w = spread_weights(first[0], frac[0], -1, 0)
    row_w = spread_weights(first[1], frac[1], -3, 2)
    col_w = spread_weights(first[2], frac[2], -3, 2)
    return wind, level_w, row_w, col_w


def wind_sum(taps, rows, total, level_w, row_w, col_w):
    total = list(total)
    for above in range(L_TAPS):
        part = [jnp.zeros((LEV, COLS), jnp.float32) for _ in range(3)]
        for across, place in rows:
            for comp in range(3):
                inner = col_w[0] * taps[place, comp, above, 0]
                for side in range(1, W_TAPS):
                    inner = inner + col_w[side] * taps[place, comp, above, side]
                part[comp] = part[comp] + row_w[across] * inner
        for comp in range(3):
            total[comp] = total[comp] + level_w[above] * part[comp]
    return total


def keep_second_weights(spread_ref, place, wind, midwind, second_ref, row):
    second = components(second_ref, row)
    frac = [
        jnp.clip(-(w + m) * 0.5 - d.astype(jnp.float32), 0.0, 1.0)
        for w, m, d in zip(wind, midwind, second)
    ]
    weights = spread_weights(second[0], frac[0], -1, 0)
    weights += spread_weights(second[1], frac[1], -2, 1)
    weights += spread_weights(second[2], frac[2], -2, 1)
    for which in range(SPREADS):
        spread_ref[place, which] = weights[which]


def move_cell(taps, first_tap, spread_ref, place, level, row, out_ref):
    def weight(which):
        return jnp.broadcast_to(spread_ref[place, which, pl.ds(level, 1), :], (8, COLS))

    row_w = [weight(L_TAPS + which) for which in range(T_TAPS)]
    col_w = [weight(L_TAPS + T_TAPS + which) for which in range(T_TAPS)]
    total = [jnp.zeros((8, COLS), jnp.float32) for _ in range(2)]
    for above in range(L_TAPS):
        source = jnp.clip(level + above - 2, 0, LEV - 1)
        level_w = weight(above)
        part = [jnp.zeros((8, COLS), jnp.float32) for _ in range(2)]
        for across in range(T_TAPS):
            for half in range(2):
                piece = taps.at[first_tap + across, source * 2 + half]
                inner = col_w[0] * piece[0]
                for side in range(1, T_TAPS):
                    inner = inner + col_w[side] * piece[side]
                part[half] = part[half] + row_w[across] * inner
        for half in range(2):
            total[half] = total[half] + level_w * part[half]
    for half in range(2):
        start = half * 8 * LEV * ROWS + level * ROWS + row
        out_ref[pl.ds(start, 8, stride=LEV * ROWS), :] = total[half]


def inner_kernel(
    tracers_ref, winds_ref, left_ref, right_ref, first_ref, second_ref, out_ref, partial_ref,
    taps_hbm, edges, wind_taps, tracer_taps, spread_ref, taps_sem,
):
    edges[...] = merged_edges(left_ref[...], right_ref[...])
    for upper in range(2):

        def own_taps(within, carry, upper=upper):
            row = upper * 8 + within
            main_of = functools.partial(tracer_piece, tracers_ref, row)
            keep_tracer_taps(tracer_taps, row, main_of, edges, 0, within, upper)
            return carry

        lax.fori_loop(0, 8, own_taps, 0)
    save = pltpu.make_async_copy(tracer_taps, taps_hbm, taps_sem)
    save.start()
    for comp in range(3):
        for row in range(ROWS):
            edge = edge_piece(edges, NTR * 8 + row % 8, comp * 2 + row // 8)
            keep_wind_taps(wind_taps, row + WIDE, comp, wind_piece(winds_ref, row, comp), edge)
    for place in (0, WIDE + ROWS):
        wind_taps[pl.ds(place, WIDE)] = jnp.zeros((WIDE,) + wind_taps.shape[1:], jnp.float32)

    def midwind_of(row):
        wind, level_w, row_w, col_w = first_weights(winds_ref, first_ref, row)
        zero = [jnp.zeros((LEV, COLS), jnp.float32)] * 3
        rows = [(across, row + across) for across in range(W_TAPS)]
        return wind, wind_sum(wind_taps, rows, zero, level_w, row_w, col_w)

    def middle_row(place, carry):
        row = place + WIDE
        wind, midwind = midwind_of(row)
        keep_second_weights(spread_ref, place, wind, midwind, second_ref, row)
        return carry

    lax.fori_loop(0, ROWS - SIDE_ROWS, middle_row, 0)

    def side_row(place, carry):
        row = jnp.where(place < WIDE, place, place + ROWS - SIDE_ROWS)
        midwind = midwind_of(row)[1]
        for comp in range(3):
            partial_ref[place, comp] = midwind[comp]
        return carry

    lax.fori_loop(0, SIDE_ROWS, side_row, 0)

    def cell(index, carry):
        place, level = index // LEV, lax.rem(index, LEV)
        row = place + WIDE
        move_cell(tracer_taps, row - NEAR, spread_ref, place, level, row, out_ref)
        return carry

    lax.fori_loop(0, (ROWS - SIDE_ROWS) * LEV, cell, 0)
    save.wait()


def inner_advect(tracers, winds, left, right, first, second):
    vmem = pl.BlockSpec(memory_space=pltpu.VMEM)
    taps = (ROWS, PER_GROUP, T_TAPS, 8, COLS)
    return pl.pallas_call(
        inner_kernel,
        in_specs=[vmem] * 6,
        out_specs=[vmem, vmem, pl.BlockSpec(memory_space=pl.ANY)],
        out_shape=[
            jax.ShapeDtypeStruct((NTR * LEV * ROWS, COLS), jnp.float32),
            jax.ShapeDtypeStruct((SIDE_ROWS, 3, LEV, COLS), jnp.float32),
            jax.ShapeDtypeStruct(taps, jnp.float32),
        ],
        scratch_shapes=[
            pltpu.VMEM((EDGE_ROWS, COLS), jnp.float32),
            pltpu.VMEM((WROWS, 3, L_TAPS, W_TAPS, LEV, COLS), jnp.float32),
            pltpu.VMEM(taps, jnp.float32),
            pltpu.VMEM((ROWS - SIDE_ROWS, SPREADS, LEV, COLS), jnp.float32),
            pltpu.SemaphoreType.DMA,
        ],
        compiler_params=params(60),
    )(tracers, winds, left, right, first, second)


def outer_kernel(
    side_ref, halo_ref, partial_ref, winds_ref, first_ref, second_ref, taps_hbm, inner_hbm, out_ref,
    wind_taps, tracer_taps, spread_ref, sems,
):
    side = side_ref[0]
    own = SIDE_TAPS - NEAR
    loads = (
        pltpu.make_async_copy(
            taps_hbm.at[pl.ds(side * (ROWS - own), own)],
            tracer_taps.at[pl.ds((1 - side) * NEAR, own)],
            sems.at[0],
        ),
        pltpu.make_async_copy(inner_hbm, out_ref, sems.at[1]),
    )
    for load in loads:
        load.start()

    def prepare(late):
        upper = 1 - late
        for comp in range(3):
            for row in range(WIDE):
                at = (row * 3 + comp) * LEV
                within = row + (8 - WIDE if upper else 0)
                edge = edge_piece(halo_ref, MSG + NTR * 8 + within, comp * 2 + upper)
                keep_wind_taps(wind_taps, row, comp, halo_ref[at : at + LEV, :], edge)
        for place in range(WIDE):
            row = place + late * (ROWS - WIDE)
            wind, level_w, row_w, col_w = first_weights(winds_ref, first_ref, row)
            if late:
                rows = [
                    (across, row + across - ROWS - WIDE)
                    for across in range(WIDE + ROWS - row, W_TAPS)
                ]
            else:
                rows = [(across, place + across) for across in range(WIDE - place)]
            total = [partial_ref[place + late * WIDE, comp] for comp in range(3)]
            midwind = wind_sum(wind_taps, rows, total, level_w, row_w, col_w)
            keep_second_weights(spread_ref, place, wind, midwind, second_ref, row)

        def halo_taps(row, carry):
            def main_of(level, half):
                at = WIND_MSG + row * LEV * NTR + level * NTR + half * 8
                return halo_ref[pl.ds(pl.multiple_of(at, 8), 8), :]

            within = row + (8 - NEAR if upper else 0)
            onto = row + late * own
            keep_tracer_taps(tracer_taps, onto, main_of, halo_ref, MSG, within, upper)
            return carry

        lax.fori_loop(0, NEAR, halo_taps, 0)

    for late in range(2):
        pl.when(side == late)(functools.partial(prepare, late))
    for load in loads:
        load.wait()

    def cell(index, carry):
        place, level = index // LEV, lax.rem(index, LEV)
        row = place + side * (ROWS - WIDE)
        move_cell(tracer_taps, place, spread_ref, place, level, row, out_ref)
        return carry

    lax.fori_loop(0, WIDE * LEV, cell, 0)


def outer_advect(side, halo, partial, winds, first, second, taps, inner):
    vmem = pl.BlockSpec(memory_space=pltpu.VMEM)
    return pl.pallas_call(
        outer_kernel,
        in_specs=[pl.BlockSpec(memory_space=pltpu.SMEM)]
        + [vmem] * 5
        + [pl.BlockSpec(memory_space=pl.ANY)] * 2,
        out_specs=vmem,
        out_shape=jax.ShapeDtypeStruct((NTR * LEV * ROWS, COLS), jnp.float32),
        scratch_shapes=[
            pltpu.VMEM((WIDE, 3, L_TAPS, W_TAPS, LEV, COLS), jnp.float32),
            pltpu.VMEM((SIDE_TAPS, PER_GROUP, T_TAPS, 8, COLS), jnp.float32),
            pltpu.VMEM((WIDE, SPREADS, LEV, COLS), jnp.float32),
            pltpu.SemaphoreType.DMA((2,)),
        ],
        compiler_params=params(60),
    )(side, halo, partial, winds, first, second, taps, inner)


def combine_kernel(
    arrived_hbm, moved_hbm, out_hbm, arrived_buf, moved_buf, out_buf, arrived_sems, moved_sem, out_sems, *totals
):
    sources, deep, cols = arrived_hbm.shape
    rows = (deep - MARK_ROWS) // CAP
    groups = sources // SOURCE_STEP

    def load(group):
        at = pl.ds(group * SOURCE_STEP, SOURCE_STEP)
        return pltpu.make_async_copy(arrived_hbm.at[at], arrived_buf.at[at], arrived_sems.at[group])

    for group in range(groups):
        load(group).start()
    moved_load = pltpu.make_async_copy(moved_hbm, moved_buf, moved_sem)
    moved_load.start()
    for total in totals:
        total[...] = jnp.zeros(total.shape, jnp.float32)

    def add(group, carry):
        load(group).wait()
        blocks = []
        for which in range(SOURCE_STEP):
            marks = arrived_buf[group * SOURCE_STEP + which, CAP * rows : deep, :]
            marks = marks.astype(jnp.float32).astype(jnp.int32)
            blocks += [marks[rank, 0] for rank in range(CAP)]
        for which in range(SOURCE_STEP):
            for rank in range(CAP):
                item = which * CAP + rank
                total = totals[item % SUMS]
                at = pl.ds(pl.multiple_of(blocks[item] * rows, rows), rows)
                piece = arrived_buf[group * SOURCE_STEP + which, rank * rows : (rank + 1) * rows, :]
                total[at, :] = total[at, :] + piece.astype(jnp.float32)
        return carry

    lax.fori_loop(0, groups, add, 0)
    moved_load.wait()
    share = rows // OUT_PARTS
    stores = []
    for part in range(OUT_PARTS):
        for row in range(part * share, (part + 1) * share):
            at = row * ROWS
            picked = moved_buf[at : at + ROWS, :]
            for total in totals:
                picked = picked + total[pl.ds(row, BLK_DEV, stride=rows), :]
            out_buf[at : at + ROWS, :] = picked
        at = pl.ds(part * share * ROWS, share * ROWS)
        stores.append(pltpu.make_async_copy(out_buf.at[at], out_hbm.at[at], out_sems.at[part]))
        stores[-1].start()
    for store in stores:
        store.wait()


def combine(arrived, moved):
    sources, deep, cols = arrived.shape
    rows = (deep - MARK_ROWS) // CAP
    anywhere = pl.BlockSpec(memory_space=pl.ANY)
    return pl.pallas_call(
        combine_kernel,
        in_specs=[anywhere] * 2,
        out_specs=anywhere,
        scratch_shapes=[
            pltpu.VMEM(arrived.shape, arrived.dtype),
            pltpu.VMEM(moved.shape, moved.dtype),
            pltpu.VMEM(moved.shape, moved.dtype),
            pltpu.SemaphoreType.DMA((sources // SOURCE_STEP,)),
            pltpu.SemaphoreType.DMA,
            pltpu.SemaphoreType.DMA((OUT_PARTS,)),
        ]
        + [pltpu.VMEM(((BLK_DEV + 1) * rows, cols), jnp.float32)] * SUMS,
        out_shape=jax.ShapeDtypeStruct(moved.shape, jnp.float32),
        compiler_params=params(60),
    )(arrived, moved)


def side_columns(tracers, winds):
    lons = lax.axis_size("lon")
    edge = pack(tracers, winds)
    around = [(i, (i + 1) % lons) for i in range(lons)]
    return lax.ppermute(edge, "lon", around), lax.ppermute(edge, "lon", [(b, a) for a, b in around])


def advect(tracers, winds, left, right, first, second):
    lats = lax.axis_size("lat")
    odd = lax.rem(lax.axis_index("lat"), 2).reshape(1).astype(jnp.int32)
    near_rows, far_rows = outer_rows(odd, tracers, winds, left, right)

    def swapped(value, start):
        pairs = [(i, i + 1) for i in range(start, lats - 1, 2)]
        return lax.ppermute(value, "lat", pairs + [(b, a) for a, b in pairs])

    near, far = swapped(near_rows, 0), swapped(far_rows, 1)
    inner, partial, taps = inner_advect(tracers, winds, left, right, first, second)
    moved = outer_advect(1 - odd, near, partial, winds, first, second, taps, inner)
    return outer_advect(odd, far, partial, winds, first, second, taps, moved)


def body(
    tracers, winds, depart_first, depart_second, fluxes, remap_weights, target_device, target_block
):
    shape = tracers.shape
    devices = lax.axis_size("lat") * lax.axis_size("lon")
    tracers, winds, depart_first, depart_second = (
        field.reshape(-1, COLS) for field in (tracers, winds, depart_first, depart_second)
    )
    left, right = side_columns(tracers, winds)
    chunks = remap(fluxes, remap_weights, target_device, target_block, devices)
    chunks, left, right = lax.optimization_barrier((chunks, left, right))
    arrived = lax.all_to_all(chunks, ("lat", "lon"), split_axis=0, concat_axis=0, tiled=True)
    moved = advect(tracers, winds, left, right, depart_first, depart_second)
    return combine(arrived, moved).reshape(shape)


def solution(mesh):
    in_specs = (
        P(None, None, "lat", "lon"),
        P(None, None, "lat", "lon"),
        P(None, None, "lat", "lon"),
        P(None, None, "lat", "lon"),
        P(("lat", "lon"), None, None),
        P(("lat", "lon"), None, None, None),
        P(("lat", "lon"), None),
        P(("lat", "lon"), None),
    )
    out_specs = P(None, None, "lat", "lon")
    return jax.shard_map(body, mesh=mesh, in_specs=in_specs, out_specs=out_specs, check_vma=False)
```

```python
import functools

import jax
import jax.numpy as jnp
from jax import lax
from jax.experimental import pallas as pl
from jax.experimental.pallas import tpu as pltpu
from jax.sharding import PartitionSpec as P

NTR = 16
LEV = 8
CAP = 2
BLK_DEV = 16
ROWS = 16
COLS = 128
WIDE = 4
NEAR = 3
WROWS = ROWS + 2 * WIDE
TROWS = ROWS + 2 * NEAR
EDGE = 2 * WIDE
PER_GROUP = COLS // EDGE
TILE_STEP = 6
SOURCE_STEP = 16
SUMS = 1
MARK_ROWS = 8
OUT_PARTS = 4


def params(mebibytes):
    return pltpu.CompilerParams(vmem_limit_bytes=mebibytes * 1024 * 1024)


def remap_kernel(
    device_ref, block_ref, flux_hbm, weight_hbm, out_hbm, flux_buf, weight_buf, held, marks, sent,
    flux_sems, weight_sems, out_sem, mark_sem, counts,
):
    tiles = flux_hbm.shape[0]
    links, rows = weight_hbm.shape[1], flux_hbm.shape[1]
    groups = tiles // TILE_STEP

    def loads(group):
        at = pl.ds(group * TILE_STEP, TILE_STEP)
        return (
            pltpu.make_async_copy(flux_hbm.at[at], flux_buf.at[at], flux_sems.at[group]),
            pltpu.make_async_copy(weight_hbm.at[at], weight_buf.at[at], weight_sems.at[group]),
        )

    for group in range(groups):
        for load in loads(group):
            load.start()

    def clear(i, carry):
        counts[i] = 0
        return carry

    lax.fori_loop(0, counts.shape[0], clear, 0, unroll=8)
    marks[...] = jnp.full(marks.shape, BLK_DEV, jnp.float32)

    def place(tile, link):
        owner = device_ref[link, tile]
        rank = counts[owner]
        counts[owner] = rank + 1
        value = block_ref[link, tile].astype(jnp.float32)
        marks[owner, pl.ds(rank, 1), :] = jnp.full((1, COLS), value, jnp.float32)
        return owner, pl.ds(pl.multiple_of(rank * rows, rows), rows)

    def work(group, carry):
        for load in loads(group):
            load.wait()
        for part in range(TILE_STEP):
            at = group * TILE_STEP + part
            flux = flux_buf[at]
            for pair in range(links // 2):
                both = jnp.concatenate(
                    [weight_buf[at, 2 * pair], weight_buf[at, 2 * pair + 1]], axis=1
                )
                made = jnp.dot(flux, both, preferred_element_type=jnp.float32)
                made = made.astype(jnp.bfloat16)
                for side in range(2):
                    into = pl.ds(side * rows, rows)
                    held[at * (links // 2) + pair, into] = made[:, side * COLS : (side + 1) * COLS]
        for part in range(TILE_STEP):
            at = group * TILE_STEP + part
            for link in range(links):
                owner, into = place(at, link)
                source = held.at[at * (links // 2) + link // 2, pl.ds(link % 2 * rows, rows)]
                pltpu.make_async_copy(source, out_hbm.at[owner, into], out_sem).start()
        return carry

    lax.fori_loop(0, groups, work, 0)
    sent[...] = marks[...].astype(jnp.bfloat16)
    last = pltpu.make_async_copy(sent, out_hbm.at[:, pl.ds(CAP * rows, MARK_ROWS)], mark_sem)
    last.start()
    last.wait()
    everything = out_hbm.at[pl.ds(0, tiles * links // 2), pl.ds(0, 2 * rows)]
    pltpu.make_async_copy(held, everything, out_sem).wait()


def remap(fluxes, remap_weights, target_device, target_block, devices):
    tiles, rows, cells = fluxes.shape
    links, cols = remap_weights.shape[1], remap_weights.shape[3]
    anywhere = pl.BlockSpec(memory_space=pl.ANY)
    groups = tiles // TILE_STEP
    return pl.pallas_call(
        remap_kernel,
        in_specs=[pl.BlockSpec(memory_space=pltpu.SMEM)] * 2 + [anywhere] * 2,
        out_specs=anywhere,
        scratch_shapes=[
            pltpu.VMEM(fluxes.shape, jnp.bfloat16),
            pltpu.VMEM(remap_weights.shape, jnp.bfloat16),
            pltpu.VMEM((tiles * links // 2, 2 * rows, cols), jnp.bfloat16),
            pltpu.VMEM((devices, MARK_ROWS, cols), jnp.float32),
            pltpu.VMEM((devices, MARK_ROWS, cols), jnp.bfloat16),
            pltpu.SemaphoreType.DMA((groups,)),
            pltpu.SemaphoreType.DMA((groups,)),
            pltpu.SemaphoreType.DMA,
            pltpu.SemaphoreType.DMA,
            pltpu.SMEM((devices,), jnp.int32),
        ],
        out_shape=jax.ShapeDtypeStruct((devices, CAP * rows + MARK_ROWS, cols), jnp.bfloat16),
        compiler_params=params(60),
    )(target_device.T, target_block.T, fluxes, remap_weights)


def wind_piece(winds_ref, row, comp):
    return winds_ref[pl.ds(comp * LEV * ROWS + row, LEV, stride=ROWS), :]


def tracer_piece(tracers_ref, row, level, half):
    start = half * 8 * LEV * ROWS + level * ROWS + row
    return tracers_ref[pl.ds(start, 8, stride=LEV * ROWS), :]


WIND_MSG = WIDE * 3 * LEV
TRACER_MSG = NEAR * LEV * NTR
MSG = WIND_MSG + TRACER_MSG
EDGE_ROWS = (NTR + LEV) * 8
LOADS = 4


def pack_kernel(tracers_hbm, winds_hbm, edge_ref, tracers_ref, winds_ref, sems):
    share = NTR * LEV * ROWS // LOADS
    loads = [pltpu.make_async_copy(winds_hbm, winds_ref, sems.at[LOADS])]
    for part in range(LOADS):
        at = pl.ds(part * share, share)
        loads.append(pltpu.make_async_copy(tracers_hbm.at[at], tracers_ref.at[at], sems.at[part]))
    for load in loads:
        load.start()
    group_of = lax.broadcasted_iota(jnp.int32, (8, COLS), 1) // EDGE

    def packed(pieces):
        held = jnp.zeros((8, COLS), jnp.float32)
        for spot, piece in enumerate(pieces):
            turned = pltpu.roll(piece, (WIDE + EDGE * spot) % COLS, 1)
            held = jnp.where(group_of == spot, turned, held)
        return held

    loads[0].wait()
    for level in range(LEV):
        starts = [
            comp * LEV * ROWS + level * ROWS + half * 8 for comp in range(3) for half in range(2)
        ]
        at = (NTR + level) * 8
        edge_ref[at : at + 8, :] = packed([winds_ref[start : start + 8, :] for start in starts])
    for tracer in range(NTR):
        if tracer % (NTR // LOADS) == 0:
            loads[1 + tracer // (NTR // LOADS)].wait()
        starts = [tracer * LEV * ROWS + spot * 8 for spot in range(PER_GROUP)]
        at = tracer * 8
        edge_ref[at : at + 8, :] = packed([tracers_ref[start : start + 8, :] for start in starts])


def pack(tracers, winds):
    return pl.pallas_call(
        pack_kernel,
        in_specs=[pl.BlockSpec(memory_space=pl.ANY)] * 2,
        out_specs=pl.BlockSpec(memory_space=pltpu.VMEM),
        out_shape=jax.ShapeDtypeStruct((EDGE_ROWS, COLS), jnp.float32),
        scratch_shapes=[
            pltpu.VMEM(tracers.shape, jnp.float32),
            pltpu.VMEM(winds.shape, jnp.float32),
            pltpu.SemaphoreType.DMA((LOADS + 1,)),
        ],
        compiler_params=params(60),
    )(tracers, winds)


def merged_edges(left, right):
    lane = lax.broadcasted_iota(jnp.int32, left.shape, 1)
    return jnp.where(lax.rem(lane, EDGE) < WIDE, left, right)


def rows_kernel(odd_ref, tracers_ref, winds_ref, left_ref, right_ref, near_ref, far_ref):
    both = merged_edges(left_ref[...], right_ref[...])

    def fill(target, wind_from, tracer_from):
        for row in range(WIDE):
            for comp in range(3):
                at = (row * 3 + comp) * LEV
                target[at : at + LEV, :] = wind_piece(winds_ref, wind_from + row, comp)
        for row in range(NEAR):
            for level in range(LEV):
                for half in range(2):
                    at = WIND_MSG + (row * LEV + level) * NTR + half * 8
                    target[at : at + 8, :] = tracer_piece(
                        tracers_ref, tracer_from + row, level, half
                    )
        target[MSG : MSG + EDGE_ROWS, :] = both

    @pl.when(odd_ref[0] == 0)
    def _():
        fill(near_ref, ROWS - WIDE, ROWS - NEAR)
        fill(far_ref, 0, 0)

    @pl.when(odd_ref[0] == 1)
    def _():
        fill(near_ref, 0, 0)
        fill(far_ref, ROWS - WIDE, ROWS - NEAR)


def outer_rows(odd, tracers, winds, left, right):
    return pl.pallas_call(
        rows_kernel,
        in_specs=[pl.BlockSpec(memory_space=pltpu.SMEM)]
        + [pl.BlockSpec(memory_space=pltpu.VMEM)] * 4,
        out_shape=[jax.ShapeDtypeStruct((MSG + EDGE_ROWS, COLS), jnp.float32)] * 2,
        compiler_params=params(8),
    )(odd, tracers, winds, left, right)


def cubic_weights(frac):
    first = -frac * (frac - 1.0) * (frac - 2.0) / 6.0
    second = (frac + 1.0) * (frac - 1.0) * (frac - 2.0) / 2.0
    third = -(frac + 1.0) * frac * (frac - 2.0) / 2.0
    fourth = (frac + 1.0) * frac * (frac - 1.0) / 6.0
    return (first, second, third, fourth)


def spread_weights(offset, frac, lowest, highest):
    stencil = cubic_weights(frac)
    hits = {value: offset == value for value in range(lowest, highest + 1)}
    spread = []
    for target in range(lowest - 1, highest + 3):
        weight = jnp.zeros(frac.shape, jnp.float32)
        for step in range(4):
            value = target - step + 1
            if value in hits:
                weight = weight + jnp.where(hits[value], stencil[step], 0.0)
        spread.append(weight)
    return spread


def column_shifts(main, edge, reach):
    lane = lax.broadcasted_iota(jnp.int32, main.shape, 1)
    shifted = []
    for step in range(-reach, reach + 1):
        if step == 0:
            shifted.append(main)
            continue
        inside = lane < COLS - step if step > 0 else lane >= -step
        turn = (COLS - step) % COLS
        shifted.append(jnp.where(inside, pltpu.roll(main, turn, 1), pltpu.roll(edge, turn, 1)))
    return shifted


def level_shift(value, step):
    if step == 0:
        return value
    level = lax.broadcasted_iota(jnp.int32, value.shape, 0)
    turned = pltpu.roll(value, (LEV - step) % LEV, 0)
    if step > 0:
        end = jnp.broadcast_to(value[LEV - 1 : LEV, :], value.shape)
        return jnp.where(level >= LEV - step, end, turned)
    end = jnp.broadcast_to(value[0:1, :], value.shape)
    return jnp.where(level < -step, end, turned)


W_TAPS = 9
T_TAPS = 7
L_TAPS = 5
SPREADS = L_TAPS + 2 * T_TAPS
SIDE_ROWS = 2 * WIDE
SIDE_TAPS = WIDE + 2 * NEAR


def edge_piece(ref, start, spot):
    return pltpu.roll(ref[pl.ds(start, 8, stride=8), :], (COLS - WIDE - EDGE * spot) % COLS, 1)


def keep_wind_taps(taps, onto, comp, main, edge):
    shifted = column_shifts(main, edge, WIDE)
    for side in range(W_TAPS):
        for above in range(L_TAPS):
            taps[onto, comp, above, side] = level_shift(shifted[side], above - 2)


def keep_tracer_taps(taps, onto, main_of, edges, base, within, upper):
    for spot in range(PER_GROUP):
        level, half = spot // 2, spot % 2
        edge = edge_piece(edges, base + half * 64 + within, level * 2 + upper)
        shifted = column_shifts(main_of(level, half), edge, NEAR)
        for side in range(T_TAPS):
            taps[onto, spot, side] = shifted[side]


def components(ref, row):
    return [ref[pl.ds(comp * LEV * ROWS + row, LEV, stride=ROWS), :] for comp in range(3)]


def first_weights(winds_ref, first_ref, row):
    wind, first = components(winds_ref, row), components(first_ref, row)
    frac = [jnp.clip(-w - d.astype(jnp.float32), 0.0, 1.0) for w, d in zip(wind, first)]
    level_w = spread_weights(first[0], frac[0], -1, 0)
    row_w = spread_weights(first[1], frac[1], -3, 2)
    col_w = spread_weights(first[2], frac[2], -3, 2)
    return wind, level_w, row_w, col_w


def wind_sum(taps, rows, total, level_w, row_w, col_w):
    total = list(total)
    for above in range(L_TAPS):
        part = [jnp.zeros((LEV, COLS), jnp.float32) for _ in range(3)]
        for across, place in rows:
            for comp in range(3):
                inner = col_w[0] * taps[place, comp, above, 0]
                for side in range(1, W_TAPS):
                    inner = inner + col_w[side] * taps[place, comp, above, side]
                part[comp] = part[comp] + row_w[across] * inner
        for comp in range(3):
            total[comp] = total[comp] + level_w[above] * part[comp]
    return total


def keep_second_weights(spread_ref, place, wind, midwind, second_ref, row):
    second = components(second_ref, row)
    frac = [
        jnp.clip(-(w + m) * 0.5 - d.astype(jnp.float32), 0.0, 1.0)
        for w, m, d in zip(wind, midwind, second)
    ]
    weights = spread_weights(second[0], frac[0], -1, 0)
    weights += spread_weights(second[1], frac[1], -2, 1)
    weights += spread_weights(second[2], frac[2], -2, 1)
    for which in range(SPREADS):
        spread_ref[place, which] = weights[which]


def move_cell(taps, first_tap, spread_ref, place, level, row, out_ref):
    def weight(which):
        return jnp.broadcast_to(spread_ref[place, which, pl.ds(level, 1), :], (8, COLS))

    row_w = [weight(L_TAPS + which) for which in range(T_TAPS)]
    col_w = [weight(L_TAPS + T_TAPS + which) for which in range(T_TAPS)]
    total = [jnp.zeros((8, COLS), jnp.float32) for _ in range(2)]
    for above in range(L_TAPS):
        source = jnp.clip(level + above - 2, 0, LEV - 1)
        level_w = weight(above)
        part = [jnp.zeros((8, COLS), jnp.float32) for _ in range(2)]
        for across in range(T_TAPS):
            for half in range(2):
                piece = taps.at[first_tap + across, source * 2 + half]
                inner = col_w[0] * piece[0]
                for side in range(1, T_TAPS):
                    inner = inner + col_w[side] * piece[side]
                part[half] = part[half] + row_w[across] * inner
        for half in range(2):
            total[half] = total[half] + level_w * part[half]
    for half in range(2):
        start = half * 8 * LEV * ROWS + level * ROWS + row
        out_ref[pl.ds(start, 8, stride=LEV * ROWS), :] = total[half]


def inner_kernel(
    tracers_ref, winds_ref, left_ref, right_ref, first_ref, second_ref, out_ref, partial_ref,
    taps_hbm, edges, wind_taps, tracer_taps, spread_ref, taps_sem,
):
    edges[...] = merged_edges(left_ref[...], right_ref[...])
    for upper in range(2):

        def own_taps(within, carry, upper=upper):
            row = upper * 8 + within
            main_of = functools.partial(tracer_piece, tracers_ref, row)
            keep_tracer_taps(tracer_taps, row, main_of, edges, 0, within, upper)
            return carry

        lax.fori_loop(0, 8, own_taps, 0)
    save = pltpu.make_async_copy(tracer_taps, taps_hbm, taps_sem)
    save.start()
    for comp in range(3):
        for row in range(ROWS):
            edge = edge_piece(edges, NTR * 8 + row % 8, comp * 2 + row // 8)
            keep_wind_taps(wind_taps, row + WIDE, comp, wind_piece(winds_ref, row, comp), edge)
    for place in (0, WIDE + ROWS):
        wind_taps[pl.ds(place, WIDE)] = jnp.zeros((WIDE,) + wind_taps.shape[1:], jnp.float32)

    def midwind_of(row):
        wind, level_w, row_w, col_w = first_weights(winds_ref, first_ref, row)
        zero = [jnp.zeros((LEV, COLS), jnp.float32)] * 3
        rows = [(across, row + across) for across in range(W_TAPS)]
        return wind, wind_sum(wind_taps, rows, zero, level_w, row_w, col_w)

    def middle_row(place, carry):
        row = place + WIDE
        wind, midwind = midwind_of(row)
        keep_second_weights(spread_ref, place, wind, midwind, second_ref, row)
        return carry

    lax.fori_loop(0, ROWS - SIDE_ROWS, middle_row, 0)

    def side_row(place, carry):
        row = jnp.where(place < WIDE, place, place + ROWS - SIDE_ROWS)
        midwind = midwind_of(row)[1]
        for comp in range(3):
            partial_ref[place, comp] = midwind[comp]
        return carry

    lax.fori_loop(0, SIDE_ROWS, side_row, 0)

    def cell(index, carry):
        place, level = index // LEV, lax.rem(index, LEV)
        row = place + WIDE
        move_cell(tracer_taps, row - NEAR, spread_ref, place, level, row, out_ref)
        return carry

    lax.fori_loop(0, (ROWS - SIDE_ROWS) * LEV, cell, 0)
    save.wait()


def inner_advect(tracers, winds, left, right, first, second):
    vmem = pl.BlockSpec(memory_space=pltpu.VMEM)
    taps = (ROWS, PER_GROUP, T_TAPS, 8, COLS)
    return pl.pallas_call(
        inner_kernel,
        in_specs=[vmem] * 6,
        out_specs=[vmem, vmem, pl.BlockSpec(memory_space=pl.ANY)],
        out_shape=[
            jax.ShapeDtypeStruct((NTR * LEV * ROWS, COLS), jnp.float32),
            jax.ShapeDtypeStruct((SIDE_ROWS, 3, LEV, COLS), jnp.float32),
            jax.ShapeDtypeStruct(taps, jnp.float32),
        ],
        scratch_shapes=[
            pltpu.VMEM((EDGE_ROWS, COLS), jnp.float32),
            pltpu.VMEM((WROWS, 3, L_TAPS, W_TAPS, LEV, COLS), jnp.float32),
            pltpu.VMEM(taps, jnp.float32),
            pltpu.VMEM((ROWS - SIDE_ROWS, SPREADS, LEV, COLS), jnp.float32),
            pltpu.SemaphoreType.DMA,
        ],
        compiler_params=params(40),
    )(tracers, winds, left, right, first, second)


def outer_kernel(
    side_ref, halo_ref, partial_ref, winds_ref, first_ref, second_ref, taps_hbm, inner_hbm, out_ref,
    wind_taps, tracer_taps, spread_ref, sems,
):
    side = side_ref[0]
    own = SIDE_TAPS - NEAR
    loads = (
        pltpu.make_async_copy(
            taps_hbm.at[pl.ds(side * (ROWS - own), own)],
            tracer_taps.at[pl.ds((1 - side) * NEAR, own)],
            sems.at[0],
        ),
        pltpu.make_async_copy(inner_hbm, out_ref, sems.at[1]),
    )
    for load in loads:
        load.start()

    def prepare(late):
        upper = 1 - late
        for comp in range(3):
            for row in range(WIDE):
                at = (row * 3 + comp) * LEV
                within = row + (8 - WIDE if upper else 0)
                edge = edge_piece(halo_ref, MSG + NTR * 8 + within, comp * 2 + upper)
                keep_wind_taps(wind_taps, row, comp, halo_ref[at : at + LEV, :], edge)
        for place in range(WIDE):
            row = place + late * (ROWS - WIDE)
            wind, level_w, row_w, col_w = first_weights(winds_ref, first_ref, row)
            if late:
                rows = [
                    (across, row + across - ROWS - WIDE)
                    for across in range(WIDE + ROWS - row, W_TAPS)
                ]
            else:
                rows = [(across, place + across) for across in range(WIDE - place)]
            total = [partial_ref[place + late * WIDE, comp] for comp in range(3)]
            midwind = wind_sum(wind_taps, rows, total, level_w, row_w, col_w)
            keep_second_weights(spread_ref, place, wind, midwind, second_ref, row)

        def halo_taps(row, carry):
            def main_of(level, half):
                at = WIND_MSG + row * LEV * NTR + level * NTR + half * 8
                return halo_ref[pl.ds(pl.multiple_of(at, 8), 8), :]

            within = row + (8 - NEAR if upper else 0)
            onto = row + late * own
            keep_tracer_taps(tracer_taps, onto, main_of, halo_ref, MSG, within, upper)
            return carry

        lax.fori_loop(0, NEAR, halo_taps, 0)

    for late in range(2):
        pl.when(side == late)(functools.partial(prepare, late))
    for load in loads:
        load.wait()

    def cell(index, carry):
        place, level = index // LEV, lax.rem(index, LEV)
        row = place + side * (ROWS - WIDE)
        move_cell(tracer_taps, place, spread_ref, place, level, row, out_ref)
        return carry

    lax.fori_loop(0, WIDE * LEV, cell, 0)


def outer_advect(side, halo, partial, winds, first, second, taps, inner):
    vmem = pl.BlockSpec(memory_space=pltpu.VMEM)
    return pl.pallas_call(
        outer_kernel,
        in_specs=[pl.BlockSpec(memory_space=pltpu.SMEM)]
        + [vmem] * 5
        + [pl.BlockSpec(memory_space=pl.ANY)] * 2,
        out_specs=vmem,
        out_shape=jax.ShapeDtypeStruct((NTR * LEV * ROWS, COLS), jnp.float32),
        scratch_shapes=[
            pltpu.VMEM((WIDE, 3, L_TAPS, W_TAPS, LEV, COLS), jnp.float32),
            pltpu.VMEM((SIDE_TAPS, PER_GROUP, T_TAPS, 8, COLS), jnp.float32),
            pltpu.VMEM((WIDE, SPREADS, LEV, COLS), jnp.float32),
            pltpu.SemaphoreType.DMA((2,)),
        ],
        compiler_params=params(60),
    )(side, halo, partial, winds, first, second, taps, inner)


def combine_kernel(
    arrived_hbm, moved_hbm, out_hbm, arrived_buf, moved_buf, out_buf, arrived_sems, moved_sem, out_sems, *totals
):
    sources, deep, cols = arrived_hbm.shape
    rows = (deep - MARK_ROWS) // CAP
    groups = sources // SOURCE_STEP

    def load(group):
        at = pl.ds(group * SOURCE_STEP, SOURCE_STEP)
        return pltpu.make_async_copy(arrived_hbm.at[at], arrived_buf.at[at], arrived_sems.at[group])

    for group in range(groups):
        load(group).start()
    moved_load = pltpu.make_async_copy(moved_hbm, moved_buf, moved_sem)
    moved_load.start()
    for total in totals:
        total[...] = jnp.zeros(total.shape, jnp.float32)

    def add(group, carry):
        load(group).wait()
        blocks = []
        for which in range(SOURCE_STEP):
            marks = arrived_buf[group * SOURCE_STEP + which, CAP * rows : deep, :]
            marks = marks.astype(jnp.float32).astype(jnp.int32)
            blocks += [marks[rank, 0] for rank in range(CAP)]
        for which in range(SOURCE_STEP):
            for rank in range(CAP):
                item = which * CAP + rank
                total = totals[item % SUMS]
                at = pl.ds(pl.multiple_of(blocks[item] * rows, rows), rows)
                piece = arrived_buf[group * SOURCE_STEP + which, rank * rows : (rank + 1) * rows, :]
                total[at, :] = total[at, :] + piece.astype(jnp.float32)
        return carry

    lax.fori_loop(0, groups, add, 0)
    moved_load.wait()
    share = rows // OUT_PARTS
    stores = []
    for part in range(OUT_PARTS):
        for row in range(part * share, (part + 1) * share):
            at = row * ROWS
            picked = moved_buf[at : at + ROWS, :]
            for total in totals:
                picked = picked + total[pl.ds(row, BLK_DEV, stride=rows), :]
            out_buf[at : at + ROWS, :] = picked
        at = pl.ds(part * share * ROWS, share * ROWS)
        stores.append(pltpu.make_async_copy(out_buf.at[at], out_hbm.at[at], out_sems.at[part]))
        stores[-1].start()
    for store in stores:
        store.wait()


def combine(arrived, moved):
    sources, deep, cols = arrived.shape
    rows = (deep - MARK_ROWS) // CAP
    anywhere = pl.BlockSpec(memory_space=pl.ANY)
    return pl.pallas_call(
        combine_kernel,
        in_specs=[anywhere] * 2,
        out_specs=anywhere,
        scratch_shapes=[
            pltpu.VMEM(arrived.shape, arrived.dtype),
            pltpu.VMEM(moved.shape, moved.dtype),
            pltpu.VMEM(moved.shape, moved.dtype),
            pltpu.SemaphoreType.DMA((sources // SOURCE_STEP,)),
            pltpu.SemaphoreType.DMA,
            pltpu.SemaphoreType.DMA((OUT_PARTS,)),
        ]
        + [pltpu.VMEM(((BLK_DEV + 1) * rows, cols), jnp.float32)] * SUMS,
        out_shape=jax.ShapeDtypeStruct(moved.shape, jnp.float32),
        compiler_params=params(60),
    )(arrived, moved)


def side_columns(tracers, winds):
    lons = lax.axis_size("lon")
    edge = pack(tracers, winds)
    around = [(i, (i + 1) % lons) for i in range(lons)]
    return lax.ppermute(edge, "lon", around), lax.ppermute(edge, "lon", [(b, a) for a, b in around])


def advect(tracers, winds, left, right, first, second):
    lats = lax.axis_size("lat")
    odd = lax.rem(lax.axis_index("lat"), 2).reshape(1).astype(jnp.int32)
    near_rows, far_rows = outer_rows(odd, tracers, winds, left, right)

    def swapped(value, start):
        pairs = [(i, i + 1) for i in range(start, lats - 1, 2)]
        return lax.ppermute(value, "lat", pairs + [(b, a) for a, b in pairs])

    near, far = swapped(near_rows, 0), swapped(far_rows, 1)
    inner, partial, taps = inner_advect(tracers, winds, left, right, first, second)
    moved = outer_advect(1 - odd, near, partial, winds, first, second, taps, inner)
    return outer_advect(odd, far, partial, winds, first, second, taps, moved)


def body(
    tracers, winds, depart_first, depart_second, fluxes, remap_weights, target_device, target_block
):
    shape = tracers.shape
    devices = lax.axis_size("lat") * lax.axis_size("lon")
    tracers, winds, depart_first, depart_second = (
        field.reshape(-1, COLS) for field in (tracers, winds, depart_first, depart_second)
    )
    left, right = side_columns(tracers, winds)
    chunks = remap(fluxes, remap_weights, target_device, target_block, devices)
    chunks, left, right = lax.optimization_barrier((chunks, left, right))
    arrived = lax.all_to_all(chunks, ("lat", "lon"), split_axis=0, concat_axis=0, tiled=True)
    moved = advect(tracers, winds, left, right, depart_first, depart_second)
    return combine(arrived, moved).reshape(shape)


def solution(mesh):
    in_specs = (
        P(None, None, "lat", "lon"),
        P(None, None, "lat", "lon"),
        P(None, None, "lat", "lon"),
        P(None, None, "lat", "lon"),
        P(("lat", "lon"), None, None),
        P(("lat", "lon"), None, None, None),
        P(("lat", "lon"), None),
        P(("lat", "lon"), None),
    )
    out_specs = P(None, None, "lat", "lon")
    return jax.shard_map(body, mesh=mesh, in_specs=in_specs, out_specs=out_specs, check_vma=False)
```

```python
import functools

import jax
import jax.numpy as jnp
from jax import lax
from jax.experimental import pallas as pl
from jax.experimental.pallas import tpu as pltpu
from jax.sharding import PartitionSpec as P

NTR = 16
LEV = 8
CAP = 2
BLK_DEV = 16
ROWS = 16
COLS = 128
WIDE = 4
NEAR = 3
WROWS = ROWS + 2 * WIDE
TROWS = ROWS + 2 * NEAR
EDGE = 2 * WIDE
PER_GROUP = COLS // EDGE
TILE_STEP = 6
SOURCE_STEP = 16
SUMS = 1
MARK_ROWS = 8
OUT_PARTS = 4


def params(mebibytes):
    return pltpu.CompilerParams(vmem_limit_bytes=mebibytes * 1024 * 1024)


def remap_kernel(
    device_ref, block_ref, flux_hbm, weight_hbm, out_hbm, flux_buf, weight_buf, held, marks, sent,
    flux_sems, weight_sems, out_sem, mark_sem, counts,
):
    tiles = flux_hbm.shape[0]
    links, rows = weight_hbm.shape[1], flux_hbm.shape[1]
    groups = tiles // TILE_STEP

    def loads(group):
        at = pl.ds(group * TILE_STEP, TILE_STEP)
        return (
            pltpu.make_async_copy(flux_hbm.at[at], flux_buf.at[at], flux_sems.at[group]),
            pltpu.make_async_copy(weight_hbm.at[at], weight_buf.at[at], weight_sems.at[group]),
        )

    for group in range(groups):
        for load in loads(group):
            load.start()

    def clear(i, carry):
        counts[i] = 0
        return carry

    lax.fori_loop(0, counts.shape[0], clear, 0, unroll=8)
    marks[...] = jnp.full(marks.shape, BLK_DEV, jnp.float32)

    def place(tile, link):
        owner = device_ref[link, tile]
        rank = counts[owner]
        counts[owner] = rank + 1
        value = block_ref[link, tile].astype(jnp.float32)
        marks[owner, pl.ds(rank, 1), :] = jnp.full((1, COLS), value, jnp.float32)
        return owner, pl.ds(pl.multiple_of(rank * rows, rows), rows)

    def work(group, carry):
        for load in loads(group):
            load.wait()
        for part in range(TILE_STEP):
            at = group * TILE_STEP + part
            flux = flux_buf[at]
            for pair in range(links // 2):
                both = jnp.concatenate(
                    [weight_buf[at, 2 * pair], weight_buf[at, 2 * pair + 1]], axis=1
                )
                made = jnp.dot(flux, both, preferred_element_type=jnp.float32)
                made = made.astype(jnp.bfloat16)
                for side in range(2):
                    into = pl.ds(side * rows, rows)
                    held[at * (links // 2) + pair, into] = made[:, side * COLS : (side + 1) * COLS]
        for part in range(TILE_STEP):
            at = group * TILE_STEP + part
            for link in range(links):
                owner, into = place(at, link)
                source = held.at[at * (links // 2) + link // 2, pl.ds(link % 2 * rows, rows)]
                pltpu.make_async_copy(source, out_hbm.at[owner, into], out_sem).start()
        return carry

    lax.fori_loop(0, groups, work, 0)
    sent[...] = marks[...].astype(jnp.bfloat16)
    last = pltpu.make_async_copy(sent, out_hbm.at[:, pl.ds(CAP * rows, MARK_ROWS)], mark_sem)
    last.start()
    last.wait()
    everything = out_hbm.at[pl.ds(0, tiles * links // 2), pl.ds(0, 2 * rows)]
    pltpu.make_async_copy(held, everything, out_sem).wait()


def remap(fluxes, remap_weights, target_device, target_block, devices):
    tiles, rows, cells = fluxes.shape
    links, cols = remap_weights.shape[1], remap_weights.shape[3]
    anywhere = pl.BlockSpec(memory_space=pl.ANY)
    groups = tiles // TILE_STEP
    return pl.pallas_call(
        remap_kernel,
        in_specs=[pl.BlockSpec(memory_space=pltpu.SMEM)] * 2 + [anywhere] * 2,
        out_specs=anywhere,
        scratch_shapes=[
            pltpu.VMEM(fluxes.shape, jnp.bfloat16),
            pltpu.VMEM(remap_weights.shape, jnp.bfloat16),
            pltpu.VMEM((tiles * links // 2, 2 * rows, cols), jnp.bfloat16),
            pltpu.VMEM((devices, MARK_ROWS, cols), jnp.float32),
            pltpu.VMEM((devices, MARK_ROWS, cols), jnp.bfloat16),
            pltpu.SemaphoreType.DMA((groups,)),
            pltpu.SemaphoreType.DMA((groups,)),
            pltpu.SemaphoreType.DMA,
            pltpu.SemaphoreType.DMA,
            pltpu.SMEM((devices,), jnp.int32),
        ],
        out_shape=jax.ShapeDtypeStruct((devices, CAP * rows + MARK_ROWS, cols), jnp.bfloat16),
        compiler_params=params(60),
    )(target_device.T, target_block.T, fluxes, remap_weights)


def wind_piece(winds_ref, row, comp):
    return winds_ref[pl.ds(comp * LEV * ROWS + row, LEV, stride=ROWS), :]


def tracer_piece(tracers_ref, row, level, half):
    start = half * 8 * LEV * ROWS + level * ROWS + row
    return tracers_ref[pl.ds(start, 8, stride=LEV * ROWS), :]


WIND_MSG = WIDE * 3 * LEV
TRACER_MSG = NEAR * LEV * NTR
MSG = WIND_MSG + TRACER_MSG
EDGE_ROWS = (NTR + LEV) * 8
LOADS = 4


def pack_kernel(tracers_hbm, winds_hbm, edge_ref, tracers_ref, winds_ref, sems):
    share = NTR * LEV * ROWS // LOADS
    loads = [pltpu.make_async_copy(winds_hbm, winds_ref, sems.at[LOADS])]
    for part in range(LOADS):
        at = pl.ds(part * share, share)
        loads.append(pltpu.make_async_copy(tracers_hbm.at[at], tracers_ref.at[at], sems.at[part]))
    for load in loads:
        load.start()
    group_of = lax.broadcasted_iota(jnp.int32, (8, COLS), 1) // EDGE

    def packed(pieces):
        held = jnp.zeros((8, COLS), jnp.float32)
        for spot, piece in enumerate(pieces):
            turned = pltpu.roll(piece, (WIDE + EDGE * spot) % COLS, 1)
            held = jnp.where(group_of == spot, turned, held)
        return held

    loads[0].wait()
    for level in range(LEV):
        starts = [
            comp * LEV * ROWS + level * ROWS + half * 8 for comp in range(3) for half in range(2)
        ]
        at = (NTR + level) * 8
        edge_ref[at : at + 8, :] = packed([winds_ref[start : start + 8, :] for start in starts])
    for tracer in range(NTR):
        if tracer % (NTR // LOADS) == 0:
            loads[1 + tracer // (NTR // LOADS)].wait()
        starts = [tracer * LEV * ROWS + spot * 8 for spot in range(PER_GROUP)]
        at = tracer * 8
        edge_ref[at : at + 8, :] = packed([tracers_ref[start : start + 8, :] for start in starts])


def pack(tracers, winds):
    return pl.pallas_call(
        pack_kernel,
        in_specs=[pl.BlockSpec(memory_space=pl.ANY)] * 2,
        out_specs=pl.BlockSpec(memory_space=pltpu.VMEM),
        out_shape=jax.ShapeDtypeStruct((EDGE_ROWS, COLS), jnp.float32),
        scratch_shapes=[
            pltpu.VMEM(tracers.shape, jnp.float32),
            pltpu.VMEM(winds.shape, jnp.float32),
            pltpu.SemaphoreType.DMA((LOADS + 1,)),
        ],
        compiler_params=params(60),
    )(tracers, winds)


def merged_edges(left, right):
    lane = lax.broadcasted_iota(jnp.int32, left.shape, 1)
    return jnp.where(lax.rem(lane, EDGE) < WIDE, left, right)


def rows_kernel(odd_ref, tracers_ref, winds_ref, left_ref, right_ref, near_ref, far_ref):
    both = merged_edges(left_ref[...], right_ref[...])

    def fill(target, wind_from, tracer_from):
        for row in range(WIDE):
            for comp in range(3):
                at = (row * 3 + comp) * LEV
                target[at : at + LEV, :] = wind_piece(winds_ref, wind_from + row, comp)
        for row in range(NEAR):
            for level in range(LEV):
                for half in range(2):
                    at = WIND_MSG + (row * LEV + level) * NTR + half * 8
                    target[at : at + 8, :] = tracer_piece(
                        tracers_ref, tracer_from + row, level, half
                    )
        target[MSG : MSG + EDGE_ROWS, :] = both

    @pl.when(odd_ref[0] == 0)
    def _():
        fill(near_ref, ROWS - WIDE, ROWS - NEAR)
        fill(far_ref, 0, 0)

    @pl.when(odd_ref[0] == 1)
    def _():
        fill(near_ref, 0, 0)
        fill(far_ref, ROWS - WIDE, ROWS - NEAR)


def outer_rows(odd, tracers, winds, left, right):
    return pl.pallas_call(
        rows_kernel,
        in_specs=[pl.BlockSpec(memory_space=pltpu.SMEM)]
        + [pl.BlockSpec(memory_space=pltpu.VMEM)] * 4,
        out_shape=[jax.ShapeDtypeStruct((MSG + EDGE_ROWS, COLS), jnp.float32)] * 2,
        compiler_params=params(8),
    )(odd, tracers, winds, left, right)


def cubic_weights(frac):
    first = -frac * (frac - 1.0) * (frac - 2.0) / 6.0
    second = (frac + 1.0) * (frac - 1.0) * (frac - 2.0) / 2.0
    third = -(frac + 1.0) * frac * (frac - 2.0) / 2.0
    fourth = (frac + 1.0) * frac * (frac - 1.0) / 6.0
    return (first, second, third, fourth)


def spread_weights(offset, frac, lowest, highest):
    stencil = cubic_weights(frac)
    hits = {value: offset == value for value in range(lowest, highest + 1)}
    spread = []
    for target in range(lowest - 1, highest + 3):
        weight = jnp.zeros(frac.shape, jnp.float32)
        for step in range(4):
            value = target - step + 1
            if value in hits:
                weight = weight + jnp.where(hits[value], stencil[step], 0.0)
        spread.append(weight)
    return spread


def column_shifts(main, edge, reach):
    lane = lax.broadcasted_iota(jnp.int32, main.shape, 1)
    shifted = []
    for step in range(-reach, reach + 1):
        if step == 0:
            shifted.append(main)
            continue
        inside = lane < COLS - step if step > 0 else lane >= -step
        turn = (COLS - step) % COLS
        shifted.append(jnp.where(inside, pltpu.roll(main, turn, 1), pltpu.roll(edge, turn, 1)))
    return shifted


def level_shift(value, step):
    if step == 0:
        return value
    level = lax.broadcasted_iota(jnp.int32, value.shape, 0)
    turned = pltpu.roll(value, (LEV - step) % LEV, 0)
    if step > 0:
        end = jnp.broadcast_to(value[LEV - 1 : LEV, :], value.shape)
        return jnp.where(level >= LEV - step, end, turned)
    end = jnp.broadcast_to(value[0:1, :], value.shape)
    return jnp.where(level < -step, end, turned)


W_TAPS = 9
T_TAPS = 7
L_TAPS = 5
SPREADS = L_TAPS + 2 * T_TAPS
SIDE_ROWS = 2 * WIDE
SIDE_TAPS = WIDE + 2 * NEAR


def edge_piece(ref, start, spot):
    return pltpu.roll(ref[pl.ds(start, 8, stride=8), :], (COLS - WIDE - EDGE * spot) % COLS, 1)


def keep_wind_taps(taps, onto, comp, main, edge):
    shifted = column_shifts(main, edge, WIDE)
    for side in range(W_TAPS):
        for above in range(L_TAPS):
            taps[onto, comp, above, side] = level_shift(shifted[side], above - 2)


def keep_tracer_taps(taps, onto, main_of, edges, base, within, upper):
    for spot in range(PER_GROUP):
        level, half = spot // 2, spot % 2
        edge = edge_piece(edges, base + half * 64 + within, level * 2 + upper)
        shifted = column_shifts(main_of(level, half), edge, NEAR)
        for side in range(T_TAPS):
            taps[onto, spot, side] = shifted[side]


def components(ref, row):
    return [ref[pl.ds(comp * LEV * ROWS + row, LEV, stride=ROWS), :] for comp in range(3)]


def first_weights(winds_ref, first_ref, row):
    wind, first = components(winds_ref, row), components(first_ref, row)
    frac = [jnp.clip(-w - d.astype(jnp.float32), 0.0, 1.0) for w, d in zip(wind, first)]
    level_w = spread_weights(first[0], frac[0], -1, 0)
    row_w = spread_weights(first[1], frac[1], -3, 2)
    col_w = spread_weights(first[2], frac[2], -3, 2)
    return wind, level_w, row_w, col_w


def wind_sum(taps, rows, total, level_w, row_w, col_w):
    total = list(total)
    for above in range(L_TAPS):
        part = [jnp.zeros((LEV, COLS), jnp.float32) for _ in range(3)]
        for across, place in rows:
            for comp in range(3):
                inner = col_w[0] * taps[place, comp, above, 0]
                for side in range(1, W_TAPS):
                    inner = inner + col_w[side] * taps[place, comp, above, side]
                part[comp] = part[comp] + row_w[across] * inner
        for comp in range(3):
            total[comp] = total[comp] + level_w[above] * part[comp]
    return total


def keep_second_weights(spread_ref, place, wind, midwind, second_ref, row):
    second = components(second_ref, row)
    frac = [
        jnp.clip(-(w + m) * 0.5 - d.astype(jnp.float32), 0.0, 1.0)
        for w, m, d in zip(wind, midwind, second)
    ]
    weights = spread_weights(second[0], frac[0], -1, 0)
    weights += spread_weights(second[1], frac[1], -2, 1)
    weights += spread_weights(second[2], frac[2], -2, 1)
    for which in range(SPREADS):
        spread_ref[place, which] = weights[which]


def move_cell(taps, first_tap, spread_ref, place, level, row, out_ref):
    def weight(which):
        return jnp.broadcast_to(spread_ref[place, which, pl.ds(level, 1), :], (8, COLS))

    row_w = [weight(L_TAPS + which) for which in range(T_TAPS)]
    col_w = [weight(L_TAPS + T_TAPS + which) for which in range(T_TAPS)]
    total = [jnp.zeros((8, COLS), jnp.float32) for _ in range(2)]
    for above in range(L_TAPS):
        source = jnp.clip(level + above - 2, 0, LEV - 1)
        level_w = weight(above)
        part = [jnp.zeros((8, COLS), jnp.float32) for _ in range(2)]
        for across in range(T_TAPS):
            for half in range(2):
                piece = taps.at[first_tap + across, source * 2 + half]
                inner = col_w[0] * piece[0]
                for side in range(1, T_TAPS):
                    inner = inner + col_w[side] * piece[side]
                part[half] = part[half] + row_w[across] * inner
        for half in range(2):
            total[half] = total[half] + level_w * part[half]
    for half in range(2):
        start = half * 8 * LEV * ROWS + level * ROWS + row
        out_ref[pl.ds(start, 8, stride=LEV * ROWS), :] = total[half]


def inner_kernel(
    tracers_ref, winds_ref, left_ref, right_ref, first_ref, second_ref, out_ref, partial_ref,
    taps_hbm, edges, wind_taps, tracer_taps, spread_ref, taps_sem,
):
    edges[...] = merged_edges(left_ref[...], right_ref[...])
    for upper in range(2):

        def own_taps(within, carry, upper=upper):
            row = upper * 8 + within
            main_of = functools.partial(tracer_piece, tracers_ref, row)
            keep_tracer_taps(tracer_taps, row, main_of, edges, 0, within, upper)
            return carry

        lax.fori_loop(0, 8, own_taps, 0)
    save = pltpu.make_async_copy(tracer_taps, taps_hbm, taps_sem)
    save.start()
    for comp in range(3):
        for row in range(ROWS):
            edge = edge_piece(edges, NTR * 8 + row % 8, comp * 2 + row // 8)
            keep_wind_taps(wind_taps, row + WIDE, comp, wind_piece(winds_ref, row, comp), edge)
    for place in (0, WIDE + ROWS):
        wind_taps[pl.ds(place, WIDE)] = jnp.zeros((WIDE,) + wind_taps.shape[1:], jnp.float32)

    def midwind_of(row):
        wind, level_w, row_w, col_w = first_weights(winds_ref, first_ref, row)
        zero = [jnp.zeros((LEV, COLS), jnp.float32)] * 3
        rows = [(across, row + across) for across in range(W_TAPS)]
        return wind, wind_sum(wind_taps, rows, zero, level_w, row_w, col_w)

    def middle_row(place, carry):
        row = place + WIDE
        wind, midwind = midwind_of(row)
        keep_second_weights(spread_ref, place, wind, midwind, second_ref, row)
        return carry

    lax.fori_loop(0, ROWS - SIDE_ROWS, middle_row, 0)

    def side_row(place, carry):
        row = jnp.where(place < WIDE, place, place + ROWS - SIDE_ROWS)
        midwind = midwind_of(row)[1]
        for comp in range(3):
            partial_ref[place, comp] = midwind[comp]
        return carry

    lax.fori_loop(0, SIDE_ROWS, side_row, 0)

    def cell(index, carry):
        place, level = index // LEV, lax.rem(index, LEV)
        row = place + WIDE
        move_cell(tracer_taps, row - NEAR, spread_ref, place, level, row, out_ref)
        return carry

    lax.fori_loop(0, (ROWS - SIDE_ROWS) * LEV, cell, 0)
    save.wait()


def inner_advect(tracers, winds, left, right, first, second):
    vmem = pl.BlockSpec(memory_space=pltpu.VMEM)
    taps = (ROWS, PER_GROUP, T_TAPS, 8, COLS)
    return pl.pallas_call(
        inner_kernel,
        in_specs=[vmem] * 6,
        out_specs=[vmem, vmem, pl.BlockSpec(memory_space=pl.ANY)],
        out_shape=[
            jax.ShapeDtypeStruct((NTR * LEV * ROWS, COLS), jnp.float32),
            jax.ShapeDtypeStruct((SIDE_ROWS, 3, LEV, COLS), jnp.float32),
            jax.ShapeDtypeStruct(taps, jnp.float32),
        ],
        scratch_shapes=[
            pltpu.VMEM((EDGE_ROWS, COLS), jnp.float32),
            pltpu.VMEM((WROWS, 3, L_TAPS, W_TAPS, LEV, COLS), jnp.float32),
            pltpu.VMEM(taps, jnp.float32),
            pltpu.VMEM((ROWS - SIDE_ROWS, SPREADS, LEV, COLS), jnp.float32),
            pltpu.SemaphoreType.DMA,
        ],
        compiler_params=params(40),
    )(tracers, winds, left, right, first, second)


def outer_kernel(
    side_ref, halo_ref, partial_ref, winds_ref, first_ref, second_ref, taps_hbm, inner_hbm, out_ref,
    wind_taps, tracer_taps, spread_ref, sems,
):
    side = side_ref[0]
    own = SIDE_TAPS - NEAR
    loads = (
        pltpu.make_async_copy(
            taps_hbm.at[pl.ds(side * (ROWS - own), own)],
            tracer_taps.at[pl.ds((1 - side) * NEAR, own)],
            sems.at[0],
        ),
        pltpu.make_async_copy(inner_hbm, out_ref, sems.at[1]),
    )
    for load in loads:
        load.start()

    def prepare(late):
        upper = 1 - late
        for comp in range(3):
            for row in range(WIDE):
                at = (row * 3 + comp) * LEV
                within = row + (8 - WIDE if upper else 0)
                edge = edge_piece(halo_ref, MSG + NTR * 8 + within, comp * 2 + upper)
                keep_wind_taps(wind_taps, row, comp, halo_ref[at : at + LEV, :], edge)
        for place in range(WIDE):
            row = place + late * (ROWS - WIDE)
            wind, level_w, row_w, col_w = first_weights(winds_ref, first_ref, row)
            if late:
                rows = [
                    (across, row + across - ROWS - WIDE)
                    for across in range(WIDE + ROWS - row, W_TAPS)
                ]
            else:
                rows = [(across, place + across) for across in range(WIDE - place)]
            total = [partial_ref[place + late * WIDE, comp] for comp in range(3)]
            midwind = wind_sum(wind_taps, rows, total, level_w, row_w, col_w)
            keep_second_weights(spread_ref, place, wind, midwind, second_ref, row)

        def halo_taps(row, carry):
            def main_of(level, half):
                at = WIND_MSG + row * LEV * NTR + level * NTR + half * 8
                return halo_ref[pl.ds(pl.multiple_of(at, 8), 8), :]

            within = row + (8 - NEAR if upper else 0)
            onto = row + late * own
            keep_tracer_taps(tracer_taps, onto, main_of, halo_ref, MSG, within, upper)
            return carry

        lax.fori_loop(0, NEAR, halo_taps, 0)

    for late in range(2):
        pl.when(side == late)(functools.partial(prepare, late))
    for load in loads:
        load.wait()

    def cell(index, carry):
        place, level = index // LEV, lax.rem(index, LEV)
        row = place + side * (ROWS - WIDE)
        move_cell(tracer_taps, place, spread_ref, place, level, row, out_ref)
        return carry

    lax.fori_loop(0, WIDE * LEV, cell, 0)


def outer_advect(side, halo, partial, winds, first, second, taps, inner):
    vmem = pl.BlockSpec(memory_space=pltpu.VMEM)
    return pl.pallas_call(
        outer_kernel,
        in_specs=[pl.BlockSpec(memory_space=pltpu.SMEM)]
        + [vmem] * 5
        + [pl.BlockSpec(memory_space=pl.ANY)] * 2,
        out_specs=vmem,
        out_shape=jax.ShapeDtypeStruct((NTR * LEV * ROWS, COLS), jnp.float32),
        scratch_shapes=[
            pltpu.VMEM((WIDE, 3, L_TAPS, W_TAPS, LEV, COLS), jnp.float32),
            pltpu.VMEM((SIDE_TAPS, PER_GROUP, T_TAPS, 8, COLS), jnp.float32),
            pltpu.VMEM((WIDE, SPREADS, LEV, COLS), jnp.float32),
            pltpu.SemaphoreType.DMA((2,)),
        ],
        compiler_params=params(24),
    )(side, halo, partial, winds, first, second, taps, inner)


def combine_kernel(
    arrived_hbm, moved_hbm, out_hbm, arrived_buf, moved_buf, out_buf, arrived_sems, moved_sem, out_sems, *totals
):
    sources, deep, cols = arrived_hbm.shape
    rows = (deep - MARK_ROWS) // CAP
    groups = sources // SOURCE_STEP

    def load(group):
        at = pl.ds(group * SOURCE_STEP, SOURCE_STEP)
        return pltpu.make_async_copy(arrived_hbm.at[at], arrived_buf.at[at], arrived_sems.at[group])

    for group in range(groups):
        load(group).start()
    moved_load = pltpu.make_async_copy(moved_hbm, moved_buf, moved_sem)
    moved_load.start()
    for total in totals:
        total[...] = jnp.zeros(total.shape, jnp.float32)

    def add(group, carry):
        load(group).wait()
        blocks = []
        for which in range(SOURCE_STEP):
            marks = arrived_buf[group * SOURCE_STEP + which, CAP * rows : deep, :]
            marks = marks.astype(jnp.float32).astype(jnp.int32)
            blocks += [marks[rank, 0] for rank in range(CAP)]
        for which in range(SOURCE_STEP):
            for rank in range(CAP):
                item = which * CAP + rank
                total = totals[item % SUMS]
                at = pl.ds(pl.multiple_of(blocks[item] * rows, rows), rows)
                piece = arrived_buf[group * SOURCE_STEP + which, rank * rows : (rank + 1) * rows, :]
                total[at, :] = total[at, :] + piece.astype(jnp.float32)
        return carry

    lax.fori_loop(0, groups, add, 0)
    moved_load.wait()
    share = rows // OUT_PARTS
    stores = []
    for part in range(OUT_PARTS):
        for row in range(part * share, (part + 1) * share):
            at = row * ROWS
            picked = moved_buf[at : at + ROWS, :]
            for total in totals:
                picked = picked + total[pl.ds(row, BLK_DEV, stride=rows), :]
            out_buf[at : at + ROWS, :] = picked
        at = pl.ds(part * share * ROWS, share * ROWS)
        stores.append(pltpu.make_async_copy(out_buf.at[at], out_hbm.at[at], out_sems.at[part]))
        stores[-1].start()
    for store in stores:
        store.wait()


def combine(arrived, moved):
    sources, deep, cols = arrived.shape
    rows = (deep - MARK_ROWS) // CAP
    anywhere = pl.BlockSpec(memory_space=pl.ANY)
    return pl.pallas_call(
        combine_kernel,
        in_specs=[anywhere] * 2,
        out_specs=anywhere,
        scratch_shapes=[
            pltpu.VMEM(arrived.shape, arrived.dtype),
            pltpu.VMEM(moved.shape, moved.dtype),
            pltpu.VMEM(moved.shape, moved.dtype),
            pltpu.SemaphoreType.DMA((sources // SOURCE_STEP,)),
            pltpu.SemaphoreType.DMA,
            pltpu.SemaphoreType.DMA((OUT_PARTS,)),
        ]
        + [pltpu.VMEM(((BLK_DEV + 1) * rows, cols), jnp.float32)] * SUMS,
        out_shape=jax.ShapeDtypeStruct(moved.shape, jnp.float32),
        compiler_params=params(60),
    )(arrived, moved)


def side_columns(tracers, winds):
    lons = lax.axis_size("lon")
    edge = pack(tracers, winds)
    around = [(i, (i + 1) % lons) for i in range(lons)]
    return lax.ppermute(edge, "lon", around), lax.ppermute(edge, "lon", [(b, a) for a, b in around])


def advect(tracers, winds, left, right, first, second):
    lats = lax.axis_size("lat")
    odd = lax.rem(lax.axis_index("lat"), 2).reshape(1).astype(jnp.int32)
    near_rows, far_rows = outer_rows(odd, tracers, winds, left, right)

    def swapped(value, start):
        pairs = [(i, i + 1) for i in range(start, lats - 1, 2)]
        return lax.ppermute(value, "lat", pairs + [(b, a) for a, b in pairs])

    near, far = swapped(near_rows, 0), swapped(far_rows, 1)
    inner, partial, taps = inner_advect(tracers, winds, left, right, first, second)
    moved = outer_advect(1 - odd, near, partial, winds, first, second, taps, inner)
    return outer_advect(odd, far, partial, winds, first, second, taps, moved)


def body(
    tracers, winds, depart_first, depart_second, fluxes, remap_weights, target_device, target_block
):
    shape = tracers.shape
    devices = lax.axis_size("lat") * lax.axis_size("lon")
    tracers, winds, depart_first, depart_second = (
        field.reshape(-1, COLS) for field in (tracers, winds, depart_first, depart_second)
    )
    left, right = side_columns(tracers, winds)
    chunks = remap(fluxes, remap_weights, target_device, target_block, devices)
    chunks, left, right = lax.optimization_barrier((chunks, left, right))
    arrived = lax.all_to_all(chunks, ("lat", "lon"), split_axis=0, concat_axis=0, tiled=True)
    moved = advect(tracers, winds, left, right, depart_first, depart_second)
    return combine(arrived, moved).reshape(shape)


def solution(mesh):
    in_specs = (
        P(None, None, "lat", "lon"),
        P(None, None, "lat", "lon"),
        P(None, None, "lat", "lon"),
        P(None, None, "lat", "lon"),
        P(("lat", "lon"), None, None),
        P(("lat", "lon"), None, None, None),
        P(("lat", "lon"), None),
        P(("lat", "lon"), None),
    )
    out_specs = P(None, None, "lat", "lon")
    return jax.shard_map(body, mesh=mesh, in_specs=in_specs, out_specs=out_specs, check_vma=False)
```
